256 devices in a mesh: band: 2 (over z), tm: 128 (over x, y, core).
Axes of the slice: x: 8, y: 8, z: 2, core: 2. Of those that a mesh axis runs over, the one named last changes fastest.
The devices are a block of a 8x8x16 slice.
Arguments:
- volts: int32 [8, 2, 25165824], P('band', None, 'tm'), parts along dimension 0, may hold values from -128 to 127, as said below
- taps: float32 [16, 4096], replicated, may hold values from -0.024 to 0.024
- pairs: int32 [4, 2], replicated, may hold values from 0 to 3, as said below
Outputs:
- coherence: float32 [8, 4096], P('band'), parts along dimension 0
- normalized: float32 [2, 8, 6144, 4096], P(None, 'band', 'tm'), parts along dimension 1
The draws below stay inside these ranges and needn't reach their ends.
There are 2 independent parts, one for each index of `band`. The reference program is written for one: setup_inputs(seed, part) draws one part's arguments, and reference() takes and returns one part's arrays. A program takes and returns all parts, laid end to end along the dimension named above; an argument that names none is the same for every part. Nothing has to cross between parts.
Inputs may be any that keep to these rules, and one draw needn't show every extreme that they name: `volts`: every sample is a whole number of the int8 range. Each pair names a stream of the first antenna (0 or 1) and then one of the second antenna (2 or 3); the four pairs are distinct.
All inputs are finite; a program needn't handle non-finite values.
Results may differ from the reference program's by a relative error of at most 0.000067.
Values sent between devices are 32-bit elements; how exact they have to be, the bound alone decides.
A program may use at most 128 MiB of HBM per device.

```python
import jax
import jax.numpy as jnp
from jax import lax

STREAMS = 4
TAPS = 16
CHANNELS = 4096
FRAMES = 6144
SAMPLES = 25165824


def draw_volts(key, part):
    common_key = jax.random.fold_in(key, 11)
    noise_key = jax.random.fold_in(key, 12)
    weight_key = jax.random.fold_in(key, 13)
    delay_key = jax.random.fold_in(key, 14)
    common = jax.random.randint(common_key, (2, SAMPLES), -64, 64)
    noise = jax.random.randint(noise_key, (STREAMS, 2, SAMPLES), -64, 64)
    weights = jax.random.randint(weight_key, (STREAMS,), 0, 2)
    delay = jax.random.randint(delay_key, (), 0, 8)
    delayed = jnp.roll(common, delay, axis=1)
    antenna = (jnp.arange(STREAMS) >= 2).astype(jnp.int32)
    chosen = jnp.where(antenna[:, None, None] == 1, delayed[None], common[None])
    return (noise + weights[:, None, None] * chosen).astype(jnp.int32)


def draw_pairs(key, part):
    order = jax.random.permutation(jax.random.fold_in(key, 21), 4)
    return jnp.stack([order // 2, 2 + order % 2], axis=1).astype(jnp.int32)


def gaussian(key, dims, width, most, held_as=jnp.bfloat16):
    return jnp.clip(width * jax.random.normal(key, dims, jnp.float32), -most, most).astype(held_as)


def setup_inputs(seed: int = 0, part: int = 0) -> dict:
    seeds = jax.random.split(jax.random.key(seed), 4)
    part_keys = jax.random.split(jax.random.fold_in(seeds[3], part), 4)
    volts = draw_volts(jax.random.fold_in(jax.random.fold_in(seeds[3], part), 71), part)
    taps = gaussian(seeds[1], (TAPS, CHANNELS), 0.004, 0.024, jnp.float32)
    pairs = draw_pairs(jax.random.fold_in(seeds[3], 71), part)
    return dict(volts=volts, taps=taps, pairs=pairs)


def reference(volts, taps, pairs):
    samples = volts.astype(jnp.float32).reshape(STREAMS, 2, FRAMES, CHANNELS)
    padded = jnp.pad(samples, ((0, 0), (0, 0), (TAPS - 1, 0), (0, 0)))
    filtered = jnp.zeros((STREAMS, 2, FRAMES, CHANNELS), jnp.float32)
    for tap_index in range(TAPS):
        begin = TAPS - 1 - tap_index
        filtered = filtered + taps[tap_index] * padded[:, :, begin:begin + FRAMES]
    spectra = jnp.fft.fft(filtered[:, 0] + 1j * filtered[:, 1], axis=-1) / jnp.sqrt(jnp.float32(CHANNELS))
    real_part = jnp.real(spectra).astype(jnp.float32)
    imag_part = jnp.imag(spectra).astype(jnp.float32)
    auto = lax.optimization_barrier(jnp.sum(real_part * real_part + imag_part * imag_part, axis=1)) / FRAMES
    first = pairs[:, 0]
    second = pairs[:, 1]
    left_re = real_part[first]
    left_im = imag_part[first]
    right_re = real_part[second]
    right_im = imag_part[second]
    prod_re = left_re * right_re + left_im * right_im
    prod_im = left_im * right_re - left_re * right_im
    cross_re = lax.optimization_barrier(jnp.sum(prod_re, axis=1)) / FRAMES
    cross_im = lax.optimization_barrier(jnp.sum(prod_im, axis=1)) / FRAMES
    denom = (auto[first] + 1e-06) * (auto[second] + 1e-06)
    coherence = (cross_re * cross_re + cross_im * cross_im) / denom
    factor = 1.0 / jnp.sqrt(denom)
    normalized = jnp.stack([prod_re * factor[:, None], prod_im * factor[:, None]])
    return (coherence, normalized)
```

```python
import functools
import math

import jax
import jax.numpy as jnp
import numpy as np
from jax import lax
from jax.experimental import pallas as pl
from jax.experimental.pallas import tpu as pltpu
from jax.sharding import Mesh
from jax.sharding import PartitionSpec as P

TM = ("tm_0", "tm_1", "tm_2")
ROWS = 32
LANES = 128
PITCH = 65
HALO = 16
GROUP = 8


def constants():
    lane = np.arange(LANES)
    j = 4 * (lane % 32) + lane // 32
    k = np.arange(LANES)
    angle = 2.0 * np.pi * ((j[:, None] * k[None, :]) % LANES) / LANES
    cos, sin = np.cos(angle) / 64.0, np.sin(angle) / 64.0
    full = np.block([[cos, -sin], [sin, cos]]).astype(np.float32)
    high = full.astype(jnp.bfloat16)
    low = (full - high.astype(np.float32)).astype(jnp.bfloat16)
    i = np.arange(ROWS)
    turn = 2.0 * np.pi * ((i[:, None] * k[None, :]) % 4096) / 4096
    return (
        high,
        low,
        np.cos(turn).astype(np.float32),
        np.sin(turn).astype(np.float32),
    )


def add(a, b):
    return (a[0] + b[0], a[1] + b[1])


def sub(a, b):
    return (a[0] - b[0], a[1] - b[1])


def fft4(x):
    a, b = add(x[0], x[2]), sub(x[0], x[2])
    c, d = add(x[1], x[3]), sub(x[1], x[3])
    return [
        add(a, c),
        (b[0] + d[1], b[1] - d[0]),
        sub(a, c),
        (b[0] - d[1], b[1] + d[0]),
    ]


def fft8(x):
    even = fft4(x[0::2])
    odd = fft4(x[1::2])
    r = np.float32(math.sqrt(0.5))
    turned = [
        odd[0],
        ((odd[1][0] + odd[1][1]) * r, (odd[1][1] - odd[1][0]) * r),
        (odd[2][1], -odd[2][0]),
        ((odd[3][1] - odd[3][0]) * r, (odd[3][0] + odd[3][1]) * -r),
    ]
    return [add(e, o) for e, o in zip(even, turned)] + [sub(e, o) for e, o in zip(even, turned)]


def rotate(x, index, length):
    index = index % length
    if index == 0:
        return x
    if index * 4 == length:
        return (x[1], -x[0])
    c = np.float32(math.cos(2 * math.pi * index / length))
    s = np.float32(math.sin(2 * math.pi * index / length))
    return (x[0] * c + x[1] * s, x[1] * c - x[0] * s)


def block_transpose(rows):
    turned = rows.T
    lane = lax.broadcasted_iota(jnp.int32, (32, LANES), 1)
    odd = (lane & 32) != 0
    upper = (lane & 64) != 0
    r = [turned[32 * b : 32 * b + 32] for b in range(4)]

    def pair(a, b, by, mask):
        return (
            jnp.where(mask, pltpu.roll(b, by, 1), a),
            jnp.where(mask, b, pltpu.roll(a, LANES - by, 1)),
        )

    a0, a1 = pair(r[0], r[1], 32, odd)
    b0, b1 = pair(r[2], r[3], 32, odd)
    o0, o2 = pair(a0, b0, 64, upper)
    o1, o3 = pair(a1, b1, 64, upper)
    return [o0, o1, o2, o3]


def permute_taps(taps_ref, tapb):
    def batch(tb, carry):
        high = tb // 2
        parts = [
            taps_ref[pl.ds(high * 256 + (tb % 2) * 4 + q, 32, stride=8), :] for q in range(4)
        ]
        out = block_transpose(jnp.concatenate(parts, axis=0))
        for q in range(4):
            for i in range(ROWS):
                tapb[pl.ds(pl.multiple_of((i * 16 + tb * 4 + q) * 8, 8), 8), :] = jnp.broadcast_to(
                    out[q][i : i + 1], (8, LANES)
                )
        return carry

    lax.fori_loop(0, 4, batch, 0)


def permute_samples(raw, xf, frame0, row0, batches):
    def batch(b, carry):
        for c in range(2):
            x = [raw[s, pl.ds((frame0 + 4 * b) * 64 + c, LANES, stride=2), :] for s in range(4)]
            packed = (
                (x[0] & 255)
                | ((x[1] & 255) << 8)
                | ((x[2] & 255) << 16)
                | (x[3] << 24)
            )
            out = block_transpose(packed)
            for q in range(4):
                for s in range(4):
                    value = out[q] << (24 - 8 * s) if s < 3 else out[q]
                    value = (value >> 24).astype(jnp.float32)
                    xf[2 * s + c, pl.ds(row0 + 4 * b + q, 32, stride=PITCH), :] = value
        return carry

    lax.fori_loop(0, batches, batch, 0)


def process_group(group, refs):
    (xf, tapb, wh, wl, twc, tws, yh, yl, v, u, pbuf, sums) = refs

    def fir(i, carry):
        base = i * PITCH + HALO + group * GROUP
        tap = [
            tapb[pl.ds(pl.multiple_of((i * 16 + t) * 8, 8), 8), :] for t in range(16)
        ]
        for c in range(2):
            for pair in range(2):
                ys = []
                for s in (2 * pair, 2 * pair + 1):
                    acc = None
                    for t in range(16):
                        term = tap[t] * xf[2 * s + c, pl.ds(base - t, 8), :]
                        acc = term if acc is None else acc + term
                    ys.append(acc)
                y = jnp.concatenate(ys, axis=0)
                high = y.astype(jnp.bfloat16)
                low = (y - high.astype(jnp.float32)).astype(jnp.bfloat16)
                at = pl.ds(pl.multiple_of(i * 32 + pair * 16, 16), 16)
                yh[at, c * LANES : (c + 1) * LANES] = high
                yl[at, c * LANES : (c + 1) * LANES] = low
        return carry

    lax.fori_loop(0, ROWS, fir, 0)

    def stage1(m, carry):
        at = pl.ds(pl.multiple_of(m * 256, 256), 256)
        h, l = yh[at, :], yl[at, :]
        dot = functools.partial(jnp.dot, preferred_element_type=jnp.float32)
        v[at, :] = dot(h, wh[...]) + dot(l, wh[...]) + dot(h, wl[...])
        return carry

    lax.fori_loop(0, 4, stage1, 0)

    def stage2a(s, carry):
        for i0 in range(4):
            xs = []
            for i1 in range(8):
                i = 4 * i1 + i0
                at = pl.ds(pl.multiple_of(i * 32 + s * 8, 8), 8)
                x = (v[at, :LANES], v[at, LANES:])
                if i:
                    c = twc[pl.ds(i, 8, stride=0), :] if False else jnp.broadcast_to(twc[i : i + 1, :], (8, LANES))
                    d = jnp.broadcast_to(tws[i : i + 1, :], (8, LANES))
                    x = (x[0] * c + x[1] * d, x[1] * c - x[0] * d)
                xs.append(x)
            for ka, x in enumerate(fft8(xs)):
                x = rotate(x, i0 * ka, 32)
                at = pl.ds(pl.multiple_of((s * 32 + i0 * 8 + ka) * 8, 8), 8)
                u[0, at, :] = x[0]
                u[1, at, :] = x[1]
        return carry

    lax.fori_loop(0, 4, stage2a, 0)

    def stage2b(ka, carry):
        spectra = []
        for s in range(4):
            xs = []
            for i0 in range(4):
                at = pl.ds(pl.multiple_of((s * 32 + i0 * 8 + ka) * 8, 8), 8)
                xs.append((u[0, at, :], u[1, at, :]))
            spectra.append(fft4(xs))
        for kb in range(4):
            k1 = ka + 8 * kb
            z = [spectra[s][kb] for s in range(4)]
            at = pl.ds(pl.multiple_of(k1 * 8, 8), 8)
            for s in range(4):
                sums[s, at, :] += z[s][0] * z[s][0] + z[s][1] * z[s][1]
            rows = pl.ds(pl.multiple_of(group * GROUP, 8), 8)
            cols = pl.ds(pl.multiple_of(k1 * LANES, LANES), LANES)
            for p in range(4):
                a, b = z[p // 2], z[2 + p % 2]
                re = a[0] * b[0] + a[1] * b[1]
                im = a[1] * b[0] - a[0] * b[1]
                sums[4 + p, at, :] += re
                sums[8 + p, at, :] += im
                pbuf[0, p, rows, cols] = re
                pbuf[1, p, rows, cols] = im
        return carry

    lax.fori_loop(0, 8, stage2b, 0)


def transform_kernel(
    samples_ref, halo_ref, taps_ref, wh, wl, twc, tws, prod_ref, sums_ref,
    xf, tapb, yh, yl, v, u, pbuf, sums, sems,
):
    refs = (xf, tapb, wh, wl, twc, tws, yh, yl, v, u, pbuf, sums)
    sums[...] = jnp.zeros_like(sums)
    permute_taps(taps_ref, tapb)
    permute_samples(samples_ref, xf, 0, HALO, 12)
    permute_samples(halo_ref, xf, 0, 0, 4)

    def out_copy(group):
        rows = pl.ds(pl.multiple_of(group * GROUP, 8), 8)
        return pltpu.make_async_copy(
            pbuf.at[:, :, rows, :], prod_ref.at[:, :, rows, :], sems.at[group]
        )

    def step(n, carry):
        group = lax.rem(n + 2, 6)
        process_group(group, refs)
        out_copy(group).start()
        return carry

    lax.fori_loop(0, 6, step, 0)
    for q in range(12):
        for k1 in range(ROWS):
            sums_ref[q, k1 : k1 + 1, :] = jnp.sum(
                sums[q, k1 * 8 : k1 * 8 + 8, :], axis=0, keepdims=True
            )
    for group in range(6):
        out_copy(group).wait()


def transform_call(rows, halo, taps_rows, interpret=False):
    streams = rows.shape[0]
    frames = rows.shape[1] // 64
    consts = [jnp.asarray(c) for c in constants()]
    vmem = pl.BlockSpec(memory_space=pltpu.VMEM)
    f32, bf16 = jnp.float32, jnp.bfloat16
    return pl.pallas_call(
        transform_kernel,
        out_shape=(
            jax.ShapeDtypeStruct((2, 4, frames, 4096), f32),
            jax.ShapeDtypeStruct((12, ROWS, LANES), f32),
        ),
        in_specs=[vmem] * 7,
        out_specs=(pl.BlockSpec(memory_space=pl.ANY), vmem),
        scratch_shapes=[
            pltpu.VMEM((8, ROWS * PITCH + 7, LANES), f32),
            pltpu.VMEM((ROWS * 16 * 8, LANES), f32),
            pltpu.VMEM((1024, 256), bf16),
            pltpu.VMEM((1024, 256), bf16),
            pltpu.VMEM((1024, 256), f32),
            pltpu.VMEM((2, 1024, LANES), f32),
            pltpu.VMEM((2, 4, frames, 4096), f32),
            pltpu.VMEM((12, ROWS * 8, LANES), f32),
            pltpu.SemaphoreType.DMA((6,)),
        ],
        compiler_params=pltpu.CompilerParams(vmem_limit_bytes=60 * 1024 * 1024),
        cost_estimate=pl.CostEstimate(flops=4_000_000_000, bytes_accessed=16_000_000, transcendentals=0),
        interpret=interpret,
        name="transform",
    )(rows, halo, taps_rows, *consts)


def normalize_kernel(total, canon_ref, pairs_ref, sums_ref, prod_ref, coh_ref, out_ref):
    pair = pl.program_id(0)
    canon = canon_ref[pair]
    first = pairs_ref[pair, 0]
    second = pairs_ref[pair, 1]
    scale = np.float32(1.0 / total)
    power = (sums_ref[first] * scale + 1e-06) * (sums_ref[second] * scale + 1e-06)
    factor = 1.0 / jnp.sqrt(power)

    @pl.when(pl.program_id(1) == 0)
    def _():
        re = sums_ref[4 + canon] * scale
        im = sums_ref[8 + canon] * scale
        coh_ref[0] = (re * re + im * im) / power

    for k1 in range(ROWS):
        cols = slice(k1 * LANES, (k1 + 1) * LANES)
        row = factor[k1 : k1 + 1]
        for part in range(2):
            out_ref[part, 0, :, cols] = prod_ref[part, 0, :, cols] * row


def normalize_call(pairs, sums, prods, total, block=24, interpret=False):
    frames = prods.shape[2]
    canon = pairs[:, 0] * 2 + pairs[:, 1] - 2
    f32 = jnp.float32
    coh, normalized = pl.pallas_call(
        functools.partial(normalize_kernel, total),
        grid_spec=pltpu.PrefetchScalarGridSpec(
            num_scalar_prefetch=2,
            grid=(4, frames // block),
            in_specs=[
                pl.BlockSpec((12, ROWS, LANES), lambda p, b, canon, pairs: (0, 0, 0)),
                pl.BlockSpec((2, 1, block, 4096), lambda p, b, canon, pairs: (0, canon[p], b, 0)),
            ],
            out_specs=[
                pl.BlockSpec((1, ROWS, LANES), lambda p, b, canon, pairs: (p, 0, 0)),
                pl.BlockSpec((2, 1, block, 4096), lambda p, b, canon, pairs: (0, p, b, 0)),
            ],
        ),
        out_shape=(
            jax.ShapeDtypeStruct((4, ROWS, LANES), f32),
            jax.ShapeDtypeStruct(prods.shape, f32),
        ),
        cost_estimate=pl.CostEstimate(flops=2_000_000, bytes_accessed=13_000_000, transcendentals=0),
        interpret=interpret,
        name="normalize",
    )(canon, pairs, sums, prods)
    return coh.reshape(4, ROWS * LANES), normalized


def sample_rows(volts):
    streams, comps, local = volts.shape
    rows = volts.reshape(streams, comps, local // LANES, LANES)
    return jnp.transpose(rows, (0, 2, 1, 3)).reshape(streams, local // LANES * comps, LANES)


def tap_rows(taps):
    taps = taps.reshape(2, 8, ROWS, LANES)
    return jnp.transpose(taps, (0, 2, 1, 3)).reshape(512, LANES)


def shifted(array, axis, by):
    devices = lax.axis_size(axis)
    pairs = [(i, i + by) for i in range(devices) if 0 <= i + by < devices]
    return lax.ppermute(array, axis, pairs)


def on_device(volts, taps, pairs):
    rows = sample_rows(volts)
    frames = rows.shape[1] // 64
    halo = shifted(rows[:, (frames - HALO) * 64 :], TM, 1)
    prods, sums = transform_call(rows, halo, tap_rows(taps))
    for axis in TM:
        sums = lax.psum(sums, axis)
    total = frames * lax.axis_size(TM)
    return normalize_call(pairs, sums, prods, total)


def solution(mesh):
    devices = mesh.devices
    finer = Mesh(
        devices.reshape(mesh.shape["band"], 8, 8, 2), ("band", "tm_0", "tm_1", "tm_2")
    )
    return jax.shard_map(
        on_device,
        mesh=finer,
        in_specs=(P("band", None, TM), P(), P()),
        out_specs=(P("band", None), P(None, "band", TM, None)),
        check_vma=False,
    )
```

```python
import functools
import math

import jax
import jax.numpy as jnp
import numpy as np
from jax import lax
from jax.experimental import pallas as pl
from jax.experimental.pallas import tpu as pltpu
from jax.sharding import Mesh
from jax.sharding import PartitionSpec as P

TM = ("tm_0", "tm_1", "tm_2")
ROWS = 32
LANES = 128
PITCH = 65
HALO = 16
GROUP = 8


def constants():
    lane = np.arange(LANES)
    j = 4 * (lane % 32) + lane // 32
    k = np.arange(LANES)
    angle = 2.0 * np.pi * ((j[:, None] * k[None, :]) % LANES) / LANES
    cos, sin = np.cos(angle) / 64.0, np.sin(angle) / 64.0
    full = np.block([[cos, -sin], [sin, cos]]).astype(np.float32)
    high = full.astype(jnp.bfloat16)
    low = (full - high.astype(np.float32)).astype(jnp.bfloat16)
    i = np.arange(ROWS)
    turn = 2.0 * np.pi * ((i[:, None] * k[None, :]) % 4096) / 4096
    return (
        high,
        low,
        np.cos(turn).astype(np.float32),
        np.sin(turn).astype(np.float32),
    )


def add(a, b):
    return (a[0] + b[0], a[1] + b[1])


def sub(a, b):
    return (a[0] - b[0], a[1] - b[1])


def fft4(x):
    a, b = add(x[0], x[2]), sub(x[0], x[2])
    c, d = add(x[1], x[3]), sub(x[1], x[3])
    return [
        add(a, c),
        (b[0] + d[1], b[1] - d[0]),
        sub(a, c),
        (b[0] - d[1], b[1] + d[0]),
    ]


def fft8(x):
    even = fft4(x[0::2])
    odd = fft4(x[1::2])
    r = np.float32(math.sqrt(0.5))
    turned = [
        odd[0],
        ((odd[1][0] + odd[1][1]) * r, (odd[1][1] - odd[1][0]) * r),
        (odd[2][1], -odd[2][0]),
        ((odd[3][1] - odd[3][0]) * r, (odd[3][0] + odd[3][1]) * -r),
    ]
    return [add(e, o) for e, o in zip(even, turned)] + [sub(e, o) for e, o in zip(even, turned)]


def rotate(x, index, length):
    index = index % length
    if index == 0:
        return x
    if index * 4 == length:
        return (x[1], -x[0])
    c = np.float32(math.cos(2 * math.pi * index / length))
    s = np.float32(math.sin(2 * math.pi * index / length))
    return (x[0] * c + x[1] * s, x[1] * c - x[0] * s)


def block_transpose(rows):
    turned = rows.T
    lane = lax.broadcasted_iota(jnp.int32, (32, LANES), 1)
    odd = (lane & 32) != 0
    upper = (lane & 64) != 0
    r = [turned[32 * b : 32 * b + 32] for b in range(4)]

    def pair(a, b, by, mask):
        return (
            jnp.where(mask, pltpu.roll(b, by, 1), a),
            jnp.where(mask, b, pltpu.roll(a, LANES - by, 1)),
        )

    a0, a1 = pair(r[0], r[1], 32, odd)
    b0, b1 = pair(r[2], r[3], 32, odd)
    o0, o2 = pair(a0, b0, 64, upper)
    o1, o3 = pair(a1, b1, 64, upper)
    return [o0, o1, o2, o3]


def permute_taps(taps_ref, tapb):
    def batch(tb, carry):
        high = tb // 2
        parts = [
            taps_ref[pl.ds(high * 256 + (tb % 2) * 4 + q, 32, stride=8), :] for q in range(4)
        ]
        out = block_transpose(jnp.concatenate(parts, axis=0))
        for q in range(4):
            for i in range(ROWS):
                tapb[pl.ds(pl.multiple_of((i * 16 + tb * 4 + q) * 8, 8), 8), :] = jnp.broadcast_to(
                    out[q][i : i + 1], (8, LANES)
                )
        return carry

    lax.fori_loop(0, 4, batch, 0)


def permute_batch(raw, xf, b, row0):
    for c in range(2):
        x = [raw[s, pl.ds(b * 256 + c, LANES, stride=2), :] for s in range(4)]
        packed = (
            (x[0] & 255) | ((x[1] & 255) << 8) | ((x[2] & 255) << 16) | (x[3] << 24)
        )
        out = block_transpose(packed)
        for q in range(4):
            for s in range(4):
                value = out[q] << (24 - 8 * s) if s < 3 else out[q]
                value = (value >> 24).astype(jnp.float32)
                xf[2 * s + c, pl.ds(row0 + 4 * b + q, 32, stride=PITCH), :] = value


def process_group(group, refs):
    (xf, tapb, wh, wl, twc, tws, yh, yl, v, u, pbuf, sums) = refs

    def fir(i, carry):
        base = i * PITCH + HALO + group * GROUP
        tap = [
            tapb[pl.ds(pl.multiple_of((i * 16 + t) * 8, 8), 8), :] for t in range(16)
        ]
        for c in range(2):
            for pair in range(2):
                ys = []
                for s in (2 * pair, 2 * pair + 1):
                    acc = None
                    for t in range(16):
                        term = tap[t] * xf[2 * s + c, pl.ds(base - t, 8), :]
                        acc = term if acc is None else acc + term
                    ys.append(acc)
                y = jnp.concatenate(ys, axis=0)
                high = y.astype(jnp.bfloat16)
                low = (y - high.astype(jnp.float32)).astype(jnp.bfloat16)
                at = pl.ds(pl.multiple_of(i * 32 + pair * 16, 16), 16)
                yh[at, c * LANES : (c + 1) * LANES] = high
                yl[at, c * LANES : (c + 1) * LANES] = low
        return carry

    lax.fori_loop(0, ROWS, fir, 0)

    def stage1(m, carry):
        at = pl.ds(pl.multiple_of(m * 256, 256), 256)
        h, l = yh[at, :], yl[at, :]
        dot = functools.partial(jnp.dot, preferred_element_type=jnp.float32)
        v[at, :] = dot(h, wh[...]) + dot(l, wh[...]) + dot(h, wl[...])
        return carry

    lax.fori_loop(0, 4, stage1, 0)

    def stage2a(s, carry):
        for i0 in range(4):
            xs = []
            for i1 in range(8):
                i = 4 * i1 + i0
                at = pl.ds(pl.multiple_of(i * 32 + s * 8, 8), 8)
                x = (v[at, :LANES], v[at, LANES:])
                if i:
                    c = jnp.broadcast_to(twc[i : i + 1, :], (8, LANES))
                    d = jnp.broadcast_to(tws[i : i + 1, :], (8, LANES))
                    x = (x[0] * c + x[1] * d, x[1] * c - x[0] * d)
                xs.append(x)
            for ka, x in enumerate(fft8(xs)):
                x = rotate(x, i0 * ka, 32)
                at = pl.ds(pl.multiple_of((s * 32 + i0 * 8 + ka) * 8, 8), 8)
                u[0, at, :] = x[0]
                u[1, at, :] = x[1]
        return carry

    lax.fori_loop(0, 4, stage2a, 0)

    def stage2b(ka, carry):
        spectra = []
        for s in range(4):
            xs = []
            for i0 in range(4):
                at = pl.ds(pl.multiple_of((s * 32 + i0 * 8 + ka) * 8, 8), 8)
                xs.append((u[0, at, :], u[1, at, :]))
            spectra.append(fft4(xs))
        for kb in range(4):
            k1 = ka + 8 * kb
            z = [spectra[s][kb] for s in range(4)]
            at = pl.ds(pl.multiple_of(k1 * 8, 8), 8)
            for s in range(4):
                sums[s, at, :] += z[s][0] * z[s][0] + z[s][1] * z[s][1]
            rows = pl.ds(pl.multiple_of(group * GROUP, 8), 8)
            cols = pl.ds(pl.multiple_of(k1 * LANES, LANES), LANES)
            for p in range(4):
                a, b = z[p // 2], z[2 + p % 2]
                re = a[0] * b[0] + a[1] * b[1]
                im = a[1] * b[0] - a[0] * b[1]
                sums[4 + p, at, :] += re
                sums[8 + p, at, :] += im
                pbuf[0, p, rows, cols] = re
                pbuf[1, p, rows, cols] = im
        return carry

    lax.fori_loop(0, 8, stage2b, 0)


def peers():
    x_name, y_name, c_name = TM
    cores = lax.axis_size(c_name)
    members = lax.axis_size(y_name) * cores
    columns = lax.axis_size(x_name)
    member = lax.axis_index(y_name) * cores + lax.axis_index(c_name)
    return member, lax.axis_index(x_name), members, columns, cores


def member_id(member, cores):
    return {"tm_1": member // cores, "tm_2": lax.rem(member, cores)}


def transform_kernel(
    total, samples_ref, taps_ref, wh, wl, twc, tws, prod_ref, stats_ref,
    raw, hraw, xf, tapb, yh, yl, v, u, pbuf, sums, part, rows_in, mine, cols_in, stat,
    out_sems, in_sems, halo_send, halo_recv, row_send, row_recv, col_send, col_recv,
    gat_send, gat_recv,
):
    member, column, members, columns, cores = peers()
    per = ROWS // members
    count = members * columns
    place = column * members + member
    has_next = place < count - 1
    has_prev = place > 0
    MESH = pl.DeviceIdType.MESH

    def tm_id(index):
        return {"tm_0": index // members, **member_id(lax.rem(index, members), cores)}

    def in_copy(b):
        rows = pl.ds(pl.multiple_of(b * 256, 256), 256)
        return pltpu.make_async_copy(samples_ref.at[:, rows, :], raw.at[:, rows, :], in_sems.at[b])

    for b in range(12):
        in_copy(b).start()

    barrier = pltpu.get_barrier_semaphore()
    for d in range(1, members):
        other = lax.rem(member + d, members)
        pl.semaphore_signal(
            barrier, inc=1, device_id=member_id(other, cores), device_id_type=MESH
        )
    for d in range(1, columns):
        other = lax.rem(column + d, columns)
        pl.semaphore_signal(barrier, inc=1, device_id={"tm_0": other}, device_id_type=MESH)

    first_member = member == 0
    last_member = member == members - 1

    @pl.when(jnp.logical_and(first_member, has_prev))
    def _():
        pl.semaphore_signal(barrier, inc=1, device_id=tm_id(place - 1), device_id_type=MESH)

    greeted = members - 1 + columns - 1

    @pl.when(jnp.logical_and(last_member, has_next))
    def _():
        pl.semaphore_wait(barrier, greeted + 1)

    @pl.when(jnp.logical_not(jnp.logical_and(last_member, has_next)))
    def _():
        pl.semaphore_wait(barrier, greeted)

    frames = samples_ref.shape[1] // 64

    def halo_copy(b):
        lead = 1 if b == 0 else 0
        at = (4 * b + lead) * 64
        size = (4 - lead) * 64
        start = (frames - HALO) * 64 + at
        return pltpu.make_async_remote_copy(
            src_ref=samples_ref.at[:, pl.ds(start, size), :],
            dst_ref=hraw.at[:, pl.ds(at, size), :],
            send_sem=halo_send.at[b],
            recv_sem=halo_recv.at[b],
            device_id=tm_id(place + 1),
            device_id_type=MESH,
        )

    @pl.when(has_next)
    def _():
        for b in (3, 2, 1, 0):
            halo_copy(b).start()

    @pl.when(jnp.logical_not(has_prev))
    def _():
        hraw[...] = jnp.zeros_like(hraw)

    def halo_wait(b):
        @pl.when(has_prev)
        def _():
            halo_copy(b).wait_recv()

    refs = (xf, tapb, wh, wl, twc, tws, yh, yl, v, u, pbuf, sums)
    sums[...] = jnp.zeros_like(sums)
    permute_taps(taps_ref, tapb)

    def own_batch(b, carry):
        in_copy(b).wait()
        permute_batch(raw, xf, b, HALO)
        return carry

    lax.fori_loop(0, 12, own_batch, 0)

    def out_copy(group):
        rows = pl.ds(pl.multiple_of(group * GROUP, 8), 8)
        return pltpu.make_async_copy(
            pbuf.at[:, :, rows, :], prod_ref.at[:, :, rows, :], out_sems.at[group]
        )

    def step(n, carry):
        group = n + 2 - (n // 4) * (2 * n - 3)

        @pl.when(n == 4)
        def _():
            halo_wait(3)
            halo_wait(2)
            permute_batch(hraw, xf, 3, 0)
            permute_batch(hraw, xf, 2, 0)

        @pl.when(n == 5)
        def _():
            halo_wait(1)
            halo_wait(0)
            permute_batch(hraw, xf, 1, 0)
            permute_batch(hraw, xf, 0, 0)

        process_group(group, refs)
        out_copy(group).start()
        return carry

    lax.fori_loop(0, 6, step, 0)

    for q in range(12):
        for k1 in range(ROWS):
            at = q * per + k1 % per
            part[k1 // per, at : at + 1, :] = jnp.sum(
                sums[q, k1 * 8 : k1 * 8 + 8, :], axis=0, keepdims=True
            )

    def row_copy(d):
        other = lax.rem(member + d, members)
        return pltpu.make_async_remote_copy(
            src_ref=part.at[other],
            dst_ref=rows_in.at[d - 1],
            send_sem=row_send.at[d - 1],
            recv_sem=row_recv.at[d - 1],
            device_id=member_id(other, cores),
            device_id_type=MESH,
        )

    for d in range(1, members):
        row_copy(d).start()
    acc = part[member]
    for d in range(1, members):
        row_copy(d).wait_recv()
        acc = acc + rows_in[d - 1]
    mine[...] = acc

    def col_copy(d):
        return pltpu.make_async_remote_copy(
            src_ref=mine,
            dst_ref=cols_in.at[d - 1],
            send_sem=col_send.at[d - 1],
            recv_sem=col_recv.at[d - 1],
            device_id={"tm_0": lax.rem(column + d, columns)},
            device_id_type=MESH,
        )

    for d in range(1, columns):
        col_copy(d).start()
    for d in range(1, columns):
        col_copy(d).wait_recv()
        acc = acc + cols_in[d - 1]
    mean = acc * np.float32(1.0 / total)
    power = [mean[per * s : per * (s + 1)] for s in range(4)]
    coh = []
    for p in range(4):
        re = mean[per * (4 + p) : per * (5 + p)]
        im = mean[per * (8 + p) : per * (9 + p)]
        coh.append(
            (re * re + im * im) / ((power[p // 2] + 1e-06) * (power[2 + p % 2] + 1e-06))
        )
    stat[...] = jnp.concatenate(power + coh, axis=0)
    stats_ref[member] = stat[...]

    def gather_copy(d):
        return pltpu.make_async_remote_copy(
            src_ref=stat,
            dst_ref=stats_ref.at[member],
            send_sem=gat_send.at[d - 1],
            recv_sem=gat_recv.at[d - 1],
            device_id=member_id(lax.rem(member + d, members), cores),
            device_id_type=MESH,
        )

    for d in range(1, members):
        gather_copy(d).start()
    for d in range(1, members):
        gather_copy(d).wait_recv()

    @pl.when(has_next)
    def _():
        for b in range(4):
            halo_copy(b).wait_send()

    for d in range(1, members):
        row_copy(d).wait_send()
        gather_copy(d).wait_send()
    for d in range(1, columns):
        col_copy(d).wait_send()
    for group in range(6):
        out_copy(group).wait()


def transform_call(rows, taps_rows, total):
    frames = rows.shape[1] // 64
    consts = [jnp.asarray(c) for c in constants()]
    vmem = pl.BlockSpec(memory_space=pltpu.VMEM)
    anywhere = pl.BlockSpec(memory_space=pl.ANY)
    f32, bf16, i32 = jnp.float32, jnp.bfloat16, jnp.int32
    members = lax.axis_size(TM[1]) * lax.axis_size(TM[2])
    columns = lax.axis_size(TM[0])
    per = ROWS // members
    dma = pltpu.SemaphoreType.DMA
    return pl.pallas_call(
        functools.partial(transform_kernel, total),
        out_shape=(
            jax.ShapeDtypeStruct((2, 4, frames, 4096), f32),
            jax.ShapeDtypeStruct((members, 8 * per, LANES), f32),
        ),
        in_specs=[anywhere] + [vmem] * 5,
        out_specs=(anywhere, vmem),
        scratch_shapes=[
            pltpu.VMEM((4, frames * 64, LANES), i32),
            pltpu.VMEM((4, HALO * 64, LANES), i32),
            pltpu.VMEM((8, ROWS * PITCH + 7, LANES), f32),
            pltpu.VMEM((ROWS * 16 * 8, LANES), f32),
            pltpu.VMEM((1024, 256), bf16),
            pltpu.VMEM((1024, 256), bf16),
            pltpu.VMEM((1024, 256), f32),
            pltpu.VMEM((2, 1024, LANES), f32),
            pltpu.VMEM((2, 4, frames, 4096), f32),
            pltpu.VMEM((12, ROWS * 8, LANES), f32),
            pltpu.VMEM((members, 12 * per, LANES), f32),
            pltpu.VMEM((members - 1, 12 * per, LANES), f32),
            pltpu.VMEM((12 * per, LANES), f32),
            pltpu.VMEM((columns - 1, 12 * per, LANES), f32),
            pltpu.VMEM((8 * per, LANES), f32),
            dma((6,)),
            dma((12,)),
            dma((4,)),
            dma((4,)),
            dma((members - 1,)),
            dma((members - 1,)),
            dma((columns - 1,)),
            dma((columns - 1,)),
            dma((members - 1,)),
            dma((members - 1,)),
        ],
        compiler_params=pltpu.CompilerParams(
            vmem_limit_bytes=60 * 1024 * 1024, collective_id=0, has_side_effects=True
        ),
        cost_estimate=pl.CostEstimate(
            flops=4_000_000_000, bytes_accessed=16_000_000, transcendentals=0
        ),
        name="transform",
    )(rows, taps_rows, *consts)


def normalize_kernel(canon_ref, pairs_ref, stats_ref, prod_ref, coh_ref, out_ref):
    pair = pl.program_id(0)
    canon = canon_ref[pair]
    first = pairs_ref[pair, 0]
    second = pairs_ref[pair, 1]
    members = stats_ref.shape[0]
    per = ROWS // members
    for m in range(members):
        power = (stats_ref[m, pl.ds(first * per, per), :] + 1e-06) * (
            stats_ref[m, pl.ds(second * per, per), :] + 1e-06
        )
        factor = 1.0 / jnp.sqrt(power)
        for r in range(per):
            k1 = m * per + r
            cols = slice(k1 * LANES, (k1 + 1) * LANES)
            row = factor[r : r + 1]
            for part in range(2):
                out_ref[part, 0, :, cols] = prod_ref[part, 0, :, cols] * row

    @pl.when(pl.program_id(1) == 0)
    def _():
        for m in range(members):
            coh_ref[0, m * per : (m + 1) * per, :] = stats_ref[m, pl.ds((4 + canon) * per, per), :]


def normalize_call(pairs, stats, prods, block=24):
    frames = prods.shape[2]
    canon = pairs[:, 0] * 2 + pairs[:, 1] - 2
    f32 = jnp.float32
    coh, normalized = pl.pallas_call(
        normalize_kernel,
        grid_spec=pltpu.PrefetchScalarGridSpec(
            num_scalar_prefetch=2,
            grid=(4, frames // block),
            in_specs=[
                pl.BlockSpec(stats.shape, lambda p, b, canon, pairs: (0, 0, 0)),
                pl.BlockSpec((2, 1, block, 4096), lambda p, b, canon, pairs: (0, canon[p], b, 0)),
            ],
            out_specs=[
                pl.BlockSpec((1, ROWS, LANES), lambda p, b, canon, pairs: (p, 0, 0)),
                pl.BlockSpec((2, 1, block, 4096), lambda p, b, canon, pairs: (0, p, b, 0)),
            ],
        ),
        out_shape=(
            jax.ShapeDtypeStruct((4, ROWS, LANES), f32),
            jax.ShapeDtypeStruct(prods.shape, f32),
        ),
        cost_estimate=pl.CostEstimate(flops=2_000_000, bytes_accessed=13_000_000, transcendentals=0),
        name="normalize",
    )(canon, pairs, stats, prods)
    return coh.reshape(4, ROWS * LANES), normalized


def sample_rows(volts):
    streams, comps, local = volts.shape
    rows = volts.reshape(streams, comps, local // LANES, LANES)
    return jnp.transpose(rows, (0, 2, 1, 3)).reshape(streams, local // LANES * comps, LANES)


def tap_rows(taps):
    taps = taps.reshape(2, 8, ROWS, LANES)
    return jnp.transpose(taps, (0, 2, 1, 3)).reshape(512, LANES)


def on_device(volts, taps, pairs):
    rows = sample_rows(volts)
    total = rows.shape[1] // 64 * lax.axis_size(TM)
    prods, stats = transform_call(rows, tap_rows(taps), total)
    return normalize_call(pairs, stats, prods)


def solution(mesh):
    devices = mesh.devices
    finer = Mesh(
        devices.reshape(mesh.shape["band"], 8, 8, 2), ("band", "tm_0", "tm_1", "tm_2")
    )
    return jax.shard_map(
        on_device,
        mesh=finer,
        in_specs=(P("band", None, TM), P(), P()),
        out_specs=(P("band", None), P(None, "band", TM, None)),
        check_vma=False,
    )
```

```python
import functools
import math

import jax
import jax.numpy as jnp
import numpy as np
from jax import lax
from jax.experimental import pallas as pl
from jax.experimental.pallas import tpu as pltpu
from jax.sharding import Mesh
from jax.sharding import PartitionSpec as P

TM = ("tm_0", "tm_1", "tm_2")
ROWS = 32
LANES = 128
PITCH = 65
HALO = 16
GROUP = 8


def constants():
    lane = np.arange(LANES)
    j = 4 * (lane % 32) + lane // 32
    k = np.arange(LANES)
    angle = 2.0 * np.pi * ((j[:, None] * k[None, :]) % LANES) / LANES
    cos, sin = np.cos(angle) / 64.0, np.sin(angle) / 64.0
    full = np.block([[cos, -sin], [sin, cos]]).astype(np.float32)
    high = full.astype(jnp.bfloat16)
    low = (full - high.astype(np.float32)).astype(jnp.bfloat16)
    i = np.arange(ROWS)
    turn = 2.0 * np.pi * ((i[:, None] * k[None, :]) % 4096) / 4096
    return (
        high,
        low,
        np.cos(turn).astype(np.float32),
        np.sin(turn).astype(np.float32),
    )


def add(a, b):
    return (a[0] + b[0], a[1] + b[1])


def sub(a, b):
    return (a[0] - b[0], a[1] - b[1])


def fft4(x):
    a, b = add(x[0], x[2]), sub(x[0], x[2])
    c, d = add(x[1], x[3]), sub(x[1], x[3])
    return [
        add(a, c),
        (b[0] + d[1], b[1] - d[0]),
        sub(a, c),
        (b[0] - d[1], b[1] + d[0]),
    ]


def fft8(x):
    even = fft4(x[0::2])
    odd = fft4(x[1::2])
    r = np.float32(math.sqrt(0.5))
    turned = [
        odd[0],
        ((odd[1][0] + odd[1][1]) * r, (odd[1][1] - odd[1][0]) * r),
        (odd[2][1], -odd[2][0]),
        ((odd[3][1] - odd[3][0]) * r, (odd[3][0] + odd[3][1]) * -r),
    ]
    return [add(e, o) for e, o in zip(even, turned)] + [sub(e, o) for e, o in zip(even, turned)]


def rotate(x, index, length):
    index = index % length
    if index == 0:
        return x
    if index * 4 == length:
        return (x[1], -x[0])
    c = np.float32(math.cos(2 * math.pi * index / length))
    s = np.float32(math.sin(2 * math.pi * index / length))
    return (x[0] * c + x[1] * s, x[1] * c - x[0] * s)


def block_transpose(rows):
    turned = rows.T
    lane = lax.broadcasted_iota(jnp.int32, (32, LANES), 1)
    odd = (lane & 32) != 0
    upper = (lane & 64) != 0
    r = [turned[32 * b : 32 * b + 32] for b in range(4)]

    def pair(a, b, by, mask):
        return (
            jnp.where(mask, pltpu.roll(b, by, 1), a),
            jnp.where(mask, b, pltpu.roll(a, LANES - by, 1)),
        )

    a0, a1 = pair(r[0], r[1], 32, odd)
    b0, b1 = pair(r[2], r[3], 32, odd)
    o0, o2 = pair(a0, b0, 64, upper)
    o1, o3 = pair(a1, b1, 64, upper)
    return [o0, o1, o2, o3]


def permute_taps(taps_ref, tapb):
    def batch(tb, carry):
        high = tb // 2
        parts = [
            taps_ref[pl.ds(high * 256 + (tb % 2) * 4 + q, 32, stride=8), :] for q in range(4)
        ]
        out = block_transpose(jnp.concatenate(parts, axis=0))
        for q in range(4):
            for i in range(ROWS):
                tapb[pl.ds(pl.multiple_of((i * 16 + tb * 4 + q) * 8, 8), 8), :] = jnp.broadcast_to(
                    out[q][i : i + 1], (8, LANES)
                )
        return carry

    lax.fori_loop(0, 4, batch, 0)


def permute_batch(raw, xf, b, row0):
    for c in range(2):
        x = [raw[s, pl.ds(b * 256 + c, LANES, stride=2), :] for s in range(4)]
        packed = (
            (x[0] & 255) | ((x[1] & 255) << 8) | ((x[2] & 255) << 16) | (x[3] << 24)
        )
        out = block_transpose(packed)
        for q in range(4):
            for s in range(4):
                value = out[q] << (24 - 8 * s) if s < 3 else out[q]
                value = (value >> 24).astype(jnp.float32)
                xf[2 * s + c, pl.ds(row0 + 4 * b + q, 32, stride=PITCH), :] = value


def order_of(i):
    return lax.rem(i, 4) * 8 + i // 4


def fir(refs, first, groups, tap0, tap1, extend=False):
    (xf, tapb, y) = refs

    def body(i, carry):
        base = i * PITCH + HALO + first * GROUP
        place = order_of(i)
        tap = {
            t: tapb[pl.ds(pl.multiple_of((i * 16 + t) * 8, 8), 8), :] for t in range(tap0, tap1)
        }
        for c in range(2):
            cols = slice(c * LANES, (c + 1) * LANES)
            for s in range(4):
                at = [
                    pl.ds(pl.multiple_of((g * 128 + s * 32 + place) * 8, 8), 8)
                    for g in range(groups)
                ]
                acc = [y[at[g], cols] if extend else None for g in range(groups)]
                for w in range(1 - tap1, 8 * (groups - 1) - tap0 + 1):
                    users = [g for g in range(groups) if tap0 <= 8 * g - w < tap1]
                    if not users:
                        continue
                    x = xf[2 * s + c, pl.ds(base + w, 8), :]
                    for g in users:
                        term = tap[8 * g - w] * x
                        acc[g] = term if acc[g] is None else acc[g] + term
                for g in range(groups):
                    y[at[g], cols] = acc[g]
        return carry

    lax.fori_loop(0, ROWS, body, 0)


def transform(refs, group0, groups):
    (y, wh, wl, twc, tws, v, u, pbuf, sums) = refs

    def stage1(m, carry):
        at = pl.ds(pl.multiple_of(m * 512, 512), 512)
        x = y[at, :]
        h = x.astype(jnp.bfloat16)
        l = (x - h.astype(jnp.float32)).astype(jnp.bfloat16)
        dot = functools.partial(jnp.dot, preferred_element_type=jnp.float32)
        v[at, :] = dot(h, wh[...]) + dot(l, wh[...]) + dot(h, wl[...])
        return carry

    lax.fori_loop(0, 2 * groups, stage1, 0)

    def tile(n):
        return pl.ds(pl.multiple_of(n * 8, 8), 8)

    def stage2a(gs, carry):
        for i0 in range(4):
            xs = []
            for i1 in range(8):
                i = 4 * i1 + i0
                at = tile(gs * 32 + i0 * 8 + i1)
                x = (v[at, :LANES], v[at, LANES:])
                if i:
                    c = jnp.broadcast_to(twc[i : i + 1, :], (8, LANES))
                    d = jnp.broadcast_to(tws[i : i + 1, :], (8, LANES))
                    x = (x[0] * c + x[1] * d, x[1] * c - x[0] * d)
                xs.append(x)
            for ka, x in enumerate(fft8(xs)):
                x = rotate(x, i0 * ka, 32)
                at = tile(gs * 37 + i0 * 9 + ka)
                u[0, at, :] = x[0]
                u[1, at, :] = x[1]
        return carry

    lax.fori_loop(0, 4 * groups, stage2a, 0)

    def stage2b(n, carry):
        g = n // 8
        ka = lax.rem(n, 8)
        rows = tile(group0 + g)
        spectra = []
        for s in range(4):
            xs = []
            for i0 in range(4):
                at = tile((g * 4 + s) * 37 + i0 * 9 + ka)
                xs.append((u[0, at, :], u[1, at, :]))
            spectra.append(fft4(xs))
        for kb in range(4):
            k1 = ka + 8 * kb
            z = [spectra[s][kb] for s in range(4)]
            at = tile(k1)
            for s in range(4):
                sums[s, at, :] += z[s][0] * z[s][0] + z[s][1] * z[s][1]
            cols = pl.ds(pl.multiple_of(k1 * LANES, LANES), LANES)
            for p in range(4):
                a, b = z[p // 2], z[2 + p % 2]
                re = a[0] * b[0] + a[1] * b[1]
                im = a[1] * b[0] - a[0] * b[1]
                sums[4 + p, at, :] += re
                sums[8 + p, at, :] += im
                pbuf[0, p, rows, cols] = re
                pbuf[1, p, rows, cols] = im
        return carry

    lax.fori_loop(0, 8 * groups, stage2b, 0)


def peers():
    x_name, y_name, c_name = TM
    cores = lax.axis_size(c_name)
    members = lax.axis_size(y_name) * cores
    columns = lax.axis_size(x_name)
    member = lax.axis_index(y_name) * cores + lax.axis_index(c_name)
    return member, lax.axis_index(x_name), members, columns, cores


def member_id(member, cores):
    return {"tm_1": member // cores, "tm_2": lax.rem(member, cores)}


def transform_kernel(
    total, samples_ref, taps_ref, wh, wl, twc, tws, prod_ref, stats_ref,
    raw, hraw, xf, tapb, y, v, u, pbuf, sums, part, rows_in, mine, cols_in, stat,
    out_sems, in_sems, halo_send, halo_recv, row_send, row_recv, col_send, col_recv,
    gat_send, gat_recv,
):
    member, column, members, columns, cores = peers()
    per = ROWS // members
    count = members * columns
    place = column * members + member
    has_next = place < count - 1
    has_prev = place > 0
    MESH = pl.DeviceIdType.MESH

    def tm_id(index):
        return {"tm_0": index // members, **member_id(lax.rem(index, members), cores)}

    def in_copy(b):
        rows = pl.ds(pl.multiple_of(b * 256, 256), 256)
        return pltpu.make_async_copy(samples_ref.at[:, rows, :], raw.at[:, rows, :], in_sems.at[b])

    for b in range(12):
        in_copy(b).start()

    barrier = pltpu.get_barrier_semaphore()
    for d in range(1, members):
        other = lax.rem(member + d, members)
        pl.semaphore_signal(
            barrier, inc=1, device_id=member_id(other, cores), device_id_type=MESH
        )
    for d in range(1, columns):
        other = lax.rem(column + d, columns)
        pl.semaphore_signal(barrier, inc=1, device_id={"tm_0": other}, device_id_type=MESH)

    first_member = member == 0
    last_member = member == members - 1

    @pl.when(jnp.logical_and(first_member, has_prev))
    def _():
        pl.semaphore_signal(barrier, inc=1, device_id=tm_id(place - 1), device_id_type=MESH)

    greeted = members - 1 + columns - 1

    @pl.when(jnp.logical_and(last_member, has_next))
    def _():
        pl.semaphore_wait(barrier, greeted + 1)

    @pl.when(jnp.logical_not(jnp.logical_and(last_member, has_next)))
    def _():
        pl.semaphore_wait(barrier, greeted)

    frames = samples_ref.shape[1] // 64

    def halo_copy(b):
        lead = 1 if b == 0 else 0
        at = (4 * b + lead) * 64
        size = (4 - lead) * 64
        start = (frames - HALO) * 64 + at
        return pltpu.make_async_remote_copy(
            src_ref=samples_ref.at[:, pl.ds(start, size), :],
            dst_ref=hraw.at[:, pl.ds(at, size), :],
            send_sem=halo_send.at[b],
            recv_sem=halo_recv.at[b],
            device_id=tm_id(place + 1),
            device_id_type=MESH,
        )

    @pl.when(has_next)
    def _():
        for b in (3, 2, 1, 0):
            halo_copy(b).start()

    @pl.when(jnp.logical_not(has_prev))
    def _():
        hraw[...] = jnp.zeros_like(hraw)

    def halo_wait(b):
        @pl.when(has_prev)
        def _():
            halo_copy(b).wait_recv()

    filters = (xf, tapb, y)
    refs = (y, wh, wl, twc, tws, v, u, pbuf, sums)
    sums[...] = jnp.zeros_like(sums)
    permute_taps(taps_ref, tapb)

    def own_batch(b, carry):
        in_copy(b).wait()
        permute_batch(raw, xf, b, HALO)
        return carry

    lax.fori_loop(0, 12, own_batch, 0)

    def out_copy(n):
        rows = (pl.ds(0, 8), pl.ds(8, 8), pl.ds(16, frames - 16))[n]
        return pltpu.make_async_copy(
            pbuf.at[:, :, rows, pl.ds(0, 4096)], prod_ref.at[:, :, rows, :], out_sems.at[n]
        )

    fir(filters, 2, 4, 0, 16)
    transform(refs, 2, 4)
    out_copy(2).start()

    halo_wait(3)
    halo_wait(2)
    permute_batch(hraw, xf, 3, 0)
    permute_batch(hraw, xf, 2, 0)
    fir(filters, 1, 1, 0, 16)
    transform(refs, 1, 1)
    out_copy(1).start()

    halo_wait(1)
    permute_batch(hraw, xf, 1, 0)
    fir(filters, 0, 1, 0, 13)
    halo_wait(0)
    permute_batch(hraw, xf, 0, 0)
    fir(filters, 0, 1, 13, 16, extend=True)
    transform(refs, 0, 1)
    out_copy(0).start()

    for q in range(12):
        for k1 in range(ROWS):
            at = q * per + k1 % per
            part[k1 // per, at : at + 1, :] = jnp.sum(
                sums[q, k1 * 8 : k1 * 8 + 8, :], axis=0, keepdims=True
            )

    def row_copy(d):
        other = lax.rem(member + d, members)
        return pltpu.make_async_remote_copy(
            src_ref=part.at[other],
            dst_ref=rows_in.at[d - 1],
            send_sem=row_send.at[d - 1],
            recv_sem=row_recv.at[d - 1],
            device_id=member_id(other, cores),
            device_id_type=MESH,
        )

    for d in range(1, members):
        row_copy(d).start()
    acc = part[member]
    for d in range(1, members):
        row_copy(d).wait_recv()
        acc = acc + rows_in[d - 1]
    mine[...] = acc

    def col_copy(d):
        return pltpu.make_async_remote_copy(
            src_ref=mine,
            dst_ref=cols_in.at[d - 1],
            send_sem=col_send.at[d - 1],
            recv_sem=col_recv.at[d - 1],
            device_id={"tm_0": lax.rem(column + d, columns)},
            device_id_type=MESH,
        )

    for d in range(1, columns):
        col_copy(d).start()
    for d in range(1, columns):
        col_copy(d).wait_recv()
        acc = acc + cols_in[d - 1]
    mean = acc * np.float32(1.0 / total)
    power = [mean[per * s : per * (s + 1)] for s in range(4)]
    coh = []
    for p in range(4):
        re = mean[per * (4 + p) : per * (5 + p)]
        im = mean[per * (8 + p) : per * (9 + p)]
        coh.append(
            (re * re + im * im) / ((power[p // 2] + 1e-06) * (power[2 + p % 2] + 1e-06))
        )
    stat[...] = jnp.concatenate(power + coh, axis=0)
    stats_ref[member] = stat[...]

    def gather_copy(d):
        return pltpu.make_async_remote_copy(
            src_ref=stat,
            dst_ref=stats_ref.at[member],
            send_sem=gat_send.at[d - 1],
            recv_sem=gat_recv.at[d - 1],
            device_id=member_id(lax.rem(member + d, members), cores),
            device_id_type=MESH,
        )

    for d in range(1, members):
        gather_copy(d).start()
    for d in range(1, members):
        gather_copy(d).wait_recv()

    @pl.when(has_next)
    def _():
        for b in range(4):
            halo_copy(b).wait_send()

    for d in range(1, members):
        row_copy(d).wait_send()
        gather_copy(d).wait_send()
    for d in range(1, columns):
        col_copy(d).wait_send()
    for n in range(3):
        out_copy(n).wait()


def transform_call(rows, taps_rows, total):
    frames = rows.shape[1] // 64
    consts = [jnp.asarray(c) for c in constants()]
    vmem = pl.BlockSpec(memory_space=pltpu.VMEM)
    anywhere = pl.BlockSpec(memory_space=pl.ANY)
    f32, i32 = jnp.float32, jnp.int32
    members = lax.axis_size(TM[1]) * lax.axis_size(TM[2])
    columns = lax.axis_size(TM[0])
    per = ROWS // members
    dma = pltpu.SemaphoreType.DMA
    return pl.pallas_call(
        functools.partial(transform_kernel, total),
        out_shape=(
            jax.ShapeDtypeStruct((2, 4, frames, 4096), f32),
            jax.ShapeDtypeStruct((members, 8 * per, LANES), f32),
        ),
        in_specs=[anywhere] + [vmem] * 5,
        out_specs=(anywhere, vmem),
        scratch_shapes=[
            pltpu.VMEM((4, frames * 64, LANES), i32),
            pltpu.VMEM((4, HALO * 64, LANES), i32),
            pltpu.VMEM((8, ROWS * PITCH + 7, LANES), f32),
            pltpu.VMEM((ROWS * 16 * 8, LANES), f32),
            pltpu.VMEM((4096, 256), f32),
            pltpu.VMEM((4096, 256), f32),
            pltpu.VMEM((2, 16 * 37 * 8 + 16, LANES), f32),
            pltpu.VMEM((2, 4, frames, 4096 + LANES), f32),
            pltpu.VMEM((12, (ROWS + 1) * 8, LANES), f32),
            pltpu.VMEM((members, 12 * per, LANES), f32),
            pltpu.VMEM((members - 1, 12 * per, LANES), f32),
            pltpu.VMEM((12 * per, LANES), f32),
            pltpu.VMEM((columns - 1, 12 * per, LANES), f32),
            pltpu.VMEM((8 * per, LANES), f32),
            dma((3,)),
            dma((12,)),
            dma((4,)),
            dma((4,)),
            dma((members - 1,)),
            dma((members - 1,)),
            dma((columns - 1,)),
            dma((columns - 1,)),
            dma((members - 1,)),
            dma((members - 1,)),
        ],
        compiler_params=pltpu.CompilerParams(
            vmem_limit_bytes=60 * 1024 * 1024, collective_id=0, has_side_effects=True
        ),
        cost_estimate=pl.CostEstimate(
            flops=4_000_000_000, bytes_accessed=16_000_000, transcendentals=0
        ),
        name="transform",
    )(rows, taps_rows, *consts)


def normalize_kernel(stats_per, pairs_ref, stats_ref, prod_ref, coh_ref, out_ref):
    pair = pl.program_id(0)
    first = pairs_ref[0, pair]
    second = pairs_ref[1, pair]
    per = stats_per
    members = ROWS // per

    def stat(q, r):
        return stats_ref[pl.ds(q * per + r, members, stride=8 * per), :]

    for r in range(per):
        power = (stat(first, r) + 1e-06) * (stat(second, r) + 1e-06)
        factor = 1.0 / jnp.sqrt(power)
        for m in range(members):
            k1 = m * per + r
            cols = slice(k1 * LANES, (k1 + 1) * LANES)
            row = factor[m : m + 1]
            for part in range(2):
                out_ref[part, 0, :, cols] = prod_ref[part, 0, :, cols] * row

    @pl.when(jnp.logical_and(pair == 0, pl.program_id(1) == 0))
    def _():
        for p in range(4):
            which = pairs_ref[0, p] * 2 + pairs_ref[1, p] - 2
            for r in range(per):
                value = stat(4 + which, r)
                for m in range(members):
                    k1 = m * per + r
                    coh_ref[p : p + 1, k1 * LANES : (k1 + 1) * LANES] = value[m : m + 1]


def normalize_call(pairs, stats, prods, block=24):
    frames = prods.shape[2]
    f32 = jnp.float32
    table = stats.reshape(-1, LANES)
    return pl.pallas_call(
        functools.partial(normalize_kernel, stats.shape[1] // 8),
        grid_spec=pltpu.PrefetchScalarGridSpec(
            num_scalar_prefetch=1,
            grid=(4, frames // block),
            in_specs=[
                pl.BlockSpec(table.shape, lambda p, b, pairs: (0, 0)),
                pl.BlockSpec(
                    (2, 1, block, 4096),
                    lambda p, b, pairs: (0, pairs[0, p] * 2 + pairs[1, p] - 2, b, 0),
                ),
            ],
            out_specs=[
                pl.BlockSpec((4, 4096), lambda p, b, pairs: (0, 0)),
                pl.BlockSpec((2, 1, block, 4096), lambda p, b, pairs: (0, p, b, 0)),
            ],
        ),
        out_shape=(
            jax.ShapeDtypeStruct((4, 4096), f32),
            jax.ShapeDtypeStruct(prods.shape, f32),
        ),
        cost_estimate=pl.CostEstimate(flops=2_000_000, bytes_accessed=13_000_000, transcendentals=0),
        name="normalize",
    )(pairs.T, table, prods)


def sample_rows(volts):
    streams, comps, local = volts.shape
    rows = volts.reshape(streams, comps, local // LANES, LANES)
    return jnp.transpose(rows, (0, 2, 1, 3)).reshape(streams, local // LANES * comps, LANES)


def tap_rows(taps):
    taps = taps.reshape(2, 8, ROWS, LANES)
    return jnp.transpose(taps, (0, 2, 1, 3)).reshape(512, LANES)


def on_device(volts, taps, pairs):
    rows = sample_rows(volts)
    total = rows.shape[1] // 64 * lax.axis_size(TM)
    prods, stats = transform_call(rows, tap_rows(taps), total)
    return normalize_call(pairs, stats, prods)


def solution(mesh):
    devices = mesh.devices
    finer = Mesh(
        devices.reshape(mesh.shape["band"], 8, 8, 2), ("band", "tm_0", "tm_1", "tm_2")
    )
    return jax.shard_map(
        on_device,
        mesh=finer,
        in_specs=(P("band", None, TM), P(), P()),
        out_specs=(P("band", None), P(None, "band", TM, None)),
        check_vma=False,
    )
```

```python
import functools
import math

import jax
import jax.numpy as jnp
import numpy as np
from jax import lax
from jax.experimental import pallas as pl
from jax.experimental.pallas import tpu as pltpu
from jax.sharding import Mesh
from jax.sharding import PartitionSpec as P

TM = ("tm_0", "tm_1", "tm_2")
ROWS = 32
LANES = 128
PITCH = 65
HALO = 16
GROUP = 8


def constants():
    lane = np.arange(LANES)
    j = 4 * (lane % 32) + lane // 32
    k = np.arange(LANES)
    angle = 2.0 * np.pi * ((j[:, None] * k[None, :]) % LANES) / LANES
    cos, sin = np.cos(angle) / 64.0, np.sin(angle) / 64.0
    full = np.block([[cos, -sin], [sin, cos]]).astype(np.float32)
    high = full.astype(jnp.bfloat16)
    low = (full - high.astype(np.float32)).astype(jnp.bfloat16)
    i = np.arange(ROWS)
    turn = 2.0 * np.pi * ((i[:, None] * k[None, :]) % 4096) / 4096
    return (
        high,
        low,
        np.cos(turn).astype(np.float32),
        np.sin(turn).astype(np.float32),
    )


def add(a, b):
    return (a[0] + b[0], a[1] + b[1])


def sub(a, b):
    return (a[0] - b[0], a[1] - b[1])


def fft4(x):
    a, b = add(x[0], x[2]), sub(x[0], x[2])
    c, d = add(x[1], x[3]), sub(x[1], x[3])
    return [
        add(a, c),
        (b[0] + d[1], b[1] - d[0]),
        sub(a, c),
        (b[0] - d[1], b[1] + d[0]),
    ]


def fft8(x):
    even = fft4(x[0::2])
    odd = fft4(x[1::2])
    r = np.float32(math.sqrt(0.5))
    turned = [
        odd[0],
        ((odd[1][0] + odd[1][1]) * r, (odd[1][1] - odd[1][0]) * r),
        (odd[2][1], -odd[2][0]),
        ((odd[3][1] - odd[3][0]) * r, (odd[3][0] + odd[3][1]) * -r),
    ]
    return [add(e, o) for e, o in zip(even, turned)] + [sub(e, o) for e, o in zip(even, turned)]


def rotate(x, index, length):
    index = index % length
    if index == 0:
        return x
    if index * 4 == length:
        return (x[1], -x[0])
    c = np.float32(math.cos(2 * math.pi * index / length))
    s = np.float32(math.sin(2 * math.pi * index / length))
    return (x[0] * c + x[1] * s, x[1] * c - x[0] * s)


def block_transpose(rows):
    turned = rows.T
    lane = lax.broadcasted_iota(jnp.int32, (32, LANES), 1)
    odd = (lane & 32) != 0
    upper = (lane & 64) != 0
    r = [turned[32 * b : 32 * b + 32] for b in range(4)]

    def pair(a, b, by, mask):
        return (
            jnp.where(mask, pltpu.roll(b, by, 1), a),
            jnp.where(mask, b, pltpu.roll(a, LANES - by, 1)),
        )

    a0, a1 = pair(r[0], r[1], 32, odd)
    b0, b1 = pair(r[2], r[3], 32, odd)
    o0, o2 = pair(a0, b0, 64, upper)
    o1, o3 = pair(a1, b1, 64, upper)
    return [o0, o1, o2, o3]


def permute_taps(taps_ref, tapb):
    def batch(tb, carry):
        high = tb // 2
        parts = [
            taps_ref[pl.ds(high * 256 + (tb % 2) * 4 + q, 32, stride=8), :] for q in range(4)
        ]
        out = block_transpose(jnp.concatenate(parts, axis=0))
        for q in range(4):
            for i in range(ROWS):
                tapb[pl.ds(pl.multiple_of((i * 16 + tb * 4 + q) * 8, 8), 8), :] = jnp.broadcast_to(
                    out[q][i : i + 1], (8, LANES)
                )
        return carry

    lax.fori_loop(0, 4, batch, 0)


def permute_batch(raw, xf, b, row0):
    for c in range(2):
        x = [raw[s, pl.ds(b * 256 + c, LANES, stride=2), :] for s in range(4)]
        packed = (
            (x[0] & 255) | ((x[1] & 255) << 8) | ((x[2] & 255) << 16) | (x[3] << 24)
        )
        out = block_transpose(packed)
        for q in range(4):
            for s in range(4):
                value = out[q] << (24 - 8 * s) if s < 3 else out[q]
                value = (value >> 24).astype(jnp.float32)
                xf[2 * s + c, pl.ds(row0 + 4 * b + q, 32, stride=PITCH), :] = value


def order_of(i):
    return lax.rem(i, 4) * 8 + i // 4


def fir(refs, first, groups, tap0, tap1, extend=False):
    (xf, tapb, y) = refs

    def body(i, carry):
        base = i * PITCH + HALO + first * GROUP
        place = order_of(i)
        tap = {
            t: tapb[pl.ds(pl.multiple_of((i * 16 + t) * 8, 8), 8), :] for t in range(tap0, tap1)
        }
        for c in range(2):
            cols = slice(c * LANES, (c + 1) * LANES)
            for s in range(4):
                at = [
                    pl.ds(pl.multiple_of((g * 128 + s * 32 + place) * 8, 8), 8)
                    for g in range(groups)
                ]
                acc = [y[at[g], cols] if extend else None for g in range(groups)]
                for w in range(1 - tap1, 8 * (groups - 1) - tap0 + 1):
                    users = [g for g in range(groups) if tap0 <= 8 * g - w < tap1]
                    if not users:
                        continue
                    x = xf[2 * s + c, pl.ds(base + w, 8), :]
                    for g in users:
                        term = tap[8 * g - w] * x
                        acc[g] = term if acc[g] is None else acc[g] + term
                for g in range(groups):
                    y[at[g], cols] = acc[g]
        return carry

    lax.fori_loop(0, ROWS, body, 0)


def transform(refs, group0, groups):
    (y, wh, wl, twc, tws, v, u, pbuf, sums) = refs

    def stage1(m, carry):
        at = pl.ds(pl.multiple_of(m * 512, 512), 512)
        x = y[at, :]
        h = x.astype(jnp.bfloat16)
        l = (x - h.astype(jnp.float32)).astype(jnp.bfloat16)
        dot = functools.partial(jnp.dot, preferred_element_type=jnp.float32)
        v[at, :] = dot(h, wh[...]) + dot(l, wh[...]) + dot(h, wl[...])
        return carry

    lax.fori_loop(0, 2 * groups, stage1, 0)

    def tile(n):
        return pl.ds(pl.multiple_of(n * 8, 8), 8)

    def stage2a(gs, carry):
        for i0 in range(4):
            xs = []
            for i1 in range(8):
                i = 4 * i1 + i0
                at = tile(gs * 32 + i0 * 8 + i1)
                x = (v[at, :LANES], v[at, LANES:])
                if i:
                    c = jnp.broadcast_to(twc[i : i + 1, :], (8, LANES))
                    d = jnp.broadcast_to(tws[i : i + 1, :], (8, LANES))
                    x = (x[0] * c + x[1] * d, x[1] * c - x[0] * d)
                xs.append(x)
            for ka, x in enumerate(fft8(xs)):
                x = rotate(x, i0 * ka, 32)
                at = tile(gs * 37 + i0 * 9 + ka)
                u[0, at, :] = x[0]
                u[1, at, :] = x[1]
        return carry

    lax.fori_loop(0, 4 * groups, stage2a, 0)

    def stage2b(n, carry):
        g = n // 8
        ka = lax.rem(n, 8)
        rows = tile(group0 + g)
        spectra = []
        for s in range(4):
            xs = []
            for i0 in range(4):
                at = tile((g * 4 + s) * 37 + i0 * 9 + ka)
                xs.append((u[0, at, :], u[1, at, :]))
            spectra.append(fft4(xs))
        for kb in range(4):
            k1 = ka + 8 * kb
            z = [spectra[s][kb] for s in range(4)]
            at = tile(k1)
            for s in range(4):
                sums[s, at, :] += z[s][0] * z[s][0] + z[s][1] * z[s][1]
            cols = pl.ds(pl.multiple_of(k1 * LANES, LANES), LANES)
            for p in range(4):
                a, b = z[p // 2], z[2 + p % 2]
                re = a[0] * b[0] + a[1] * b[1]
                im = a[1] * b[0] - a[0] * b[1]
                sums[4 + p, at, :] += re
                sums[8 + p, at, :] += im
                pbuf[0, p, rows, cols] = re
                pbuf[1, p, rows, cols] = im
        return carry

    lax.fori_loop(0, 8 * groups, stage2b, 0)


HALF = ROWS // 2


class Ring:
    def __init__(self, half, a, b):
        self.half, self.a, self.b, self.c = half, a, b, TM[2]
        self.na, self.nb, self.nc = (lax.axis_size(n) for n in (a, b, self.c))
        self.members = self.na * self.nc
        self.per = HALF // self.members
        far = sorted(range(self.na), key=lambda d: -min(d, self.na - d))
        self.steps = [(d, e) for d in far for e in range(self.nc) if (d, e) != (0, 0)]
        self.shifts = sorted(range(1, self.nb), key=lambda d: -min(d, self.nb - d))

    def member(self, d=0, e=0):
        at = lax.rem(lax.axis_index(self.a) + d, self.na)
        core = lax.rem(lax.axis_index(self.c) + e, self.nc)
        return at * self.nc + core

    def member_id(self, d, e):
        return {
            self.a: lax.rem(lax.axis_index(self.a) + d, self.na),
            self.c: lax.rem(lax.axis_index(self.c) + e, self.nc),
        }

    def column_id(self, d):
        return {self.b: lax.rem(lax.axis_index(self.b) + d, self.nb)}


def rings():
    return (Ring(0, TM[1], TM[0]), Ring(1, TM[0], TM[1]))


def remote(src, dst, send, recv, to):
    return pltpu.make_async_remote_copy(
        src_ref=src,
        dst_ref=dst,
        send_sem=send,
        recv_sem=recv,
        device_id=to,
        device_id_type=pl.DeviceIdType.MESH,
    )


def all_reduce(total, sums, stats_ref, scratch):
    both = rings()
    work = []
    for ring in both:
        part, rows_in, mine, cols_in, stat, sems = scratch[ring.half]
        work.append((ring, part, rows_in, mine, cols_in, stat, sems))

    def row_copy(job, n):
        ring, part, rows_in, _, _, _, sems = job
        d, e = ring.steps[n]
        return remote(
            part.at[ring.member(d, e)], rows_in.at[n], sems.at[0, n], sems.at[1, n],
            ring.member_id(d, e),
        )

    def col_copy(job, n):
        ring, _, _, mine, cols_in, _, sems = job
        return remote(
            mine, cols_in.at[n], sems.at[2, n], sems.at[3, n], ring.column_id(ring.shifts[n])
        )

    def place(ring):
        return pl.ds(HALF * ring.half + ring.member() * ring.per, ring.per)

    def gather_copy(job, n):
        ring, _, _, _, _, stat, sems = job
        return remote(
            stat, stats_ref.at[place(ring)], sems.at[4, n], sems.at[5, n],
            ring.member_id(*ring.steps[n]),
        )

    for job in work:
        ring, part = job[:2]
        for k in range(HALF):
            k1 = HALF * ring.half + k
            for j in range(3):
                part[k // ring.per, k % ring.per, j] = jnp.concatenate(
                    [
                        jnp.sum(sums[4 * j + q, k1 * 8 : k1 * 8 + 8, :], axis=0, keepdims=True)
                        for q in range(4)
                    ],
                    axis=0,
                )
        for n in range(len(ring.steps)):
            row_copy(job, n).start()

    totals = []
    for job in work:
        ring, part, rows_in, mine = job[:4]
        acc = part[ring.member()]
        for n in reversed(range(len(ring.steps))):
            row_copy(job, n).wait_recv()
            acc = acc + rows_in[n]
        mine[...] = acc
        for n in range(len(ring.shifts)):
            col_copy(job, n).start()
        totals.append(acc)

    for job, acc in zip(work, totals):
        ring, _, _, _, cols_in, stat, _ = job
        for n in reversed(range(len(ring.shifts))):
            col_copy(job, n).wait_recv()
            acc = acc + cols_in[n]
        mean = acc * np.float32(1.0 / total)
        for r in range(ring.per):
            power, re, im = mean[r, 0], mean[r, 1], mean[r, 2]
            raised = power + 1e-06
            denom = jnp.concatenate(
                [raised[p // 2 : p // 2 + 1] * raised[2 + p % 2 : 3 + p % 2] for p in range(4)],
                axis=0,
            )
            stat[r, 0] = power
            stat[r, 1] = (re * re + im * im) / denom
        for n in range(len(ring.steps)):
            gather_copy(job, n).start()
        stats_ref[place(ring)] = stat[...]

    for job in work:
        ring = job[0]
        for n in reversed(range(len(ring.steps))):
            gather_copy(job, n).wait_recv()
    for job in work:
        ring = job[0]
        for n in range(len(ring.steps)):
            row_copy(job, n).wait_send()
            gather_copy(job, n).wait_send()
        for n in range(len(ring.shifts)):
            col_copy(job, n).wait_send()


def transform_kernel(
    total, samples_ref, taps_ref, wh, wl, twc, tws, prod_ref, stats_ref,
    raw, hraw, xf, tapb, y, v, u, pbuf, sums,
    part0, rows0, mine0, cols0, stat0, sems0, part1, rows1, mine1, cols1, stat1, sems1,
    out_sems, in_sems, halo_send, halo_recv,
):
    MESH = pl.DeviceIdType.MESH
    x_name, y_name, c_name = TM
    nx, ny, nc = (lax.axis_size(n) for n in TM)
    me = [lax.axis_index(n) for n in TM]
    place = (me[0] * ny + me[1]) * nc + me[2]
    has_next = place < nx * ny * nc - 1
    has_prev = place > 0

    def tm_id(index):
        return {
            x_name: index // (ny * nc),
            y_name: lax.rem(index // nc, ny),
            c_name: lax.rem(index, nc),
        }

    barrier = pltpu.get_barrier_semaphore()
    greeted = 0
    for ring in rings():
        for d, e in ring.steps:
            if ring.half == 1 and d == 0:
                continue
            pl.semaphore_signal(
                barrier, inc=1, device_id=ring.member_id(d, e), device_id_type=MESH
            )
            greeted += 1
    row_start = jnp.logical_and(me[1] == 0, me[2] == 0)
    row_end = jnp.logical_and(me[1] == ny - 1, me[2] == nc - 1)

    @pl.when(jnp.logical_and(row_start, has_prev))
    def _():
        pl.semaphore_signal(barrier, inc=1, device_id=tm_id(place - 1), device_id_type=MESH)

    def in_copy(b):
        rows = pl.ds(pl.multiple_of(b * 256, 256), 256)
        return pltpu.make_async_copy(samples_ref.at[:, rows, :], raw.at[:, rows, :], in_sems.at[b])

    for b in range(12):
        in_copy(b).start()

    more = jnp.logical_and(row_end, has_next)

    @pl.when(more)
    def _():
        pl.semaphore_wait(barrier, greeted + 1)

    @pl.when(jnp.logical_not(more))
    def _():
        pl.semaphore_wait(barrier, greeted)

    frames = samples_ref.shape[1] // 64

    def halo_copy(b):
        lead = 1 if b == 0 else 0
        at = (4 * b + lead) * 64
        size = (4 - lead) * 64
        start = (frames - HALO) * 64 + at
        return remote(
            samples_ref.at[:, pl.ds(start, size), :], hraw.at[:, pl.ds(at, size), :],
            halo_send.at[b], halo_recv.at[b], tm_id(place + 1),
        )

    @pl.when(has_next)
    def _():
        for b in (3, 2, 1, 0):
            halo_copy(b).start()

    @pl.when(jnp.logical_not(has_prev))
    def _():
        hraw[...] = jnp.zeros_like(hraw)

    def halo_wait(b):
        @pl.when(has_prev)
        def _():
            halo_copy(b).wait_recv()

    filters = (xf, tapb, y)
    refs = (y, wh, wl, twc, tws, v, u, pbuf, sums)
    sums[...] = jnp.zeros_like(sums)
    permute_taps(taps_ref, tapb)

    def own_batch(b, carry):
        in_copy(b).wait()
        permute_batch(raw, xf, b, HALO)
        return carry

    lax.fori_loop(0, 12, own_batch, 0)

    def out_copy(n):
        rows = (pl.ds(0, 8), pl.ds(8, 8), pl.ds(16, frames - 16))[n]
        return pltpu.make_async_copy(
            pbuf.at[:, :, rows, pl.ds(0, 4096)], prod_ref.at[:, :, rows, :], out_sems.at[n]
        )

    fir(filters, 2, 4, 0, 16)
    transform(refs, 2, 4)
    out_copy(2).start()

    halo_wait(3)
    halo_wait(2)
    permute_batch(hraw, xf, 3, 0)
    permute_batch(hraw, xf, 2, 0)
    fir(filters, 1, 1, 0, 16)
    transform(refs, 1, 1)
    out_copy(1).start()

    halo_wait(1)
    permute_batch(hraw, xf, 1, 0)
    fir(filters, 0, 1, 0, 13)
    halo_wait(0)
    permute_batch(hraw, xf, 0, 0)
    fir(filters, 0, 1, 13, 16, extend=True)
    transform(refs, 0, 1)
    out_copy(0).start()

    all_reduce(
        total, sums, stats_ref,
        (
            (part0, rows0, mine0, cols0, stat0, sems0),
            (part1, rows1, mine1, cols1, stat1, sems1),
        ),
    )

    @pl.when(has_next)
    def _():
        for b in range(4):
            halo_copy(b).wait_send()

    for n in range(3):
        out_copy(n).wait()


def transform_call(rows, taps_rows, total):
    frames = rows.shape[1] // 64
    consts = [jnp.asarray(c) for c in constants()]
    vmem = pl.BlockSpec(memory_space=pltpu.VMEM)
    anywhere = pl.BlockSpec(memory_space=pl.ANY)
    f32, i32 = jnp.float32, jnp.int32
    dma = pltpu.SemaphoreType.DMA
    exchange = []
    for ring in rings():
        exchange += [
            pltpu.VMEM((ring.members, ring.per, 3, 4, LANES), f32),
            pltpu.VMEM((ring.members - 1, ring.per, 3, 4, LANES), f32),
            pltpu.VMEM((ring.per, 3, 4, LANES), f32),
            pltpu.VMEM((max(ring.nb - 1, 1), ring.per, 3, 4, LANES), f32),
            pltpu.VMEM((ring.per, 2, 4, LANES), f32),
            dma((6, max(ring.members, ring.nb) - 1)),
        ]
    return pl.pallas_call(
        functools.partial(transform_kernel, total),
        out_shape=(
            jax.ShapeDtypeStruct((2, 4, frames, 4096), f32),
            jax.ShapeDtypeStruct((ROWS, 2, 4, LANES), f32),
        ),
        in_specs=[anywhere] + [vmem] * 5,
        out_specs=(anywhere, vmem),
        scratch_shapes=[
            pltpu.VMEM((4, frames * 64, LANES), i32),
            pltpu.VMEM((4, HALO * 64, LANES), i32),
            pltpu.VMEM((8, ROWS * PITCH + 7, LANES), f32),
            pltpu.VMEM((ROWS * 16 * 8, LANES), f32),
            pltpu.VMEM((4096, 256), f32),
            pltpu.VMEM((4096, 256), f32),
            pltpu.VMEM((2, 16 * 37 * 8 + 16, LANES), f32),
            pltpu.VMEM((2, 4, frames, 4096 + LANES), f32),
            pltpu.VMEM((12, (ROWS + 1) * 8, LANES), f32),
            *exchange,
            dma((3,)),
            dma((12,)),
            dma((4,)),
            dma((4,)),
        ],
        compiler_params=pltpu.CompilerParams(
            vmem_limit_bytes=60 * 1024 * 1024, collective_id=0, has_side_effects=True
        ),
        cost_estimate=pl.CostEstimate(
            flops=4_000_000_000, bytes_accessed=16_000_000, transcendentals=0
        ),
        name="transform",
    )(rows, taps_rows, *consts)


def normalize_kernel(pairs_ref, stats_ref, prod_ref, coh_ref, out_ref, buf, factors, reads, writes):
    def which(p):
        return pairs_ref[0, p] * 2 + pairs_ref[1, p] - 2

    def read(n):
        p, part = n // 2, lax.rem(n, 2)
        return pltpu.make_async_copy(prod_ref.at[part, which(p)], buf.at[n], reads.at[n])

    def write(n):
        p, part = n // 2, lax.rem(n, 2)
        return pltpu.make_async_copy(buf.at[n], out_ref.at[part, p], writes.at[n])

    for n in range(8):
        read(n).start()

    def stat(q):
        return stats_ref[pl.ds(q, ROWS, stride=8), :]

    for p in range(4):
        power = (stat(pairs_ref[0, p]) + 1e-06) * (stat(pairs_ref[1, p]) + 1e-06)
        factors[p * ROWS : (p + 1) * ROWS, :] = 1.0 / jnp.sqrt(power)
        value = stat(4 + which(p))
        for k1 in range(ROWS):
            coh_ref[p : p + 1, k1 * LANES : (k1 + 1) * LANES] = value[k1 : k1 + 1]

    def chunk(n, carry):
        read(n).wait()
        p = n // 2
        factor = factors[pl.ds(pl.multiple_of(p * ROWS, ROWS), ROWS), :]
        for k1 in range(ROWS):
            cols = slice(k1 * LANES, (k1 + 1) * LANES)
            buf[n, :, cols] = buf[n, :, cols] * factor[k1 : k1 + 1]
        write(n).start()
        return carry

    lax.fori_loop(0, 8, chunk, 0)
    for n in range(8):
        write(n).wait()


def normalize_call(pairs, stats, prods):
    frames = prods.shape[2]
    f32 = jnp.float32
    table = stats.reshape(-1, LANES)
    vmem = pl.BlockSpec(memory_space=pltpu.VMEM)
    anywhere = pl.BlockSpec(memory_space=pl.ANY)
    return pl.pallas_call(
        normalize_kernel,
        in_specs=[pl.BlockSpec(memory_space=pltpu.SMEM), vmem, anywhere],
        out_specs=(vmem, anywhere),
        out_shape=(
            jax.ShapeDtypeStruct((4, 4096), f32),
            jax.ShapeDtypeStruct(prods.shape, f32),
        ),
        scratch_shapes=[
            pltpu.VMEM((8, frames, 4096), f32),
            pltpu.VMEM((4 * ROWS, LANES), f32),
            pltpu.SemaphoreType.DMA((8,)),
            pltpu.SemaphoreType.DMA((8,)),
        ],
        compiler_params=pltpu.CompilerParams(vmem_limit_bytes=60 * 1024 * 1024),
        cost_estimate=pl.CostEstimate(flops=2_000_000, bytes_accessed=13_000_000, transcendentals=0),
        name="normalize",
    )(pairs.T, table, prods)


def sample_rows(volts):
    streams, comps, local = volts.shape
    rows = volts.reshape(streams, comps, local // LANES, LANES)
    return jnp.transpose(rows, (0, 2, 1, 3)).reshape(streams, local // LANES * comps, LANES)


def tap_rows(taps):
    taps = taps.reshape(2, 8, ROWS, LANES)
    return jnp.transpose(taps, (0, 2, 1, 3)).reshape(512, LANES)


def on_device(volts, taps, pairs):
    rows = sample_rows(volts)
    total = rows.shape[1] // 64 * lax.axis_size(TM)
    prods, stats = transform_call(rows, tap_rows(taps), total)
    return normalize_call(pairs, stats, prods)


def solution(mesh):
    devices = mesh.devices
    finer = Mesh(
        devices.reshape(mesh.shape["band"], 8, 8, 2), ("band", "tm_0", "tm_1", "tm_2")
    )
    return jax.shard_map(
        on_device,
        mesh=finer,
        in_specs=(P("band", None, TM), P(), P()),
        out_specs=(P("band", None), P(None, "band", TM, None)),
        check_vma=False,
    )
```

```python
import functools
import math

import jax
import jax.numpy as jnp
import numpy as np
from jax import lax
from jax.experimental import pallas as pl
from jax.experimental.pallas import tpu as pltpu
from jax.sharding import Mesh
from jax.sharding import PartitionSpec as P

TM = ("tm_0", "tm_1", "tm_2")
ROWS = 32
LANES = 128
PITCH = 65
HALO = 16
GROUP = 8


def constants():
    lane = np.arange(LANES)
    j = 4 * (lane % 32) + lane // 32
    k = np.arange(LANES)
    angle = 2.0 * np.pi * ((j[:, None] * k[None, :]) % LANES) / LANES
    cos, sin = np.cos(angle) / 64.0, np.sin(angle) / 64.0
    full = np.block([[cos, -sin], [sin, cos]]).astype(np.float32)
    high = full.astype(jnp.bfloat16)
    low = (full - high.astype(np.float32)).astype(jnp.bfloat16)
    i = np.arange(ROWS)
    turn = 2.0 * np.pi * ((i[:, None] * k[None, :]) % 4096) / 4096
    return (
        high,
        low,
        np.cos(turn).astype(np.float32),
        np.sin(turn).astype(np.float32),
    )


def add(a, b):
    return (a[0] + b[0], a[1] + b[1])


def sub(a, b):
    return (a[0] - b[0], a[1] - b[1])


def fft4(x):
    a, b = add(x[0], x[2]), sub(x[0], x[2])
    c, d = add(x[1], x[3]), sub(x[1], x[3])
    return [
        add(a, c),
        (b[0] + d[1], b[1] - d[0]),
        sub(a, c),
        (b[0] - d[1], b[1] + d[0]),
    ]


def fft8(x):
    even = fft4(x[0::2])
    odd = fft4(x[1::2])
    r = np.float32(math.sqrt(0.5))
    turned = [
        odd[0],
        ((odd[1][0] + odd[1][1]) * r, (odd[1][1] - odd[1][0]) * r),
        (odd[2][1], -odd[2][0]),
        ((odd[3][1] - odd[3][0]) * r, (odd[3][0] + odd[3][1]) * -r),
    ]
    return [add(e, o) for e, o in zip(even, turned)] + [sub(e, o) for e, o in zip(even, turned)]


def rotate(x, index, length):
    index = index % length
    if index == 0:
        return x
    if index * 4 == length:
        return (x[1], -x[0])
    c = np.float32(math.cos(2 * math.pi * index / length))
    s = np.float32(math.sin(2 * math.pi * index / length))
    return (x[0] * c + x[1] * s, x[1] * c - x[0] * s)


def block_transpose(rows):
    turned = rows.T
    lane = lax.broadcasted_iota(jnp.int32, (32, LANES), 1)
    odd = (lane & 32) != 0
    upper = (lane & 64) != 0
    r = [turned[32 * b : 32 * b + 32] for b in range(4)]

    def pair(a, b, by, mask):
        return (
            jnp.where(mask, pltpu.roll(b, by, 1), a),
            jnp.where(mask, b, pltpu.roll(a, LANES - by, 1)),
        )

    a0, a1 = pair(r[0], r[1], 32, odd)
    b0, b1 = pair(r[2], r[3], 32, odd)
    o0, o2 = pair(a0, b0, 64, upper)
    o1, o3 = pair(a1, b1, 64, upper)
    return [o0, o1, o2, o3]


def permute_taps(taps_ref, tapb):
    def batch(tb, carry):
        high = tb // 2
        parts = [
            taps_ref[pl.ds(high * 256 + (tb % 2) * 4 + q, 32, stride=8), :] for q in range(4)
        ]
        out = block_transpose(jnp.concatenate(parts, axis=0))
        for q in range(4):
            for i in range(ROWS):
                tapb[pl.ds(pl.multiple_of((i * 16 + tb * 4 + q) * 8, 8), 8), :] = jnp.broadcast_to(
                    out[q][i : i + 1], (8, LANES)
                )
        return carry

    lax.fori_loop(0, 4, batch, 0)


def permute_batch(raw, xf, b, row0):
    for c in range(2):
        x = [raw[s, pl.ds(b * 256 + c, LANES, stride=2), :] for s in range(4)]
        packed = (
            (x[0] & 255) | ((x[1] & 255) << 8) | ((x[2] & 255) << 16) | (x[3] << 24)
        )
        out = block_transpose(packed)
        for q in range(4):
            for s in range(4):
                value = out[q] << (24 - 8 * s) if s < 3 else out[q]
                value = (value >> 24).astype(jnp.float32)
                xf[2 * s + c, pl.ds(row0 + 4 * b + q, 32, stride=PITCH), :] = value


def order_of(i):
    return lax.rem(i, 4) * 8 + i // 4


def fir(refs, first, groups, tap0, tap1, extend=False):
    (xf, tapb, y) = refs

    def body(i, carry):
        base = i * PITCH + HALO + first * GROUP
        place = order_of(i)
        tap = {
            t: tapb[pl.ds(pl.multiple_of((i * 16 + t) * 8, 8), 8), :] for t in range(tap0, tap1)
        }
        for c in range(2):
            cols = slice(c * LANES, (c + 1) * LANES)
            for s in range(4):
                at = [
                    pl.ds(pl.multiple_of((g * 128 + s * 32 + place) * 8, 8), 8)
                    for g in range(groups)
                ]
                acc = [y[at[g], cols] if extend else None for g in range(groups)]
                for w in range(1 - tap1, 8 * (groups - 1) - tap0 + 1):
                    users = [g for g in range(groups) if tap0 <= 8 * g - w < tap1]
                    if not users:
                        continue
                    x = xf[2 * s + c, pl.ds(base + w, 8), :]
                    for g in users:
                        term = tap[8 * g - w] * x
                        acc[g] = term if acc[g] is None else acc[g] + term
                for g in range(groups):
                    y[at[g], cols] = acc[g]
        return carry

    lax.fori_loop(0, ROWS, body, 0)


def transform(refs, row_group, groups, fresh=False):
    (y, wh, wl, twc, tws, v, u, pbuf, sums) = refs

    def stage1(m, carry):
        at = pl.ds(pl.multiple_of(m * 512, 512), 512)
        x = y[at, :]
        h = x.astype(jnp.bfloat16)
        l = (x - h.astype(jnp.float32)).astype(jnp.bfloat16)
        dot = functools.partial(jnp.dot, preferred_element_type=jnp.float32)
        v[at, :] = dot(h, wh[...]) + dot(l, wh[...]) + dot(h, wl[...])
        return carry

    lax.fori_loop(0, 2 * groups, stage1, 0)

    def tile(n):
        return pl.ds(pl.multiple_of(n * 8, 8), 8)

    def stage2a(gs, carry):
        for i0 in range(4):
            xs = []
            for i1 in range(8):
                i = 4 * i1 + i0
                at = tile(gs * 32 + i0 * 8 + i1)
                x = (v[at, :LANES], v[at, LANES:])
                if i:
                    c = jnp.broadcast_to(twc[i : i + 1, :], (8, LANES))
                    d = jnp.broadcast_to(tws[i : i + 1, :], (8, LANES))
                    x = (x[0] * c + x[1] * d, x[1] * c - x[0] * d)
                xs.append(x)
            for ka, x in enumerate(fft8(xs)):
                x = rotate(x, i0 * ka, 32)
                at = tile(gs * 37 + i0 * 9 + ka)
                u[0, at, :] = x[0]
                u[1, at, :] = x[1]
        return carry

    lax.fori_loop(0, 4 * groups, stage2a, 0)

    def stage2b(n, carry):
        g = n // 8
        ka = lax.rem(n, 8)
        rows = tile(row_group + g)

        def tally(q, value):
            sums[q, at, :] = value if fresh else sums[q, at, :] + value

        spectra = []
        for s in range(4):
            xs = []
            for i0 in range(4):
                at = tile((g * 4 + s) * 37 + i0 * 9 + ka)
                xs.append((u[0, at, :], u[1, at, :]))
            spectra.append(fft4(xs))
        for kb in range(4):
            k1 = ka + 8 * kb
            z = [spectra[s][kb] for s in range(4)]
            at = tile(k1)
            for s in range(4):
                tally(s, z[s][0] * z[s][0] + z[s][1] * z[s][1])
            cols = pl.ds(pl.multiple_of(k1 * LANES, LANES), LANES)
            for p in range(4):
                a, b = z[p // 2], z[2 + p % 2]
                re = a[0] * b[0] + a[1] * b[1]
                im = a[1] * b[0] - a[0] * b[1]
                tally(4 + p, re)
                tally(8 + p, im)
                pbuf[0, p, rows, cols] = re
                pbuf[1, p, rows, cols] = im
        return carry

    lax.fori_loop(0, 8 * groups, stage2b, 0)


HALF = ROWS // 2


class Ring:
    def __init__(self, half, a, b):
        self.half, self.a, self.b, self.c = half, a, b, TM[2]
        self.na, self.nb, self.nc = (lax.axis_size(n) for n in (a, b, self.c))
        self.members = self.na * self.nc
        self.per = HALF // self.members
        far = sorted(range(self.na), key=lambda d: -min(d, self.na - d))
        self.steps = [(d, e) for d in far for e in range(self.nc) if (d, e) != (0, 0)]
        self.shifts = sorted(range(1, self.nb), key=lambda d: -min(d, self.nb - d))

    def member(self, d=0, e=0):
        at = lax.rem(lax.axis_index(self.a) + d, self.na)
        core = lax.rem(lax.axis_index(self.c) + e, self.nc)
        return at * self.nc + core

    def member_id(self, d, e):
        return {
            self.a: lax.rem(lax.axis_index(self.a) + d, self.na),
            self.c: lax.rem(lax.axis_index(self.c) + e, self.nc),
        }

    def column_id(self, d):
        return {self.b: lax.rem(lax.axis_index(self.b) + d, self.nb)}


def rings():
    return (Ring(0, TM[1], TM[0]), Ring(1, TM[0], TM[1]))


def remote(src, dst, send, recv, to):
    return pltpu.make_async_remote_copy(
        src_ref=src,
        dst_ref=dst,
        send_sem=send,
        recv_sem=recv,
        device_id=to,
        device_id_type=pl.DeviceIdType.MESH,
    )


def all_reduce(total, sums, more, stats_ref, scratch, ready):
    both = rings()
    work = []
    for ring in both:
        part, rows_in, mine, cols_in, stat, sems = scratch[ring.half]
        work.append((ring, part, rows_in, mine, cols_in, stat, sems))

    def row_copy(job, n):
        ring, part, rows_in, _, _, _, sems = job
        d, e = ring.steps[n]
        return remote(
            part.at[ring.member(d, e)], rows_in.at[n], sems.at[0, n], sems.at[1, n],
            ring.member_id(d, e),
        )

    def col_copy(job, n):
        ring, _, _, mine, cols_in, _, sems = job
        return remote(
            mine, cols_in.at[n], sems.at[2, n], sems.at[3, n], ring.column_id(ring.shifts[n])
        )

    def place(ring):
        return pl.ds(HALF * ring.half + ring.member() * ring.per, ring.per)

    def gather_copy(job, n):
        ring, _, _, _, _, stat, sems = job
        return remote(
            stat, stats_ref.at[place(ring)], sems.at[4, n], sems.at[5, n],
            ring.member_id(*ring.steps[n]),
        )

    for job in work:
        ring, part = job[:2]
        for k in range(HALF):
            k1 = HALF * ring.half + k
            for j in range(3):
                part[k // ring.per, k % ring.per, j] = jnp.concatenate(
                    [
                        jnp.sum(
                            sums[4 * j + q, k1 * 8 : k1 * 8 + 8, :]
                            + more[4 * j + q, k1 * 8 : k1 * 8 + 8, :],
                            axis=0,
                            keepdims=True,
                        )
                        for q in range(4)
                    ],
                    axis=0,
                )
        if ring.half == 0:
            ready()
        for n in range(len(ring.steps)):
            row_copy(job, n).start()

    totals = []
    for job in work:
        ring, part, rows_in, mine = job[:4]
        acc = part[ring.member()]
        for n in reversed(range(len(ring.steps))):
            row_copy(job, n).wait_recv()
            acc = acc + rows_in[n]
        mine[...] = acc
        for n in range(len(ring.shifts)):
            col_copy(job, n).start()
        totals.append(acc)

    for job, acc in zip(work, totals):
        ring, _, _, _, cols_in, stat, _ = job
        for n in reversed(range(len(ring.shifts))):
            col_copy(job, n).wait_recv()
            acc = acc + cols_in[n]
        mean = acc * np.float32(1.0 / total)
        for r in range(ring.per):
            power, re, im = mean[r, 0], mean[r, 1], mean[r, 2]
            raised = power + 1e-06
            denom = jnp.concatenate(
                [raised[p // 2 : p // 2 + 1] * raised[2 + p % 2 : 3 + p % 2] for p in range(4)],
                axis=0,
            )
            stat[r, 0] = power
            stat[r, 1] = (re * re + im * im) / denom
        for n in range(len(ring.steps)):
            gather_copy(job, n).start()
        stats_ref[place(ring)] = stat[...]

    for job in work:
        ring = job[0]
        for n in reversed(range(len(ring.steps))):
            gather_copy(job, n).wait_recv()
    for job in work:
        ring = job[0]
        for n in range(len(ring.steps)):
            row_copy(job, n).wait_send()
            gather_copy(job, n).wait_send()
        for n in range(len(ring.shifts)):
            col_copy(job, n).wait_send()


def filter_kernel(
    samples_ref, taps_ref, wh, wl, twc, tws, prod_ref, y0_ref, sums,
    raw, hraw, xf, tapb, y, v, u, in_sems, halo_send, halo_recv,
):
    x_name, y_name, c_name = TM
    nx, ny, nc = (lax.axis_size(n) for n in TM)
    me = [lax.axis_index(n) for n in TM]
    place = (me[0] * ny + me[1]) * nc + me[2]
    has_next = place < nx * ny * nc - 1
    has_prev = place > 0

    def tm_id(index):
        return {
            x_name: index // (ny * nc),
            y_name: lax.rem(index // nc, ny),
            c_name: lax.rem(index, nc),
        }

    barrier = pltpu.get_barrier_semaphore()

    @pl.when(has_prev)
    def _():
        pl.semaphore_signal(
            barrier, inc=1, device_id=tm_id(place - 1), device_id_type=pl.DeviceIdType.MESH
        )

    frames = samples_ref.shape[1] // 64

    def halo_copy(b):
        lead = 1 if b == 0 else 0
        at = (4 * b + lead) * 64
        size = (4 - lead) * 64
        start = (frames - HALO) * 64 + at
        return remote(
            samples_ref.at[:, pl.ds(start, size), :], hraw.at[:, pl.ds(at, size), :],
            halo_send.at[b], halo_recv.at[b], tm_id(place + 1),
        )

    def in_copy(b):
        rows = pl.ds(pl.multiple_of(b * 256, 256), 256)
        return pltpu.make_async_copy(samples_ref.at[:, rows, :], raw.at[:, rows, :], in_sems.at[b])

    for b in range(12):
        in_copy(b).start()

    permute_taps(taps_ref, tapb)

    @pl.when(has_next)
    def _():
        pl.semaphore_wait(barrier, 1)
        for b in (3, 2, 1, 0):
            halo_copy(b).start()

    @pl.when(jnp.logical_not(has_prev))
    def _():
        hraw[...] = jnp.zeros_like(hraw)

    def halo_wait(b):
        @pl.when(has_prev)
        def _():
            halo_copy(b).wait_recv()

    filters = (xf, tapb, y)
    refs = (y, wh, wl, twc, tws, v, u, prod_ref, sums)
    sums[...] = jnp.zeros_like(sums)

    def own_batch(b, carry):
        in_copy(b).wait()
        permute_batch(raw, xf, b, HALO)
        return carry

    lax.fori_loop(0, 12, own_batch, 0)

    fir(filters, 2, 4, 0, 16)
    transform(refs, 1, 4)

    halo_wait(3)
    halo_wait(2)
    permute_batch(hraw, xf, 3, 0)
    permute_batch(hraw, xf, 2, 0)
    fir(filters, 1, 1, 0, 16)
    transform(refs, 0, 1)

    filters = (xf, tapb, y0_ref)
    halo_wait(1)
    permute_batch(hraw, xf, 1, 0)
    fir(filters, 0, 1, 0, 13)
    halo_wait(0)
    permute_batch(hraw, xf, 0, 0)
    fir(filters, 0, 1, 13, 16, extend=True)

    @pl.when(has_next)
    def _():
        for b in range(4):
            halo_copy(b).wait_send()


def reduce_kernel(
    total, y0, sums_ref, wh, wl, twc, tws, prod_ref, stats_ref,
    v, u, sums, part0, rows0, mine0, cols0, stat0, sems0,
    part1, rows1, mine1, cols1, stat1, sems1,
):
    barrier = pltpu.get_barrier_semaphore()
    greeted = 0
    for ring in rings():
        for d, e in ring.steps:
            if ring.half == 1 and d == 0:
                continue
            pl.semaphore_signal(
                barrier,
                inc=1,
                device_id=ring.member_id(d, e),
                device_id_type=pl.DeviceIdType.MESH,
            )
            greeted += 1

    transform((y0, wh, wl, twc, tws, v, u, prod_ref, sums), 0, 1, fresh=True)
    all_reduce(
        total, sums, sums_ref, stats_ref,
        (
            (part0, rows0, mine0, cols0, stat0, sems0),
            (part1, rows1, mine1, cols1, stat1, sems1),
        ),
        lambda: pl.semaphore_wait(barrier, greeted),
    )


VMEM_ALL = pl.BlockSpec(memory_space=pltpu.VMEM)
ANYWHERE = pl.BlockSpec(memory_space=pl.ANY)
WIDE = 4096 + LANES
MIB = 1024 * 1024


def filter_call(rows, taps_rows, consts):
    frames = rows.shape[1] // 64
    f32, i32 = jnp.float32, jnp.int32
    dma = pltpu.SemaphoreType.DMA
    return pl.pallas_call(
        filter_kernel,
        out_shape=(
            jax.ShapeDtypeStruct((2, 4, frames - GROUP, WIDE), f32),
            jax.ShapeDtypeStruct((1024, 256), f32),
            jax.ShapeDtypeStruct((12, (ROWS + 1) * 8, LANES), f32),
        ),
        in_specs=[ANYWHERE] + [VMEM_ALL] * 5,
        out_specs=(VMEM_ALL, VMEM_ALL, VMEM_ALL),
        scratch_shapes=[
            pltpu.VMEM((4, frames * 64, LANES), i32),
            pltpu.VMEM((4, HALO * 64, LANES), i32),
            pltpu.VMEM((8, ROWS * PITCH + 7, LANES), f32),
            pltpu.VMEM((ROWS * 16 * 8, LANES), f32),
            pltpu.VMEM((4096, 256), f32),
            pltpu.VMEM((4096, 256), f32),
            pltpu.VMEM((2, 16 * 37 * 8 + 16, LANES), f32),
            dma((12,)),
            dma((4,)),
            dma((4,)),
        ],
        compiler_params=pltpu.CompilerParams(
            vmem_limit_bytes=45 * MIB, collective_id=0, has_side_effects=True
        ),
        cost_estimate=pl.CostEstimate(
            flops=4_000_000_000, bytes_accessed=16_000_000, transcendentals=0
        ),
        name="filter",
    )(rows, taps_rows, *consts)


def reduce_call(y0, sums, consts, total):
    f32 = jnp.float32
    dma = pltpu.SemaphoreType.DMA
    exchange = []
    for ring in rings():
        exchange += [
            pltpu.VMEM((ring.members, ring.per, 3, 4, LANES), f32),
            pltpu.VMEM((ring.members - 1, ring.per, 3, 4, LANES), f32),
            pltpu.VMEM((ring.per, 3, 4, LANES), f32),
            pltpu.VMEM((max(ring.nb - 1, 1), ring.per, 3, 4, LANES), f32),
            pltpu.VMEM((ring.per, 2, 4, LANES), f32),
            dma((6, max(ring.members, ring.nb) - 1)),
        ]
    return pl.pallas_call(
        functools.partial(reduce_kernel, total),
        out_shape=(
            jax.ShapeDtypeStruct((2, 4, GROUP, WIDE), f32),
            jax.ShapeDtypeStruct((ROWS, 2, 4, LANES), f32),
        ),
        in_specs=[VMEM_ALL] * 6,
        out_specs=(VMEM_ALL, VMEM_ALL),
        scratch_shapes=[
            pltpu.VMEM((1024, 256), f32),
            pltpu.VMEM((2, 4 * 37 * 8 + 16, LANES), f32),
            pltpu.VMEM((12, (ROWS + 1) * 8, LANES), f32),
            *exchange,
        ],
        compiler_params=pltpu.CompilerParams(
            vmem_limit_bytes=16 * MIB, collective_id=1, has_side_effects=True
        ),
        cost_estimate=pl.CostEstimate(
            flops=400_000_000, bytes_accessed=3_000_000, transcendentals=0
        ),
        name="reduce",
    )(y0, sums, *consts)


def normalize_kernel(pairs_ref, stats_ref, first_ref, rest_ref, coh_ref, out_ref, buf, writes):
    frames = buf.shape[2]

    def write(p, part):
        return pltpu.make_async_copy(
            buf.at[p, part], out_ref.at[part, p], writes.at[2 * p + part]
        )

    def stat(q):
        return stats_ref[pl.ds(q, ROWS, stride=8), :]

    def pair(p, carry):
        which = pairs_ref[0, p] * 2 + pairs_ref[1, p] - 2
        power = (stat(pairs_ref[0, p]) + 1e-06) * (stat(pairs_ref[1, p]) + 1e-06)
        factor = 1.0 / jnp.sqrt(power)
        for part in range(2):
            for k1 in range(ROWS):
                cols = slice(k1 * LANES, (k1 + 1) * LANES)
                row = factor[k1 : k1 + 1]
                buf[p, part, 0:GROUP, cols] = first_ref[part, which, :, cols] * row
                buf[p, part, GROUP:frames, cols] = rest_ref[part, which, :, cols] * row
            write(p, part).start()
        return carry

    lax.fori_loop(0, 4, pair, 0)
    for p in range(4):
        value = stat(4 + pairs_ref[0, p] * 2 + pairs_ref[1, p] - 2)
        for k1 in range(ROWS):
            coh_ref[p : p + 1, k1 * LANES : (k1 + 1) * LANES] = value[k1 : k1 + 1]
    for p in range(4):
        for part in range(2):
            write(p, part).wait()


def normalize_call(pairs, stats, first, rest):
    frames = first.shape[2] + rest.shape[2]
    f32 = jnp.float32
    return pl.pallas_call(
        normalize_kernel,
        in_specs=[pl.BlockSpec(memory_space=pltpu.SMEM)] + [VMEM_ALL] * 3,
        out_specs=(VMEM_ALL, ANYWHERE),
        out_shape=(
            jax.ShapeDtypeStruct((4, 4096), f32),
            jax.ShapeDtypeStruct((2, 4, frames, 4096), f32),
        ),
        scratch_shapes=[
            pltpu.VMEM((4, 2, frames, 4096), f32),
            pltpu.SemaphoreType.DMA((8,)),
        ],
        compiler_params=pltpu.CompilerParams(vmem_limit_bytes=20 * MIB),
        cost_estimate=pl.CostEstimate(flops=2_000_000, bytes_accessed=13_000_000, transcendentals=0),
        name="normalize",
    )(pairs.T, stats.reshape(-1, LANES), first, rest)


def sample_rows(volts):
    streams, comps, local = volts.shape
    rows = volts.reshape(streams, comps, local // LANES, LANES)
    return jnp.transpose(rows, (0, 2, 1, 3)).reshape(streams, local // LANES * comps, LANES)


def tap_rows(taps):
    taps = taps.reshape(2, 8, ROWS, LANES)
    return jnp.transpose(taps, (0, 2, 1, 3)).reshape(512, LANES)


def on_device(volts, taps, pairs):
    rows = sample_rows(volts)
    total = rows.shape[1] // 64 * lax.axis_size(TM)
    consts = [jnp.asarray(c) for c in constants()]
    rest, y0, sums = filter_call(rows, tap_rows(taps), consts)
    first, stats = reduce_call(y0, sums, consts, total)
    return normalize_call(pairs, stats, first, rest)


def solution(mesh):
    devices = mesh.devices
    finer = Mesh(
        devices.reshape(mesh.shape["band"], 8, 8, 2), ("band", "tm_0", "tm_1", "tm_2")
    )
    return jax.shard_map(
        on_device,
        mesh=finer,
        in_specs=(P("band", None, TM), P(), P()),
        out_specs=(P("band", None), P(None, "band", TM, None)),
        check_vma=False,
    )
```

```python
import functools
import math

import jax
import jax.numpy as jnp
import numpy as np
from jax import lax
from jax.experimental import pallas as pl
from jax.experimental.pallas import tpu as pltpu
from jax.sharding import Mesh
from jax.sharding import PartitionSpec as P

TM = ("tm_0", "tm_1", "tm_2")
ROWS = 32
LANES = 128
PITCH = 65
HALO = 16
GROUP = 8


def fill_tables(wh, wl, twc, tws):
    row = lax.broadcasted_iota(jnp.int32, (LANES, LANES), 0)
    k = lax.broadcasted_iota(jnp.int32, (LANES, LANES), 1)
    j = 4 * (row & 31) + (row >> 5)
    angle = ((j * k) & (LANES - 1)).astype(jnp.float32) * np.float32(2.0 * math.pi / LANES)
    cos, sin = jnp.cos(angle) * np.float32(1 / 64), jnp.sin(angle) * np.float32(1 / 64)
    low, high = slice(0, LANES), slice(LANES, 2 * LANES)
    for rows, cols, value in (
        (low, low, cos), (low, high, -sin), (high, low, sin), (high, high, cos),
    ):
        head = value.astype(jnp.bfloat16)
        wh[rows, cols] = head
        wl[rows, cols] = (value - head.astype(jnp.float32)).astype(jnp.bfloat16)
    i = lax.broadcasted_iota(jnp.int32, (ROWS, LANES), 0)
    k = lax.broadcasted_iota(jnp.int32, (ROWS, LANES), 1)
    turn = (i * k).astype(jnp.float32) * np.float32(2.0 * math.pi / 4096)
    twc[...] = jnp.cos(turn)
    tws[...] = jnp.sin(turn)


def add(a, b):
    return (a[0] + b[0], a[1] + b[1])


def sub(a, b):
    return (a[0] - b[0], a[1] - b[1])


def fft4(x):
    a, b = add(x[0], x[2]), sub(x[0], x[2])
    c, d = add(x[1], x[3]), sub(x[1], x[3])
    return [
        add(a, c),
        (b[0] + d[1], b[1] - d[0]),
        sub(a, c),
        (b[0] - d[1], b[1] + d[0]),
    ]


def fft8(x):
    even = fft4(x[0::2])
    odd = fft4(x[1::2])
    r = np.float32(math.sqrt(0.5))
    turned = [
        odd[0],
        ((odd[1][0] + odd[1][1]) * r, (odd[1][1] - odd[1][0]) * r),
        (odd[2][1], -odd[2][0]),
        ((odd[3][1] - odd[3][0]) * r, (odd[3][0] + odd[3][1]) * -r),
    ]
    return [add(e, o) for e, o in zip(even, turned)] + [sub(e, o) for e, o in zip(even, turned)]


def rotate(x, index, length):
    index = index % length
    if index == 0:
        return x
    if index * 4 == length:
        return (x[1], -x[0])
    c = np.float32(math.cos(2 * math.pi * index / length))
    s = np.float32(math.sin(2 * math.pi * index / length))
    return (x[0] * c + x[1] * s, x[1] * c - x[0] * s)


def block_transpose(rows):
    turned = rows.T
    lane = lax.broadcasted_iota(jnp.int32, (32, LANES), 1)
    odd = (lane & 32) != 0
    upper = (lane & 64) != 0
    r = [turned[32 * b : 32 * b + 32] for b in range(4)]

    def pair(a, b, by, mask):
        return (
            jnp.where(mask, pltpu.roll(b, by, 1), a),
            jnp.where(mask, b, pltpu.roll(a, LANES - by, 1)),
        )

    a0, a1 = pair(r[0], r[1], 32, odd)
    b0, b1 = pair(r[2], r[3], 32, odd)
    o0, o2 = pair(a0, b0, 64, upper)
    o1, o3 = pair(a1, b1, 64, upper)
    return [o0, o1, o2, o3]


def permute_taps(taps_ref, tapb):
    def batch(tb, carry):
        high = tb // 2
        parts = [
            taps_ref[pl.ds(high * 256 + (tb % 2) * 4 + q, 32, stride=8), :] for q in range(4)
        ]
        out = block_transpose(jnp.concatenate(parts, axis=0))
        for q in range(4):
            for i in range(ROWS):
                tapb[pl.ds(pl.multiple_of((i * 16 + tb * 4 + q) * 8, 8), 8), :] = jnp.broadcast_to(
                    out[q][i : i + 1], (8, LANES)
                )
        return carry

    lax.fori_loop(0, 4, batch, 0)


def permute_batch(raw, xf, b, row0):
    for c in range(2):
        x = [raw[s, pl.ds(b * 256 + c, LANES, stride=2), :] for s in range(4)]
        packed = (
            (x[0] & 255) | ((x[1] & 255) << 8) | ((x[2] & 255) << 16) | (x[3] << 24)
        )
        out = block_transpose(packed)
        for q in range(4):
            for s in range(4):
                value = out[q] << (24 - 8 * s) if s < 3 else out[q]
                value = (value >> 24).astype(jnp.float32)
                xf[2 * s + c, pl.ds(row0 + 4 * b + q, 32, stride=PITCH), :] = value


def order_of(i):
    return lax.rem(i, 4) * 8 + i // 4


def fir(refs, first, groups, tap0, tap1, extend=False):
    (xf, tapb, y) = refs

    def body(i, carry):
        base = i * PITCH + HALO + first * GROUP
        place = order_of(i)
        tap = {
            t: tapb[pl.ds(pl.multiple_of((i * 16 + t) * 8, 8), 8), :] for t in range(tap0, tap1)
        }
        for s in range(4):
            at = [
                pl.ds(pl.multiple_of((g * 128 + s * 32 + place) * 8, 8), 8)
                for g in range(groups)
            ]
            cols = [slice(c * LANES, (c + 1) * LANES) for c in range(2)]
            acc = [
                [y[at[g], cols[c]] if extend else None for c in range(2)] for g in range(groups)
            ]
            for w in range(1 - tap1, 8 * (groups - 1) - tap0 + 1):
                users = [g for g in range(groups) if tap0 <= 8 * g - w < tap1]
                if not users:
                    continue
                x = [xf[2 * s + c, pl.ds(base + w, 8), :] for c in range(2)]
                for g in users:
                    for c in range(2):
                        term = tap[8 * g - w] * x[c]
                        acc[g][c] = term if acc[g][c] is None else acc[g][c] + term
            for g in range(groups):
                for c in range(2):
                    y[at[g], cols[c]] = acc[g][c]
        return carry

    lax.fori_loop(0, ROWS, body, 0)


def transform(refs, row_group, groups, fresh=False):
    (y, wh, wl, twc, tws, v, u, pbuf, sums) = refs

    def stage1(m, carry):
        at = pl.ds(pl.multiple_of(m * 1024, 1024), 1024)
        x = y[at, :]
        h = x.astype(jnp.bfloat16)
        l = (x - h.astype(jnp.float32)).astype(jnp.bfloat16)
        dot = functools.partial(jnp.dot, preferred_element_type=jnp.float32)
        v[at, :] = dot(h, wh[...]) + dot(l, wh[...]) + dot(h, wl[...])
        return carry

    lax.fori_loop(0, groups, stage1, 0)

    def tile(n):
        return pl.ds(pl.multiple_of(n * 8, 8), 8)

    def stage2a(gs, carry):
        for i0 in range(4):
            xs = []
            for i1 in range(8):
                i = 4 * i1 + i0
                at = tile(gs * 32 + i0 * 8 + i1)
                x = (v[at, :LANES], v[at, LANES:])
                if i:
                    c = jnp.broadcast_to(twc[i : i + 1, :], (8, LANES))
                    d = jnp.broadcast_to(tws[i : i + 1, :], (8, LANES))
                    x = (x[0] * c + x[1] * d, x[1] * c - x[0] * d)
                xs.append(x)
            for ka, x in enumerate(fft8(xs)):
                x = rotate(x, i0 * ka, 32)
                at = tile(gs * 37 + i0 * 9 + ka)
                u[0, at, :] = x[0]
                u[1, at, :] = x[1]
        return carry

    lax.fori_loop(0, 4 * groups, stage2a, 0)

    def stage2b(n, carry):
        g = n // 8
        ka = lax.rem(n, 8)
        rows = tile(row_group + g)

        def tally(q, value):
            sums[q, at, :] = value if fresh else sums[q, at, :] + value

        spectra = []
        for s in range(4):
            xs = []
            for i0 in range(4):
                at = tile((g * 4 + s) * 37 + i0 * 9 + ka)
                xs.append((u[0, at, :], u[1, at, :]))
            spectra.append(fft4(xs))
        for kb in range(4):
            k1 = ka + 8 * kb
            z = [spectra[s][kb] for s in range(4)]
            at = tile(k1)
            for s in range(4):
                tally(s, z[s][0] * z[s][0] + z[s][1] * z[s][1])
            cols = pl.ds(pl.multiple_of(k1 * LANES, LANES), LANES)
            for p in range(4):
                a, b = z[p // 2], z[2 + p % 2]
                re = a[0] * b[0] + a[1] * b[1]
                im = a[1] * b[0] - a[0] * b[1]
                tally(4 + p, re)
                tally(8 + p, im)
                pbuf[0, p, rows, cols] = re
                pbuf[1, p, rows, cols] = im
        return carry

    lax.fori_loop(0, 8 * groups, stage2b, 0)


HALF = ROWS // 2


class Ring:
    def __init__(self, half, a, b):
        self.half, self.a, self.b, self.c = half, a, b, TM[2]
        self.na, self.nb, self.nc = (lax.axis_size(n) for n in (a, b, self.c))
        self.members = self.na * self.nc
        self.per = HALF // self.members
        far = sorted(range(self.na), key=lambda d: -min(d, self.na - d))
        self.steps = [(d, e) for d in far for e in range(self.nc) if (d, e) != (0, 0)]
        self.shifts = sorted(range(1, self.nb), key=lambda d: -min(d, self.nb - d))

    def member(self, d=0, e=0):
        at = lax.rem(lax.axis_index(self.a) + d, self.na)
        core = lax.rem(lax.axis_index(self.c) + e, self.nc)
        return at * self.nc + core

    def member_id(self, d, e):
        return {
            self.a: lax.rem(lax.axis_index(self.a) + d, self.na),
            self.c: lax.rem(lax.axis_index(self.c) + e, self.nc),
        }

    def column_id(self, d):
        return {self.b: lax.rem(lax.axis_index(self.b) + d, self.nb)}


def rings():
    return (Ring(0, TM[1], TM[0]), Ring(1, TM[0], TM[1]))


def remote(src, dst, send, recv, to):
    return pltpu.make_async_remote_copy(
        src_ref=src,
        dst_ref=dst,
        send_sem=send,
        recv_sem=recv,
        device_id=to,
        device_id_type=pl.DeviceIdType.MESH,
    )


def all_reduce(total, sums, more, stats_ref, scratch, ready):
    both = rings()
    work = []
    for ring in both:
        part, rows_in, mine, cols_in, stat, sems = scratch[ring.half]
        work.append((ring, part, rows_in, mine, cols_in, stat, sems))

    def row_copy(job, n):
        ring, part, rows_in, _, _, _, sems = job
        d, e = ring.steps[n]
        return remote(
            part.at[ring.member(d, e)], rows_in.at[n], sems.at[0, n], sems.at[1, n],
            ring.member_id(d, e),
        )

    def col_copy(job, n):
        ring, _, _, mine, cols_in, _, sems = job
        return remote(
            mine, cols_in.at[n], sems.at[2, n], sems.at[3, n], ring.column_id(ring.shifts[n])
        )

    def place(ring):
        return pl.ds(HALF * ring.half + ring.member() * ring.per, ring.per)

    def gather_copy(job, n):
        ring, _, _, _, _, stat, sems = job
        return remote(
            stat, stats_ref.at[place(ring)], sems.at[4, n], sems.at[5, n],
            ring.member_id(*ring.steps[n]),
        )

    for job in work:
        ring, part = job[:2]
        for k in range(HALF):
            k1 = HALF * ring.half + k
            for j in range(3):
                part[k // ring.per, k % ring.per, j] = jnp.concatenate(
                    [
                        jnp.sum(
                            sums[4 * j + q, k1 * 8 : k1 * 8 + 8, :]
                            + more[4 * j + q, k1 * 8 : k1 * 8 + 8, :],
                            axis=0,
                            keepdims=True,
                        )
                        for q in range(4)
                    ],
                    axis=0,
                )
        if ring.half == 0:
            ready()
        for n in range(len(ring.steps)):
            row_copy(job, n).start()

    totals = []
    for job in work:
        ring, part, rows_in, mine = job[:4]
        acc = part[ring.member()]
        for n in reversed(range(len(ring.steps))):
            row_copy(job, n).wait_recv()
            acc = acc + rows_in[n]
        mine[...] = acc
        for n in range(len(ring.shifts)):
            col_copy(job, n).start()
        totals.append(acc)

    for job, acc in zip(work, totals):
        ring, _, _, _, cols_in, stat, _ = job
        for n in reversed(range(len(ring.shifts))):
            col_copy(job, n).wait_recv()
            acc = acc + cols_in[n]
        mean = acc * np.float32(1.0 / total)
        for r in range(ring.per):
            power, re, im = mean[r, 0], mean[r, 1], mean[r, 2]
            raised = power + 1e-06
            denom = jnp.concatenate(
                [raised[p // 2 : p // 2 + 1] * raised[2 + p % 2 : 3 + p % 2] for p in range(4)],
                axis=0,
            )
            stat[r, 0] = power
            stat[r, 1] = (re * re + im * im) / denom
        for n in range(len(ring.steps)):
            gather_copy(job, n).start()
        stats_ref[place(ring)] = stat[...]

    for job in work:
        ring = job[0]
        for n in reversed(range(len(ring.steps))):
            gather_copy(job, n).wait_recv()
    for job in work:
        ring = job[0]
        for n in range(len(ring.steps)):
            row_copy(job, n).wait_send()
            gather_copy(job, n).wait_send()
        for n in range(len(ring.shifts)):
            col_copy(job, n).wait_send()


def filter_kernel(
    samples_ref, taps_ref,
    prod_ref, y0_ref, sums, wh, wl, twc, tws,
    raw, hraw, xf, tapb, y, v, u, in_sems, halo_send, halo_recv,
):
    x_name, y_name, c_name = TM
    nx, ny, nc = (lax.axis_size(n) for n in TM)
    me = [lax.axis_index(n) for n in TM]
    place = (me[0] * ny + me[1]) * nc + me[2]
    has_next = place < nx * ny * nc - 1
    has_prev = place > 0

    def tm_id(index):
        return {
            x_name: index // (ny * nc),
            y_name: lax.rem(index // nc, ny),
            c_name: lax.rem(index, nc),
        }

    barrier = pltpu.get_barrier_semaphore()

    @pl.when(has_prev)
    def _():
        pl.semaphore_signal(
            barrier, inc=1, device_id=tm_id(place - 1), device_id_type=pl.DeviceIdType.MESH
        )

    frames = samples_ref.shape[1] // 64

    def halo_copy(b):
        lead = 1 if b == 0 else 0
        at = (4 * b + lead) * 64
        size = (4 - lead) * 64
        start = (frames - HALO) * 64 + at
        return remote(
            samples_ref.at[:, pl.ds(start, size), :], hraw.at[:, pl.ds(at, size), :],
            halo_send.at[b], halo_recv.at[b], tm_id(place + 1),
        )

    def in_copy(b):
        rows = pl.ds(pl.multiple_of(b * 256, 256), 256)
        return pltpu.make_async_copy(samples_ref.at[:, rows, :], raw.at[:, rows, :], in_sems.at[b])

    for b in range(12):
        in_copy(b).start()

    @pl.when(has_next)
    def _():
        pl.semaphore_wait(barrier, 1)
        for b in (3, 2, 1, 0):
            halo_copy(b).start()

    @pl.when(jnp.logical_not(has_prev))
    def _():
        hraw[...] = jnp.zeros_like(hraw)

    def halo_wait(b):
        @pl.when(has_prev)
        def _():
            halo_copy(b).wait_recv()

    filters = (xf, tapb, y)
    refs = (y, wh, wl, twc, tws, v, u, prod_ref, sums)
    sums[...] = jnp.zeros_like(sums)
    fill_tables(wh, wl, twc, tws)
    permute_taps(taps_ref, tapb)

    def own_batch(b, carry):
        in_copy(b).wait()
        permute_batch(raw, xf, b, HALO)
        return carry

    lax.fori_loop(0, 12, own_batch, 0)

    fir(filters, 2, 4, 0, 16)
    transform(refs, 1, 4)

    halo_wait(3)
    halo_wait(2)
    permute_batch(hraw, xf, 3, 0)
    permute_batch(hraw, xf, 2, 0)
    fir(filters, 1, 1, 0, 16)
    transform(refs, 0, 1)

    filters = (xf, tapb, y0_ref)
    halo_wait(1)
    permute_batch(hraw, xf, 1, 0)
    fir(filters, 0, 1, 0, 13)
    halo_wait(0)
    permute_batch(hraw, xf, 0, 0)
    fir(filters, 0, 1, 13, 16, extend=True)

    @pl.when(has_next)
    def _():
        for b in range(4):
            halo_copy(b).wait_send()


def reduce_kernel(
    total, y0, sums_ref, wh, wl, twc, tws, prod_ref, stats_ref,
    v, u, sums, part0, rows0, mine0, cols0, stat0, sems0,
    part1, rows1, mine1, cols1, stat1, sems1,
):
    barrier = pltpu.get_barrier_semaphore()
    greeted = 0
    for ring in rings():
        for d, e in ring.steps:
            if ring.half == 1 and d == 0:
                continue
            pl.semaphore_signal(
                barrier,
                inc=1,
                device_id=ring.member_id(d, e),
                device_id_type=pl.DeviceIdType.MESH,
            )
            greeted += 1

    transform((y0, wh, wl, twc, tws, v, u, prod_ref, sums), 0, 1, fresh=True)
    all_reduce(
        total, sums, sums_ref, stats_ref,
        (
            (part0, rows0, mine0, cols0, stat0, sems0),
            (part1, rows1, mine1, cols1, stat1, sems1),
        ),
        lambda: pl.semaphore_wait(barrier, greeted),
    )


VMEM_ALL = pl.BlockSpec(memory_space=pltpu.VMEM)
ANYWHERE = pl.BlockSpec(memory_space=pl.ANY)
WIDE = 4096 + LANES
MIB = 1024 * 1024


def filter_call(rows, taps_rows):
    frames = rows.shape[1] // 64
    f32, i32 = jnp.float32, jnp.int32
    dma = pltpu.SemaphoreType.DMA
    return pl.pallas_call(
        filter_kernel,
        out_shape=(
            jax.ShapeDtypeStruct((2, 4, frames - GROUP, WIDE), f32),
            jax.ShapeDtypeStruct((1024, 256), f32),
            jax.ShapeDtypeStruct((12, (ROWS + 1) * 8, LANES), f32),
            *[jax.ShapeDtypeStruct((256, 256), jnp.bfloat16)] * 2,
            *[jax.ShapeDtypeStruct((ROWS, LANES), f32)] * 2,
        ),
        in_specs=[ANYWHERE, VMEM_ALL],
        out_specs=(VMEM_ALL,) * 7,
        scratch_shapes=[
            pltpu.VMEM((4, frames * 64, LANES), i32),
            pltpu.VMEM((4, HALO * 64, LANES), i32),
            pltpu.VMEM((8, ROWS * PITCH + 7, LANES), f32),
            pltpu.VMEM((ROWS * 16 * 8, LANES), f32),
            pltpu.VMEM((4096, 256), f32),
            pltpu.VMEM((4096, 256), f32),
            pltpu.VMEM((2, 16 * 37 * 8 + 16, LANES), f32),
            dma((12,)),
            dma((4,)),
            dma((4,)),
        ],
        compiler_params=pltpu.CompilerParams(
            vmem_limit_bytes=45 * MIB, collective_id=0, has_side_effects=True
        ),
        cost_estimate=pl.CostEstimate(
            flops=4_000_000_000, bytes_accessed=16_000_000, transcendentals=0
        ),
        name="filter",
    )(rows, taps_rows)


def reduce_call(y0, sums, consts, total):
    f32 = jnp.float32
    dma = pltpu.SemaphoreType.DMA
    exchange = []
    for ring in rings():
        exchange += [
            pltpu.VMEM((ring.members, ring.per, 3, 4, LANES), f32),
            pltpu.VMEM((ring.members - 1, ring.per, 3, 4, LANES), f32),
            pltpu.VMEM((ring.per, 3, 4, LANES), f32),
            pltpu.VMEM((max(ring.nb - 1, 1), ring.per, 3, 4, LANES), f32),
            pltpu.VMEM((ring.per, 2, 4, LANES), f32),
            dma((6, max(ring.members, ring.nb) - 1)),
        ]
    return pl.pallas_call(
        functools.partial(reduce_kernel, total),
        out_shape=(
            jax.ShapeDtypeStruct((2, 4, GROUP, WIDE), f32),
            jax.ShapeDtypeStruct((ROWS, 2, 4, LANES), f32),
        ),
        in_specs=[VMEM_ALL] * 6,
        out_specs=(VMEM_ALL, VMEM_ALL),
        scratch_shapes=[
            pltpu.VMEM((1024, 256), f32),
            pltpu.VMEM((2, 4 * 37 * 8 + 16, LANES), f32),
            pltpu.VMEM((12, (ROWS + 1) * 8, LANES), f32),
            *exchange,
        ],
        compiler_params=pltpu.CompilerParams(
            vmem_limit_bytes=16 * MIB, collective_id=1, has_side_effects=True
        ),
        cost_estimate=pl.CostEstimate(
            flops=400_000_000, bytes_accessed=3_000_000, transcendentals=0
        ),
        name="reduce",
    )(y0, sums, *consts)


def normalize_kernel(pairs_ref, stats_ref, first_ref, rest_ref, coh_ref, out_ref, buf, writes):
    frames = buf.shape[2]

    def write(p, part):
        return pltpu.make_async_copy(
            buf.at[p, part], out_ref.at[part, p], writes.at[2 * p + part]
        )

    def stat(q):
        return stats_ref[pl.ds(q, ROWS, stride=8), :]

    def pair(p, carry):
        which = pairs_ref[0, p] * 2 + pairs_ref[1, p] - 2
        power = (stat(pairs_ref[0, p]) + 1e-06) * (stat(pairs_ref[1, p]) + 1e-06)
        factor = 1.0 / jnp.sqrt(power)
        for part in range(2):
            for k1 in range(ROWS):
                cols = slice(k1 * LANES, (k1 + 1) * LANES)
                row = factor[k1 : k1 + 1]
                buf[p, part, 0:GROUP, cols] = first_ref[part, which, :, cols] * row
                buf[p, part, GROUP:frames, cols] = rest_ref[part, which, :, cols] * row
            write(p, part).start()
        return carry

    lax.fori_loop(0, 4, pair, 0)
    for p in range(4):
        value = stat(4 + pairs_ref[0, p] * 2 + pairs_ref[1, p] - 2)
        for k1 in range(ROWS):
            coh_ref[p : p + 1, k1 * LANES : (k1 + 1) * LANES] = value[k1 : k1 + 1]
    for p in range(4):
        for part in range(2):
            write(p, part).wait()


def normalize_call(pairs, stats, first, rest):
    frames = first.shape[2] + rest.shape[2]
    f32 = jnp.float32
    return pl.pallas_call(
        normalize_kernel,
        in_specs=[pl.BlockSpec(memory_space=pltpu.SMEM)] + [VMEM_ALL] * 3,
        out_specs=(VMEM_ALL, ANYWHERE),
        out_shape=(
            jax.ShapeDtypeStruct((4, 4096), f32),
            jax.ShapeDtypeStruct((2, 4, frames, 4096), f32),
        ),
        scratch_shapes=[
            pltpu.VMEM((4, 2, frames, 4096), f32),
            pltpu.SemaphoreType.DMA((8,)),
        ],
        compiler_params=pltpu.CompilerParams(vmem_limit_bytes=20 * MIB),
        cost_estimate=pl.CostEstimate(flops=2_000_000, bytes_accessed=13_000_000, transcendentals=0),
        name="normalize",
    )(pairs.T, stats.reshape(-1, LANES), first, rest)


def sample_rows(volts):
    streams, comps, local = volts.shape
    rows = volts.reshape(streams, comps, local // LANES, LANES)
    return jnp.transpose(rows, (0, 2, 1, 3)).reshape(streams, local // LANES * comps, LANES)


def tap_rows(taps):
    taps = taps.reshape(2, 8, ROWS, LANES)
    return jnp.transpose(taps, (0, 2, 1, 3)).reshape(512, LANES)


def on_device(volts, taps, pairs):
    rows = sample_rows(volts)
    total = rows.shape[1] // 64 * lax.axis_size(TM)
    rest, y0, sums, *held = filter_call(rows, tap_rows(taps))
    first, stats = reduce_call(y0, sums, held, total)
    return normalize_call(pairs, stats, first, rest)


def solution(mesh):
    devices = mesh.devices
    finer = Mesh(
        devices.reshape(mesh.shape["band"], 8, 8, 2), ("band", "tm_0", "tm_1", "tm_2")
    )
    return jax.shard_map(
        on_device,
        mesh=finer,
        in_specs=(P("band", None, TM), P(), P()),
        out_specs=(P("band", None), P(None, "band", TM, None)),
        check_vma=False,
    )
```

```python
import functools
import math

import jax
import jax.numpy as jnp
import numpy as np
from jax import lax
from jax.experimental import pallas as pl
from jax.experimental.pallas import tpu as pltpu
from jax.sharding import Mesh
from jax.sharding import PartitionSpec as P

TM = ("tm_0", "tm_1", "tm_2")
ROWS = 32
LANES = 128
PITCH = 65
HALO = 16
GROUP = 8


def fill_tables(wh, wl, twc, tws):
    row = lax.broadcasted_iota(jnp.int32, (LANES, LANES), 0)
    k = lax.broadcasted_iota(jnp.int32, (LANES, LANES), 1)
    j = 4 * (row & 31) + (row >> 5)
    angle = ((j * k) & (LANES - 1)).astype(jnp.float32) * np.float32(2.0 * math.pi / LANES)
    cos, sin = jnp.cos(angle) * np.float32(1 / 64), jnp.sin(angle) * np.float32(1 / 64)
    low, high = slice(0, LANES), slice(LANES, 2 * LANES)
    for rows, cols, value in (
        (low, low, cos), (low, high, -sin), (high, low, sin), (high, high, cos),
    ):
        head = value.astype(jnp.bfloat16)
        wh[rows, cols] = head
        wl[rows, cols] = (value - head.astype(jnp.float32)).astype(jnp.bfloat16)
    i = lax.broadcasted_iota(jnp.int32, (ROWS, LANES), 0)
    k = lax.broadcasted_iota(jnp.int32, (ROWS, LANES), 1)
    turn = (i * k).astype(jnp.float32) * np.float32(2.0 * math.pi / 4096)
    twc[...] = jnp.cos(turn)
    tws[...] = jnp.sin(turn)


def add(a, b):
    return (a[0] + b[0], a[1] + b[1])


def sub(a, b):
    return (a[0] - b[0], a[1] - b[1])


def fft4(x):
    a, b = add(x[0], x[2]), sub(x[0], x[2])
    c, d = add(x[1], x[3]), sub(x[1], x[3])
    return [
        add(a, c),
        (b[0] + d[1], b[1] - d[0]),
        sub(a, c),
        (b[0] - d[1], b[1] + d[0]),
    ]


def fft8(x):
    even = fft4(x[0::2])
    odd = fft4(x[1::2])
    r = np.float32(math.sqrt(0.5))
    turned = [
        odd[0],
        ((odd[1][0] + odd[1][1]) * r, (odd[1][1] - odd[1][0]) * r),
        (odd[2][1], -odd[2][0]),
        ((odd[3][1] - odd[3][0]) * r, (odd[3][0] + odd[3][1]) * -r),
    ]
    return [add(e, o) for e, o in zip(even, turned)] + [sub(e, o) for e, o in zip(even, turned)]


def rotate(x, index, length):
    index = index % length
    if index == 0:
        return x
    if index * 4 == length:
        return (x[1], -x[0])
    c = np.float32(math.cos(2 * math.pi * index / length))
    s = np.float32(math.sin(2 * math.pi * index / length))
    return (x[0] * c + x[1] * s, x[1] * c - x[0] * s)


def block_transpose(rows):
    turned = rows.T
    lane = lax.broadcasted_iota(jnp.int32, (32, LANES), 1)
    odd = (lane & 32) != 0
    upper = (lane & 64) != 0
    r = [turned[32 * b : 32 * b + 32] for b in range(4)]

    def pair(a, b, by, mask):
        return (
            jnp.where(mask, pltpu.roll(b, by, 1), a),
            jnp.where(mask, b, pltpu.roll(a, LANES - by, 1)),
        )

    a0, a1 = pair(r[0], r[1], 32, odd)
    b0, b1 = pair(r[2], r[3], 32, odd)
    o0, o2 = pair(a0, b0, 64, upper)
    o1, o3 = pair(a1, b1, 64, upper)
    return [o0, o1, o2, o3]


def permute_taps(taps_ref, tapb):
    def batch(tb, carry):
        high = tb // 2
        parts = [
            taps_ref[pl.ds(high * 256 + (tb % 2) * 4 + q, 32, stride=8), :] for q in range(4)
        ]
        out = block_transpose(jnp.concatenate(parts, axis=0))
        for q in range(4):
            for i in range(ROWS):
                tapb[pl.ds(pl.multiple_of((i * 16 + tb * 4 + q) * 8, 8), 8), :] = jnp.broadcast_to(
                    out[q][i : i + 1], (8, LANES)
                )
        return carry

    lax.fori_loop(0, 4, batch, 0)


def permute_batch(raw, xf, b, row0):
    for c in range(2):
        x = [raw[s, pl.ds(b * 256 + c, LANES, stride=2), :] for s in range(4)]
        packed = (
            (x[0] & 255) | ((x[1] & 255) << 8) | ((x[2] & 255) << 16) | (x[3] << 24)
        )
        out = block_transpose(packed)
        for q in range(4):
            for s in range(4):
                value = out[q] << (24 - 8 * s) if s < 3 else out[q]
                value = (value >> 24).astype(jnp.float32)
                xf[2 * s + c, pl.ds(row0 + 4 * b + q, 32, stride=PITCH), :] = value


def order_of(i):
    return lax.rem(i, 4) * 8 + i // 4


def fir(xf, tapb, first, parts, extend=False):
    groups = len(parts)
    lowest = min(p[0] for p in parts)
    highest = max(p[1] for p in parts)

    def body(i, carry):
        base = i * PITCH + HALO + first * GROUP
        place = order_of(i)
        tap = {
            t: tapb[pl.ds(pl.multiple_of((i * 16 + t) * 8, 8), 8), :]
            for t in range(lowest, highest)
        }
        for s in range(4):
            at = [
                pl.ds(pl.multiple_of((p[3] * 128 + s * 32 + place) * 8, 8), 8) for p in parts
            ]
            cols = [slice(c * LANES, (c + 1) * LANES) for c in range(2)]
            acc = [
                [p[2][at[g], cols[c]] if extend else None for c in range(2)]
                for g, p in enumerate(parts)
            ]
            for w in range(1 - highest, 8 * (groups - 1) - lowest + 1):
                users = [g for g, p in enumerate(parts) if p[0] <= 8 * g - w < p[1]]
                if not users:
                    continue
                x = [xf[2 * s + c, pl.ds(base + w, 8), :] for c in range(2)]
                for g in users:
                    for c in range(2):
                        term = tap[8 * g - w] * x[c]
                        acc[g][c] = term if acc[g][c] is None else acc[g][c] + term
            for g, p in enumerate(parts):
                for c in range(2):
                    p[2][at[g], cols[c]] = acc[g][c]
        return carry

    lax.fori_loop(0, ROWS, body, 0)


def transform(refs, row_group, groups, fresh=False):
    (y, wh, wl, twc, tws, v, u, pbuf, sums) = refs

    def stage1(m, carry):
        at = pl.ds(pl.multiple_of(m * 1024, 1024), 1024)
        x = y[at, :]
        h = x.astype(jnp.bfloat16)
        l = (x - h.astype(jnp.float32)).astype(jnp.bfloat16)
        dot = functools.partial(jnp.dot, preferred_element_type=jnp.float32)
        v[at, :] = dot(h, wh[...]) + dot(l, wh[...]) + dot(h, wl[...])
        return carry

    lax.fori_loop(0, groups, stage1, 0)

    def tile(n):
        return pl.ds(pl.multiple_of(n * 8, 8), 8)

    def stage2a(gs, carry):
        for i0 in range(4):
            xs = []
            for i1 in range(8):
                i = 4 * i1 + i0
                at = tile(gs * 32 + i0 * 8 + i1)
                x = (v[at, :LANES], v[at, LANES:])
                if i:
                    c = jnp.broadcast_to(twc[i : i + 1, :], (8, LANES))
                    d = jnp.broadcast_to(tws[i : i + 1, :], (8, LANES))
                    x = (x[0] * c + x[1] * d, x[1] * c - x[0] * d)
                xs.append(x)
            for ka, x in enumerate(fft8(xs)):
                x = rotate(x, i0 * ka, 32)
                at = tile(gs * 37 + i0 * 9 + ka)
                u[0, at, :] = x[0]
                u[1, at, :] = x[1]
        return carry

    lax.fori_loop(0, 4 * groups, stage2a, 0)

    def stage2b(n, carry, fresh=False):
        g = n // 8
        ka = lax.rem(n, 8)
        rows = tile(row_group + g)

        def tally(q, value):
            sums[q, at, :] = value if fresh else sums[q, at, :] + value

        spectra = []
        for s in range(4):
            xs = []
            for i0 in range(4):
                at = tile((g * 4 + s) * 37 + i0 * 9 + ka)
                xs.append((u[0, at, :], u[1, at, :]))
            spectra.append(fft4(xs))
        for kb in range(4):
            k1 = ka + 8 * kb
            z = [spectra[s][kb] for s in range(4)]
            at = tile(k1)
            for s in range(4):
                tally(s, z[s][0] * z[s][0] + z[s][1] * z[s][1])
            cols = pl.ds(pl.multiple_of(k1 * LANES, LANES), LANES)
            for p in range(4):
                a, b = z[p // 2], z[2 + p % 2]
                re = a[0] * b[0] + a[1] * b[1]
                im = a[1] * b[0] - a[0] * b[1]
                tally(4 + p, re)
                tally(8 + p, im)
                pbuf[0, p, rows, cols] = re
                pbuf[1, p, rows, cols] = im
        return carry

    if fresh:
        lax.fori_loop(0, 8, functools.partial(stage2b, fresh=True), 0)
    if groups > 1 or not fresh:
        lax.fori_loop(8 if fresh else 0, 8 * groups, stage2b, 0)


HALF = ROWS // 2


class Ring:
    def __init__(self, half, a, b):
        self.half, self.a, self.b, self.c = half, a, b, TM[2]
        self.na, self.nb, self.nc = (lax.axis_size(n) for n in (a, b, self.c))
        self.members = self.na * self.nc
        self.per = HALF // self.members
        far = sorted(range(self.na), key=lambda d: -min(d, self.na - d))
        self.steps = [(d, e) for d in far for e in range(self.nc) if (d, e) != (0, 0)]
        self.shifts = sorted(range(1, self.nb), key=lambda d: -min(d, self.nb - d))

    def member(self, d=0, e=0):
        at = lax.rem(lax.axis_index(self.a) + d, self.na)
        core = lax.rem(lax.axis_index(self.c) + e, self.nc)
        return at * self.nc + core

    def member_id(self, d, e):
        return {
            self.a: lax.rem(lax.axis_index(self.a) + d, self.na),
            self.c: lax.rem(lax.axis_index(self.c) + e, self.nc),
        }

    def column_id(self, d):
        return {self.b: lax.rem(lax.axis_index(self.b) + d, self.nb)}


def rings():
    return (Ring(0, TM[1], TM[0]), Ring(1, TM[0], TM[1]))


def remote(src, dst, send, recv, to):
    return pltpu.make_async_remote_copy(
        src_ref=src,
        dst_ref=dst,
        send_sem=send,
        recv_sem=recv,
        device_id=to,
        device_id_type=pl.DeviceIdType.MESH,
    )


def all_reduce(total, sums, more, stats_ref, scratch, ready):
    both = rings()
    work = []
    for ring in both:
        part, rows_in, mine, cols_in, stat, sems = scratch[ring.half]
        work.append((ring, part, rows_in, mine, cols_in, stat, sems))

    def row_copy(job, n):
        ring, part, rows_in, _, _, _, sems = job
        d, e = ring.steps[n]
        return remote(
            part.at[ring.member(d, e)], rows_in.at[n], sems.at[0], sems.at[1],
            ring.member_id(d, e),
        )

    def col_copy(job, n):
        ring, _, _, mine, cols_in, _, sems = job
        return remote(
            mine, cols_in.at[n], sems.at[2], sems.at[3], ring.column_id(ring.shifts[n])
        )

    def place(ring):
        return pl.ds(HALF * ring.half + ring.member() * ring.per, ring.per)

    def gather_copy(job, n):
        ring, _, _, _, _, stat, sems = job
        return remote(
            stat, stats_ref.at[place(ring)], sems.at[4], sems.at[5],
            ring.member_id(*ring.steps[n]),
        )

    def whole(job, kind):
        ring, _, rows_in, _, cols_in, _, sems = job
        if kind == 2:
            ref = stats_ref.at[pl.ds(0, (ring.members - 1) * ring.per)]
        else:
            ref = cols_in if kind else rows_in
        return remote(
            ref, ref, sems.at[2 * kind], sems.at[2 * kind + 1], ring.member_id(*ring.steps[0])
        )

    for job in work:
        ring, part = job[:2]
        for k in range(HALF):
            k1 = HALF * ring.half + k
            for j in range(3):
                part[k // ring.per, k % ring.per, j] = jnp.concatenate(
                    [
                        jnp.sum(
                            sums[4 * j + q, k1 * 8 : k1 * 8 + 8, :]
                            + more[4 * j + q, k1 * 8 : k1 * 8 + 8, :],
                            axis=0,
                            keepdims=True,
                        )
                        for q in range(4)
                    ],
                    axis=0,
                )
        if ring.half == 0:
            ready()
        for n in range(len(ring.steps)):
            row_copy(job, n).start()

    totals = []
    for job in work:
        ring, part, rows_in, mine = job[:4]
        acc = part[ring.member()]
        whole(job, 0).wait_recv()
        for n in range(len(ring.steps)):
            acc = acc + rows_in[n]
        mine[...] = acc
        for n in range(len(ring.shifts)):
            col_copy(job, n).start()
        totals.append(acc)

    for job, acc in zip(work, totals):
        ring, _, _, _, cols_in, stat, _ = job
        if ring.shifts:
            whole(job, 1).wait_recv()
        for n in range(len(ring.shifts)):
            acc = acc + cols_in[n]
        mean = acc * np.float32(1.0 / total)
        for r in range(ring.per):
            power, re, im = mean[r, 0], mean[r, 1], mean[r, 2]
            raised = power + 1e-06
            denom = jnp.concatenate(
                [raised[p // 2 : p // 2 + 1] * raised[2 + p % 2 : 3 + p % 2] for p in range(4)],
                axis=0,
            )
            stat[r, 0] = power
            stat[r, 1] = (re * re + im * im) / denom
        for n in range(len(ring.steps)):
            gather_copy(job, n).start()
        stats_ref[place(ring)] = stat[...]

    for job in work:
        whole(job, 2).wait_recv()
    for job in work:
        whole(job, 0).wait_send()
        if job[0].shifts:
            whole(job, 1).wait_send()
        whole(job, 2).wait_send()


def filter_kernel(
    samples_ref, taps_ref,
    prod_ref, y0_ref, sums, wh, wl, twc, tws,
    raw, hraw, xf, tapb, y, v, u, in_sems, halo_send, halo_recv,
):
    x_name, y_name, c_name = TM
    nx, ny, nc = (lax.axis_size(n) for n in TM)
    me = [lax.axis_index(n) for n in TM]
    place = (me[0] * ny + me[1]) * nc + me[2]
    has_next = place < nx * ny * nc - 1
    has_prev = place > 0

    def tm_id(index):
        return {
            x_name: index // (ny * nc),
            y_name: lax.rem(index // nc, ny),
            c_name: lax.rem(index, nc),
        }

    barrier = pltpu.get_barrier_semaphore()

    @pl.when(has_prev)
    def _():
        pl.semaphore_signal(
            barrier, inc=1, device_id=tm_id(place - 1), device_id_type=pl.DeviceIdType.MESH
        )

    frames = samples_ref.shape[1] // 64

    def halo_copy(b):
        lead = 1 if b == 0 else 0
        at = (4 * b + lead) * 64
        size = (4 - lead) * 64
        start = (frames - HALO) * 64 + at
        return remote(
            samples_ref.at[:, pl.ds(start, size), :], hraw.at[:, pl.ds(at, size), :],
            halo_send.at[b], halo_recv.at[b], tm_id(place + 1),
        )

    def in_copy(b):
        rows = pl.ds(pl.multiple_of(b * 256, 256), 256)
        return pltpu.make_async_copy(samples_ref.at[:, rows, :], raw.at[:, rows, :], in_sems.at[b])

    for b in range(12):
        in_copy(b).start()

    @pl.when(has_next)
    def _():
        pl.semaphore_wait(barrier, 1)
        for b in (3, 2, 1, 0):
            halo_copy(b).start()

    @pl.when(jnp.logical_not(has_prev))
    def _():
        hraw[...] = jnp.zeros_like(hraw)

    def halo_wait(b):
        @pl.when(has_prev)
        def _():
            halo_copy(b).wait_recv()

    refs = (y, wh, wl, twc, tws, v, u, prod_ref, sums)
    fill_tables(wh, wl, twc, tws)
    permute_taps(taps_ref, tapb)

    def own_batch(b, carry):
        in_copy(b).wait()
        permute_batch(raw, xf, b, HALO)
        return carry

    lax.fori_loop(0, 12, own_batch, 0)

    fir(xf, tapb, 2, [(0, 16, y, g) for g in range(4)])
    transform(refs, 1, 4, fresh=True)

    halo_wait(3)
    halo_wait(2)
    permute_batch(hraw, xf, 3, 0)
    permute_batch(hraw, xf, 2, 0)
    fir(xf, tapb, 0, [(0, 9, y0_ref, 0), (0, 16, y, 0)])
    transform(refs, 0, 1)

    halo_wait(1)
    permute_batch(hraw, xf, 1, 0)
    halo_wait(0)
    permute_batch(hraw, xf, 0, 0)
    fir(xf, tapb, 0, [(9, 16, y0_ref, 0)], extend=True)

    @pl.when(has_next)
    def _():
        for b in range(4):
            halo_copy(b).wait_send()


def reduce_kernel(
    total, y0, sums_ref, wh, wl, twc, tws, prod_ref, stats_ref,
    v, u, sums, part0, rows0, mine0, cols0, stat0, sems0,
    part1, rows1, mine1, cols1, stat1, sems1,
):
    barrier = pltpu.get_barrier_semaphore()
    greeted = 0
    for ring in rings():
        for d, e in ring.steps:
            if ring.half == 1 and d == 0:
                continue
            pl.semaphore_signal(
                barrier,
                inc=1,
                device_id=ring.member_id(d, e),
                device_id_type=pl.DeviceIdType.MESH,
            )
            greeted += 1

    transform((y0, wh, wl, twc, tws, v, u, prod_ref, sums), 0, 1, fresh=True)
    all_reduce(
        total, sums, sums_ref, stats_ref,
        (
            (part0, rows0, mine0, cols0, stat0, sems0),
            (part1, rows1, mine1, cols1, stat1, sems1),
        ),
        lambda: pl.semaphore_wait(barrier, greeted),
    )


VMEM_ALL = pl.BlockSpec(memory_space=pltpu.VMEM)
ANYWHERE = pl.BlockSpec(memory_space=pl.ANY)
WIDE = 4096 + LANES
MIB = 1024 * 1024


def filter_call(rows, taps_rows):
    frames = rows.shape[1] // 64
    f32, i32 = jnp.float32, jnp.int32
    dma = pltpu.SemaphoreType.DMA
    return pl.pallas_call(
        filter_kernel,
        out_shape=(
            jax.ShapeDtypeStruct((2, 4, frames - GROUP, WIDE), f32),
            jax.ShapeDtypeStruct((1024, 256), f32),
            jax.ShapeDtypeStruct((12, (ROWS + 1) * 8, LANES), f32),
            *[jax.ShapeDtypeStruct((256, 256), jnp.bfloat16)] * 2,
            *[jax.ShapeDtypeStruct((ROWS, LANES), f32)] * 2,
        ),
        in_specs=[ANYWHERE, VMEM_ALL],
        out_specs=(VMEM_ALL,) * 7,
        scratch_shapes=[
            pltpu.VMEM((4, frames * 64, LANES), i32),
            pltpu.VMEM((4, HALO * 64, LANES), i32),
            pltpu.VMEM((8, ROWS * PITCH + 7, LANES), f32),
            pltpu.VMEM((ROWS * 16 * 8, LANES), f32),
            pltpu.VMEM((4096, 256), f32),
            pltpu.VMEM((4096, 256), f32),
            pltpu.VMEM((2, 16 * 37 * 8 + 16, LANES), f32),
            dma((12,)),
            dma((4,)),
            dma((4,)),
        ],
        compiler_params=pltpu.CompilerParams(
            vmem_limit_bytes=45 * MIB, collective_id=0, has_side_effects=True
        ),
        cost_estimate=pl.CostEstimate(
            flops=4_000_000_000, bytes_accessed=16_000_000, transcendentals=0
        ),
        name="filter",
    )(rows, taps_rows)


def reduce_call(y0, sums, consts, total):
    f32 = jnp.float32
    dma = pltpu.SemaphoreType.DMA
    exchange = []
    for ring in rings():
        exchange += [
            pltpu.VMEM((ring.members, ring.per, 3, 4, LANES), f32),
            pltpu.VMEM((ring.members - 1, ring.per, 3, 4, LANES), f32),
            pltpu.VMEM((ring.per, 3, 4, LANES), f32),
            pltpu.VMEM((max(ring.nb - 1, 1), ring.per, 3, 4, LANES), f32),
            pltpu.VMEM((ring.per, 2, 4, LANES), f32),
            dma((6,)),
        ]
    return pl.pallas_call(
        functools.partial(reduce_kernel, total),
        out_shape=(
            jax.ShapeDtypeStruct((2, 4, GROUP, WIDE), f32),
            jax.ShapeDtypeStruct((ROWS, 2, 4, LANES), f32),
        ),
        in_specs=[VMEM_ALL] * 6,
        out_specs=(VMEM_ALL, VMEM_ALL),
        scratch_shapes=[
            pltpu.VMEM((1024, 256), f32),
            pltpu.VMEM((2, 4 * 37 * 8 + 16, LANES), f32),
            pltpu.VMEM((12, (ROWS + 1) * 8, LANES), f32),
            *exchange,
        ],
        compiler_params=pltpu.CompilerParams(
            vmem_limit_bytes=16 * MIB, collective_id=1, has_side_effects=True
        ),
        cost_estimate=pl.CostEstimate(
            flops=400_000_000, bytes_accessed=3_000_000, transcendentals=0
        ),
        name="reduce",
    )(y0, sums, *consts)


def normalize_kernel(pairs_ref, stats_ref, first_ref, rest_ref, coh_ref, out_ref, buf, writes):
    frames = buf.shape[2]

    def write(p, part):
        return pltpu.make_async_copy(
            buf.at[p, part], out_ref.at[part, p], writes.at[2 * p + part]
        )

    def stat(q):
        return stats_ref[pl.ds(q, ROWS, stride=8), :]

    def pair(p, carry):
        which = pairs_ref[0, p] * 2 + pairs_ref[1, p] - 2
        power = (stat(pairs_ref[0, p]) + 1e-06) * (stat(pairs_ref[1, p]) + 1e-06)
        factor = 1.0 / jnp.sqrt(power)
        for part in range(2):
            for k1 in range(ROWS):
                cols = slice(k1 * LANES, (k1 + 1) * LANES)
                row = factor[k1 : k1 + 1]
                buf[p, part, 0:GROUP, cols] = first_ref[part, which, :, cols] * row
                buf[p, part, GROUP:frames, cols] = rest_ref[part, which, :, cols] * row
            write(p, part).start()
        return carry

    lax.fori_loop(0, 4, pair, 0)
    for p in range(4):
        value = stat(4 + pairs_ref[0, p] * 2 + pairs_ref[1, p] - 2)
        for k1 in range(ROWS):
            coh_ref[p : p + 1, k1 * LANES : (k1 + 1) * LANES] = value[k1 : k1 + 1]
    for p in range(4):
        for part in range(2):
            write(p, part).wait()


def normalize_call(pairs, stats, first, rest):
    frames = first.shape[2] + rest.shape[2]
    f32 = jnp.float32
    return pl.pallas_call(
        normalize_kernel,
        in_specs=[pl.BlockSpec(memory_space=pltpu.SMEM)] + [VMEM_ALL] * 3,
        out_specs=(VMEM_ALL, ANYWHERE),
        out_shape=(
            jax.ShapeDtypeStruct((4, 4096), f32),
            jax.ShapeDtypeStruct((2, 4, frames, 4096), f32),
        ),
        scratch_shapes=[
            pltpu.VMEM((4, 2, frames, 4096), f32),
            pltpu.SemaphoreType.DMA((8,)),
        ],
        compiler_params=pltpu.CompilerParams(vmem_limit_bytes=20 * MIB),
        cost_estimate=pl.CostEstimate(flops=2_000_000, bytes_accessed=13_000_000, transcendentals=0),
        name="normalize",
    )(pairs.T, stats.reshape(-1, LANES), first, rest)


def sample_rows(volts):
    streams, comps, local = volts.shape
    rows = volts.reshape(streams, comps, local // LANES, LANES)
    return jnp.transpose(rows, (0, 2, 1, 3)).reshape(streams, local // LANES * comps, LANES)


def tap_rows(taps):
    taps = taps.reshape(2, 8, ROWS, LANES)
    return jnp.transpose(taps, (0, 2, 1, 3)).reshape(512, LANES)


def on_device(volts, taps, pairs):
    rows = sample_rows(volts)
    total = rows.shape[1] // 64 * lax.axis_size(TM)
    rest, y0, sums, *held = filter_call(rows, tap_rows(taps))
    first, stats = reduce_call(y0, sums, held, total)
    return normalize_call(pairs, stats, first, rest)


def solution(mesh):
    devices = mesh.devices
    finer = Mesh(
        devices.reshape(mesh.shape["band"], 8, 8, 2), ("band", "tm_0", "tm_1", "tm_2")
    )
    return jax.shard_map(
        on_device,
        mesh=finer,
        in_specs=(P("band", None, TM), P(), P()),
        out_specs=(P("band", None), P(None, "band", TM, None)),
        check_vma=False,
    )
```

```python
import functools
import math

import jax
import jax.numpy as jnp
import numpy as np
from jax import lax
from jax.experimental import pallas as pl
from jax.experimental.pallas import tpu as pltpu
from jax.sharding import Mesh
from jax.sharding import PartitionSpec as P

TM = ("tm_0", "tm_1", "tm_2")
ROWS = 32
LANES = 128
PITCH = 65
HALO = 16
GROUP = 8


def fill_tables(wh, wl, twc, tws):
    row = lax.broadcasted_iota(jnp.int32, (LANES, LANES), 0)
    k = lax.broadcasted_iota(jnp.int32, (LANES, LANES), 1)
    j = 4 * (row & 31) + (row >> 5)
    angle = ((j * k) & (LANES - 1)).astype(jnp.float32) * np.float32(2.0 * math.pi / LANES)
    cos, sin = jnp.cos(angle) * np.float32(1 / 64), jnp.sin(angle) * np.float32(1 / 64)
    low, high = slice(0, LANES), slice(LANES, 2 * LANES)
    for rows, cols, value in (
        (low, low, cos), (low, high, -sin), (high, low, sin), (high, high, cos),
    ):
        head = value.astype(jnp.bfloat16)
        wh[rows, cols] = head
        wl[rows, cols] = (value - head.astype(jnp.float32)).astype(jnp.bfloat16)
    i = lax.broadcasted_iota(jnp.int32, (ROWS, LANES), 0)
    k = lax.broadcasted_iota(jnp.int32, (ROWS, LANES), 1)
    turn = (i * k).astype(jnp.float32) * np.float32(2.0 * math.pi / 4096)
    twc[...] = jnp.cos(turn)
    tws[...] = jnp.sin(turn)


def add(a, b):
    return (a[0] + b[0], a[1] + b[1])


def sub(a, b):
    return (a[0] - b[0], a[1] - b[1])


def fft4(x):
    a, b = add(x[0], x[2]), sub(x[0], x[2])
    c, d = add(x[1], x[3]), sub(x[1], x[3])
    return [
        add(a, c),
        (b[0] + d[1], b[1] - d[0]),
        sub(a, c),
        (b[0] - d[1], b[1] + d[0]),
    ]


def fft8(x):
    even = fft4(x[0::2])
    odd = fft4(x[1::2])
    r = np.float32(math.sqrt(0.5))
    turned = [
        odd[0],
        ((odd[1][0] + odd[1][1]) * r, (odd[1][1] - odd[1][0]) * r),
        (odd[2][1], -odd[2][0]),
        ((odd[3][1] - odd[3][0]) * r, (odd[3][0] + odd[3][1]) * -r),
    ]
    return [add(e, o) for e, o in zip(even, turned)] + [sub(e, o) for e, o in zip(even, turned)]


def rotate(x, index, length):
    index = index % length
    if index == 0:
        return x
    if index * 4 == length:
        return (x[1], -x[0])
    c = np.float32(math.cos(2 * math.pi * index / length))
    s = np.float32(math.sin(2 * math.pi * index / length))
    return (x[0] * c + x[1] * s, x[1] * c - x[0] * s)


def block_transpose(rows):
    turned = rows.T
    lane = lax.broadcasted_iota(jnp.int32, (32, LANES), 1)
    odd = (lane & 32) != 0
    upper = (lane & 64) != 0
    r = [turned[32 * b : 32 * b + 32] for b in range(4)]

    def pair(a, b, by, mask):
        return (
            jnp.where(mask, pltpu.roll(b, by, 1), a),
            jnp.where(mask, b, pltpu.roll(a, LANES - by, 1)),
        )

    a0, a1 = pair(r[0], r[1], 32, odd)
    b0, b1 = pair(r[2], r[3], 32, odd)
    o0, o2 = pair(a0, b0, 64, upper)
    o1, o3 = pair(a1, b1, 64, upper)
    return [o0, o1, o2, o3]


def permute_taps(taps_ref, tapb):
    def batch(tb, carry):
        high = tb // 2
        parts = [
            taps_ref[pl.ds(high * 256 + (tb % 2) * 4 + q, 32, stride=8), :] for q in range(4)
        ]
        out = block_transpose(jnp.concatenate(parts, axis=0))
        for q in range(4):
            for i in range(ROWS):
                tapb[pl.ds(pl.multiple_of((i * 16 + tb * 4 + q) * 8, 8), 8), :] = jnp.broadcast_to(
                    out[q][i : i + 1], (8, LANES)
                )
        return carry

    lax.fori_loop(0, 4, batch, 0)


def permute_batch(raw, xf, b, row0):
    for c in range(2):
        x = [raw[s, pl.ds(b * 256 + c, LANES, stride=2), :] for s in range(4)]
        packed = (
            (x[0] & 255) | ((x[1] & 255) << 8) | ((x[2] & 255) << 16) | (x[3] << 24)
        )
        out = block_transpose(packed)
        for q in range(4):
            for s in range(4):
                value = out[q] << (24 - 8 * s) if s < 3 else out[q]
                value = (value >> 24).astype(jnp.float32)
                xf[2 * s + c, pl.ds(row0 + 4 * b + q, 32, stride=PITCH), :] = value


def order_of(i):
    return lax.rem(i, 4) * 8 + i // 4


def fir(xf, tapb, first, parts, extend=False):
    groups = len(parts)
    lowest = min(p[0] for p in parts)
    highest = max(p[1] for p in parts)

    def body(i, carry):
        base = i * PITCH + HALO + first * GROUP
        place = order_of(i)
        tap = {
            t: tapb[pl.ds(pl.multiple_of((i * 16 + t) * 8, 8), 8), :]
            for t in range(lowest, highest)
        }
        for s in range(4):
            at = [
                pl.ds(pl.multiple_of((p[3] * 128 + s * 32 + place) * 8, 8), 8) for p in parts
            ]
            cols = [slice(c * LANES, (c + 1) * LANES) for c in range(2)]
            acc = [
                [p[2][at[g], cols[c]] if extend else None for c in range(2)]
                for g, p in enumerate(parts)
            ]
            for w in range(1 - highest, 8 * (groups - 1) - lowest + 1):
                users = [g for g, p in enumerate(parts) if p[0] <= 8 * g - w < p[1]]
                if not users:
                    continue
                x = [xf[2 * s + c, pl.ds(base + w, 8), :] for c in range(2)]
                for g in users:
                    for c in range(2):
                        term = tap[8 * g - w] * x[c]
                        acc[g][c] = term if acc[g][c] is None else acc[g][c] + term
            for g, p in enumerate(parts):
                for c in range(2):
                    p[2][at[g], cols[c]] = acc[g][c]
        return carry

    lax.fori_loop(0, ROWS, body, 0)


def transform(refs, row_group, groups, fresh=False):
    (y, wh, wl, twc, tws, v, u, pbuf, sums) = refs

    def stage1(m, carry):
        at = pl.ds(pl.multiple_of(m * 1024, 1024), 1024)
        x = y[at, :]
        h = x.astype(jnp.bfloat16)
        l = (x - h.astype(jnp.float32)).astype(jnp.bfloat16)
        dot = functools.partial(jnp.dot, preferred_element_type=jnp.float32)
        v[at, :] = dot(h, wh[...]) + dot(l, wh[...]) + dot(h, wl[...])
        return carry

    lax.fori_loop(0, groups, stage1, 0)

    def tile(n):
        return pl.ds(pl.multiple_of(n * 8, 8), 8)

    def stage2a(gs, carry):
        for i0 in range(4):
            xs = []
            for i1 in range(8):
                i = 4 * i1 + i0
                at = tile(gs * 32 + i0 * 8 + i1)
                x = (v[at, :LANES], v[at, LANES:])
                if i:
                    c = jnp.broadcast_to(twc[i : i + 1, :], (8, LANES))
                    d = jnp.broadcast_to(tws[i : i + 1, :], (8, LANES))
                    x = (x[0] * c + x[1] * d, x[1] * c - x[0] * d)
                xs.append(x)
            for ka, x in enumerate(fft8(xs)):
                x = rotate(x, i0 * ka, 32)
                at = tile(gs * 37 + i0 * 9 + ka)
                u[0, at, :] = x[0]
                u[1, at, :] = x[1]
        return carry

    lax.fori_loop(0, 4 * groups, stage2a, 0)

    def stage2b(n, carry, fresh=False):
        g = n // 8
        ka = lax.rem(n, 8)
        rows = tile(row_group + g)

        def tally(q, value):
            sums[q, at, :] = value if fresh else sums[q, at, :] + value

        spectra = []
        for s in range(4):
            xs = []
            for i0 in range(4):
                at = tile((g * 4 + s) * 37 + i0 * 9 + ka)
                xs.append((u[0, at, :], u[1, at, :]))
            spectra.append(fft4(xs))
        for kb in range(4):
            k1 = ka + 8 * kb
            z = [spectra[s][kb] for s in range(4)]
            at = tile(k1)
            for s in range(4):
                tally(s, z[s][0] * z[s][0] + z[s][1] * z[s][1])
            cols = pl.ds(pl.multiple_of(k1 * LANES, LANES), LANES)
            for p in range(4):
                a, b = z[p // 2], z[2 + p % 2]
                re = a[0] * b[0] + a[1] * b[1]
                im = a[1] * b[0] - a[0] * b[1]
                tally(4 + p, re)
                tally(8 + p, im)
                pbuf[0, p, rows, cols] = re
                pbuf[1, p, rows, cols] = im
        return carry

    if fresh:
        lax.fori_loop(0, 8, functools.partial(stage2b, fresh=True), 0)
    if groups > 1 or not fresh:
        lax.fori_loop(8 if fresh else 0, 8 * groups, stage2b, 0)


HALF = ROWS // 2


def turned(index, by, size):
    return lax.rem(index + by, size) if by else index


class Ring:
    def __init__(self, half, a, b):
        self.half, self.a, self.b, self.c = half, a, b, TM[2]
        self.na, self.nb, self.nc = (lax.axis_size(n) for n in (a, b, self.c))
        self.members = self.na * self.nc
        self.per = HALF // self.members
        far = sorted(range(self.na), key=lambda d: -min(d, self.na - d))
        self.steps = [(d, e) for d in far for e in range(self.nc) if (d, e) != (0, 0)]
        self.shifts = sorted(range(1, self.nb), key=lambda d: -min(d, self.nb - d))

    def member(self, d=0, e=0):
        at = turned(lax.axis_index(self.a), d, self.na)
        return at * self.nc + turned(lax.axis_index(self.c), e, self.nc)

    def member_id(self, d, e):
        return {
            self.a: turned(lax.axis_index(self.a), d, self.na),
            self.c: turned(lax.axis_index(self.c), e, self.nc),
        }

    def column_id(self, d):
        return {self.b: turned(lax.axis_index(self.b), d, self.nb)}


def rings():
    return (Ring(0, TM[1], TM[0]), Ring(1, TM[0], TM[1]))


def remote(src, dst, send, recv, to):
    return pltpu.make_async_remote_copy(
        src_ref=src,
        dst_ref=dst,
        send_sem=send,
        recv_sem=recv,
        device_id=to,
        device_id_type=pl.DeviceIdType.MESH,
    )


def all_reduce(total, sums, more, stats_ref, scratch, ready):
    both = rings()
    work = []
    for ring in both:
        part, rows_in, mine, cols_in, stat, sems = scratch[ring.half]
        work.append((ring, part, rows_in, mine, cols_in, stat, sems))

    def row_copy(job, n):
        ring, part, rows_in, _, _, _, sems = job
        d, e = ring.steps[n]
        return remote(
            part.at[ring.member(d, e)], rows_in.at[n], sems.at[0], sems.at[1],
            ring.member_id(d, e),
        )

    def col_copy(job, n):
        ring, _, _, mine, cols_in, _, sems = job
        return remote(
            mine, cols_in.at[n], sems.at[2], sems.at[3], ring.column_id(ring.shifts[n])
        )

    def place(ring):
        return pl.ds(HALF * ring.half + ring.member() * ring.per, ring.per)

    def gather_copy(job, n):
        ring, _, _, _, _, stat, sems = job
        return remote(
            stat, stats_ref.at[place(ring)], sems.at[4], sems.at[5],
            ring.member_id(*ring.steps[n]),
        )

    def whole(job, kind):
        ring, _, rows_in, _, cols_in, _, sems = job
        if kind == 2:
            ref = stats_ref.at[pl.ds(0, (ring.members - 1) * ring.per)]
        else:
            ref = cols_in if kind else rows_in
        return remote(
            ref, ref, sems.at[2 * kind], sems.at[2 * kind + 1], ring.member_id(*ring.steps[0])
        )

    for job in work:
        ring, part = job[:2]
        for k in range(HALF):
            k1 = HALF * ring.half + k
            for j in range(3):
                part[k // ring.per, k % ring.per, j] = jnp.concatenate(
                    [
                        jnp.sum(
                            sums[4 * j + q, k1 * 8 : k1 * 8 + 8, :]
                            + more[4 * j + q, k1 * 8 : k1 * 8 + 8, :],
                            axis=0,
                            keepdims=True,
                        )
                        for q in range(4)
                    ],
                    axis=0,
                )
        if ring.half == 0:
            ready()
        for n in range(len(ring.steps)):
            row_copy(job, n).start()

    totals = []
    for job in work:
        ring, part, rows_in, mine = job[:4]
        acc = part[ring.member()]
        whole(job, 0).wait_recv()
        for n in range(len(ring.steps)):
            acc = acc + rows_in[n]
        mine[...] = acc
        for n in range(len(ring.shifts)):
            col_copy(job, n).start()
        totals.append(acc)

    for job, acc in zip(work, totals):
        ring, _, _, _, cols_in, stat, _ = job
        if ring.shifts:
            whole(job, 1).wait_recv()
        for n in range(len(ring.shifts)):
            acc = acc + cols_in[n]
        mean = acc * np.float32(1.0 / total)
        for r in range(ring.per):
            power, re, im = mean[r, 0], mean[r, 1], mean[r, 2]
            raised = power + 1e-06
            denom = jnp.concatenate(
                [raised[p // 2 : p // 2 + 1] * raised[2 + p % 2 : 3 + p % 2] for p in range(4)],
                axis=0,
            )
            stat[r, 0] = power
            stat[r, 1] = (re * re + im * im) / denom
        for n in range(len(ring.steps)):
            gather_copy(job, n).start()
        stats_ref[place(ring)] = stat[...]

    for job in work:
        whole(job, 2).wait_recv()
    for job in work:
        whole(job, 0).wait_send()
        if job[0].shifts:
            whole(job, 1).wait_send()
        whole(job, 2).wait_send()


def filter_kernel(
    samples_ref, taps_ref,
    prod_ref, y0_ref, sums, wh, wl, twc, tws,
    raw, hraw, xf, tapb, y, v, u, in_sems, halo_send, halo_recv,
):
    x_name, y_name, c_name = TM
    nx, ny, nc = (lax.axis_size(n) for n in TM)
    me = [lax.axis_index(n) for n in TM]
    place = (me[0] * ny + me[1]) * nc + me[2]
    has_next = place < nx * ny * nc - 1
    has_prev = place > 0

    def tm_id(index):
        return {
            x_name: index // (ny * nc),
            y_name: lax.rem(index // nc, ny),
            c_name: lax.rem(index, nc),
        }

    barrier = pltpu.get_barrier_semaphore()

    @pl.when(has_prev)
    def _():
        pl.semaphore_signal(
            barrier, inc=1, device_id=tm_id(place - 1), device_id_type=pl.DeviceIdType.MESH
        )

    frames = samples_ref.shape[1] // 64

    def halo_copy(b):
        lead = 1 if b == 0 else 0
        at = (4 * b + lead) * 64
        size = (4 - lead) * 64
        start = (frames - HALO) * 64 + at
        return remote(
            samples_ref.at[:, pl.ds(start, size), :], hraw.at[:, pl.ds(at, size), :],
            halo_send.at[b], halo_recv.at[b], tm_id(place + 1),
        )

    def in_copy(b):
        rows = pl.ds(pl.multiple_of(b * 256, 256), 256)
        return pltpu.make_async_copy(samples_ref.at[:, rows, :], raw.at[:, rows, :], in_sems.at[b])

    for b in range(12):
        in_copy(b).start()

    @pl.when(has_next)
    def _():
        pl.semaphore_wait(barrier, 1)
        for b in (3, 2, 1, 0):
            halo_copy(b).start()

    @pl.when(jnp.logical_not(has_prev))
    def _():
        hraw[...] = jnp.zeros_like(hraw)

    def halo_wait(b):
        @pl.when(has_prev)
        def _():
            halo_copy(b).wait_recv()

    refs = (y, wh, wl, twc, tws, v, u, prod_ref, sums)
    fill_tables(wh, wl, twc, tws)
    permute_taps(taps_ref, tapb)

    def own_batch(b, carry):
        in_copy(b).wait()
        permute_batch(raw, xf, b, HALO)
        return carry

    lax.fori_loop(0, 12, own_batch, 0)

    fir(xf, tapb, 2, [(0, 16, y, g) for g in range(4)])
    transform(refs, 1, 4, fresh=True)

    halo_wait(3)
    halo_wait(2)
    permute_batch(hraw, xf, 3, 0)
    permute_batch(hraw, xf, 2, 0)
    fir(xf, tapb, 0, [(0, 9, y0_ref, 0), (0, 16, y, 0)])
    transform(refs, 0, 1)

    halo_wait(1)
    permute_batch(hraw, xf, 1, 0)
    halo_wait(0)
    permute_batch(hraw, xf, 0, 0)
    fir(xf, tapb, 0, [(9, 16, y0_ref, 0)], extend=True)

    @pl.when(has_next)
    def _():
        for b in range(4):
            halo_copy(b).wait_send()


def reduce_kernel(
    total, y0, sums_ref, wh, wl, twc, tws, prod_ref, stats_ref,
    v, u, sums, part0, rows0, mine0, cols0, stat0, sems0,
    part1, rows1, mine1, cols1, stat1, sems1,
):
    barrier = pltpu.get_barrier_semaphore()
    greeted = 0
    for ring in rings():
        for d, e in ring.steps:
            if ring.half == 1 and d == 0:
                continue
            pl.semaphore_signal(
                barrier,
                inc=1,
                device_id=ring.member_id(d, e),
                device_id_type=pl.DeviceIdType.MESH,
            )
            greeted += 1

    transform((y0, wh, wl, twc, tws, v, u, prod_ref, sums), 0, 1, fresh=True)
    all_reduce(
        total, sums, sums_ref, stats_ref,
        (
            (part0, rows0, mine0, cols0, stat0, sems0),
            (part1, rows1, mine1, cols1, stat1, sems1),
        ),
        lambda: pl.semaphore_wait(barrier, greeted),
    )


VMEM_ALL = pl.BlockSpec(memory_space=pltpu.VMEM)
ANYWHERE = pl.BlockSpec(memory_space=pl.ANY)
WIDE = 4096 + LANES
MIB = 1024 * 1024


def filter_call(rows, taps_rows):
    frames = rows.shape[1] // 64
    f32, i32 = jnp.float32, jnp.int32
    dma = pltpu.SemaphoreType.DMA
    return pl.pallas_call(
        filter_kernel,
        out_shape=(
            jax.ShapeDtypeStruct((2, 4, frames - GROUP, WIDE), f32),
            jax.ShapeDtypeStruct((1024, 256), f32),
            jax.ShapeDtypeStruct((12, (ROWS + 1) * 8, LANES), f32),
            *[jax.ShapeDtypeStruct((256, 256), jnp.bfloat16)] * 2,
            *[jax.ShapeDtypeStruct((ROWS, LANES), f32)] * 2,
        ),
        in_specs=[ANYWHERE, VMEM_ALL],
        out_specs=(VMEM_ALL,) * 7,
        scratch_shapes=[
            pltpu.VMEM((4, frames * 64, LANES), i32),
            pltpu.VMEM((4, HALO * 64, LANES), i32),
            pltpu.VMEM((8, ROWS * PITCH + 7, LANES), f32),
            pltpu.VMEM((ROWS * 16 * 8, LANES), f32),
            pltpu.VMEM((4096, 256), f32),
            pltpu.VMEM((4096, 256), f32),
            pltpu.VMEM((2, 16 * 37 * 8 + 16, LANES), f32),
            dma((12,)),
            dma((4,)),
            dma((4,)),
        ],
        compiler_params=pltpu.CompilerParams(
            vmem_limit_bytes=45 * MIB, collective_id=0, has_side_effects=True
        ),
        cost_estimate=pl.CostEstimate(
            flops=4_000_000_000, bytes_accessed=16_000_000, transcendentals=0
        ),
        name="filter",
    )(rows, taps_rows)


def reduce_call(y0, sums, consts, total):
    f32 = jnp.float32
    dma = pltpu.SemaphoreType.DMA
    exchange = []
    for ring in rings():
        exchange += [
            pltpu.VMEM((ring.members, ring.per, 3, 4, LANES), f32),
            pltpu.VMEM((ring.members - 1, ring.per, 3, 4, LANES), f32),
            pltpu.VMEM((ring.per, 3, 4, LANES), f32),
            pltpu.VMEM((max(ring.nb - 1, 1), ring.per, 3, 4, LANES), f32),
            pltpu.VMEM((ring.per, 2, 4, LANES), f32),
            dma((6,)),
        ]
    return pl.pallas_call(
        functools.partial(reduce_kernel, total),
        out_shape=(
            jax.ShapeDtypeStruct((2, 4, GROUP, WIDE), f32),
            jax.ShapeDtypeStruct((ROWS, 2, 4, LANES), f32),
        ),
        in_specs=[VMEM_ALL] * 6,
        out_specs=(VMEM_ALL, VMEM_ALL),
        scratch_shapes=[
            pltpu.VMEM((1024, 256), f32),
            pltpu.VMEM((2, 4 * 37 * 8 + 16, LANES), f32),
            pltpu.VMEM((12, (ROWS + 1) * 8, LANES), f32),
            *exchange,
        ],
        compiler_params=pltpu.CompilerParams(
            vmem_limit_bytes=16 * MIB, collective_id=1, has_side_effects=True
        ),
        cost_estimate=pl.CostEstimate(
            flops=400_000_000, bytes_accessed=3_000_000, transcendentals=0
        ),
        name="reduce",
    )(y0, sums, *consts)


def normalize_kernel(
    pairs_ref, stats_ref, first_ref, rest_ref, coh_out, out_ref, buf, coh_ref, writes, coh_sem
):
    frames = buf.shape[2]

    def write(p, part):
        return pltpu.make_async_copy(
            buf.at[p, part], out_ref.at[part, p], writes.at[2 * p + part]
        )

    def stat(q):
        return stats_ref[pl.ds(q, ROWS, stride=8), :]

    def pair(p, carry):
        which = pairs_ref[0, p] * 2 + pairs_ref[1, p] - 2
        power = (stat(pairs_ref[0, p]) + 1e-06) * (stat(pairs_ref[1, p]) + 1e-06)
        factor = 1.0 / jnp.sqrt(power)
        for part in range(2):
            for k1 in range(ROWS):
                cols = slice(k1 * LANES, (k1 + 1) * LANES)
                row = factor[k1 : k1 + 1]
                buf[p, part, 0:GROUP, cols] = first_ref[part, which, :, cols] * row
                buf[p, part, GROUP:frames, cols] = rest_ref[part, which, :, cols] * row
            write(p, part).start()
        return carry

    lax.fori_loop(0, 4, pair, 0)
    for p in range(4):
        value = stat(4 + pairs_ref[0, p] * 2 + pairs_ref[1, p] - 2)
        for k1 in range(ROWS):
            coh_ref[p : p + 1, k1 * LANES : (k1 + 1) * LANES] = value[k1 : k1 + 1]
    coh_copy = pltpu.make_async_copy(coh_ref, coh_out, coh_sem)
    coh_copy.start()
    for p in range(4):
        for part in range(2):
            write(p, part).wait()
    coh_copy.wait()


def normalize_call(pairs, stats, first, rest):
    frames = first.shape[2] + rest.shape[2]
    f32 = jnp.float32
    return pl.pallas_call(
        normalize_kernel,
        in_specs=[pl.BlockSpec(memory_space=pltpu.SMEM)] + [VMEM_ALL] * 3,
        out_specs=(ANYWHERE, ANYWHERE),
        out_shape=(
            jax.ShapeDtypeStruct((4, 4096), f32),
            jax.ShapeDtypeStruct((2, 4, frames, 4096), f32),
        ),
        scratch_shapes=[
            pltpu.VMEM((4, 2, frames, 4096), f32),
            pltpu.VMEM((4, 4096), f32),
            pltpu.SemaphoreType.DMA((8,)),
            pltpu.SemaphoreType.DMA,
        ],
        compiler_params=pltpu.CompilerParams(vmem_limit_bytes=20 * MIB),
        cost_estimate=pl.CostEstimate(flops=2_000_000, bytes_accessed=13_000_000, transcendentals=0),
        name="normalize",
    )(pairs.T, stats.reshape(-1, LANES), first, rest)


def sample_rows(volts):
    streams, comps, local = volts.shape
    rows = volts.reshape(streams, comps, local // LANES, LANES)
    return jnp.transpose(rows, (0, 2, 1, 3)).reshape(streams, local // LANES * comps, LANES)


def tap_rows(taps):
    taps = taps.reshape(2, 8, ROWS, LANES)
    return jnp.transpose(taps, (0, 2, 1, 3)).reshape(512, LANES)


def on_device(volts, taps, pairs):
    rows = sample_rows(volts)
    total = rows.shape[1] // 64 * lax.axis_size(TM)
    rest, y0, sums, *held = filter_call(rows, tap_rows(taps))
    first, stats = reduce_call(y0, sums, held, total)
    return normalize_call(pairs, stats, first, rest)


def solution(mesh):
    devices = mesh.devices
    finer = Mesh(
        devices.reshape(mesh.shape["band"], 8, 8, 2), ("band", "tm_0", "tm_1", "tm_2")
    )
    return jax.shard_map(
        on_device,
        mesh=finer,
        in_specs=(P("band", None, TM), P(), P()),
        out_specs=(P("band", None), P(None, "band", TM, None)),
        check_vma=False,
    )
```

```python
import functools
import math

import jax
import jax.numpy as jnp
import numpy as np
from jax import lax
from jax.experimental import pallas as pl
from jax.experimental.pallas import tpu as pltpu
from jax.sharding import Mesh
from jax.sharding import PartitionSpec as P

TM = ("tm_0", "tm_1", "tm_2")
ROWS = 32
LANES = 128
PITCH = 65
HALO = 16
GROUP = 8


def fill_tables(wh, wl, twc, tws):
    row = lax.broadcasted_iota(jnp.int32, (LANES, LANES), 0)
    k = lax.broadcasted_iota(jnp.int32, (LANES, LANES), 1)
    j = 4 * (row & 31) + (row >> 5)
    angle = ((j * k) & (LANES - 1)).astype(jnp.float32) * np.float32(2.0 * math.pi / LANES)
    cos, sin = jnp.cos(angle) * np.float32(1 / 64), jnp.sin(angle) * np.float32(1 / 64)
    low, high = slice(0, LANES), slice(LANES, 2 * LANES)
    for rows, cols, value in (
        (low, low, cos), (low, high, -sin), (high, low, sin), (high, high, cos),
    ):
        head = value.astype(jnp.bfloat16)
        wh[rows, cols] = head
        wl[rows, cols] = (value - head.astype(jnp.float32)).astype(jnp.bfloat16)
    i = lax.broadcasted_iota(jnp.int32, (ROWS, LANES), 0)
    k = lax.broadcasted_iota(jnp.int32, (ROWS, LANES), 1)
    turn = (i * k).astype(jnp.float32) * np.float32(2.0 * math.pi / 4096)
    twc[...] = jnp.cos(turn)
    tws[...] = jnp.sin(turn)


def add(a, b):
    return (a[0] + b[0], a[1] + b[1])


def sub(a, b):
    return (a[0] - b[0], a[1] - b[1])


def fft4(x):
    a, b = add(x[0], x[2]), sub(x[0], x[2])
    c, d = add(x[1], x[3]), sub(x[1], x[3])
    return [
        add(a, c),
        (b[0] + d[1], b[1] - d[0]),
        sub(a, c),
        (b[0] - d[1], b[1] + d[0]),
    ]


def fft8(x):
    even = fft4(x[0::2])
    odd = fft4(x[1::2])
    r = np.float32(math.sqrt(0.5))
    turned = [
        odd[0],
        ((odd[1][0] + odd[1][1]) * r, (odd[1][1] - odd[1][0]) * r),
        (odd[2][1], -odd[2][0]),
        ((odd[3][1] - odd[3][0]) * r, (odd[3][0] + odd[3][1]) * -r),
    ]
    return [add(e, o) for e, o in zip(even, turned)] + [sub(e, o) for e, o in zip(even, turned)]


def rotate(x, index, length):
    index = index % length
    if index == 0:
        return x
    if index * 4 == length:
        return (x[1], -x[0])
    c = np.float32(math.cos(2 * math.pi * index / length))
    s = np.float32(math.sin(2 * math.pi * index / length))
    return (x[0] * c + x[1] * s, x[1] * c - x[0] * s)


def block_transpose(rows):
    turned = rows.T
    lane = lax.broadcasted_iota(jnp.int32, (32, LANES), 1)
    odd = (lane & 32) != 0
    upper = (lane & 64) != 0
    r = [turned[32 * b : 32 * b + 32] for b in range(4)]

    def pair(a, b, by, mask):
        return (
            jnp.where(mask, pltpu.roll(b, by, 1), a),
            jnp.where(mask, b, pltpu.roll(a, LANES - by, 1)),
        )

    a0, a1 = pair(r[0], r[1], 32, odd)
    b0, b1 = pair(r[2], r[3], 32, odd)
    o0, o2 = pair(a0, b0, 64, upper)
    o1, o3 = pair(a1, b1, 64, upper)
    return [o0, o1, o2, o3]


def permute_taps(taps_ref, tapb):
    def batch(tb, carry):
        high = tb // 2
        parts = [
            taps_ref[pl.ds(high * 256 + (tb % 2) * 4 + q, 32, stride=8), :] for q in range(4)
        ]
        out = block_transpose(jnp.concatenate(parts, axis=0))
        for q in range(4):
            for i in range(ROWS):
                tapb[pl.ds(pl.multiple_of((i * 16 + tb * 4 + q) * 8, 8), 8), :] = jnp.broadcast_to(
                    out[q][i : i + 1], (8, LANES)
                )
        return carry

    lax.fori_loop(0, 4, batch, 0)


def permute_batch(raw, xf, b, row0):
    for c in range(2):
        x = [raw[s, pl.ds(b * 256 + c, LANES, stride=2), :] for s in range(4)]
        packed = (
            (x[0] & 255) | ((x[1] & 255) << 8) | ((x[2] & 255) << 16) | (x[3] << 24)
        )
        out = block_transpose(packed)
        for q in range(4):
            for s in range(4):
                value = out[q] << (24 - 8 * s) if s < 3 else out[q]
                value = (value >> 24).astype(jnp.float32)
                xf[2 * s + c, pl.ds(row0 + 4 * b + q, 32, stride=PITCH), :] = value


def order_of(i):
    return lax.rem(i, 4) * 8 + i // 4


def fir(xf, tapb, first, parts, extend=False):
    groups = len(parts)
    lowest = min(p[0] for p in parts)
    highest = max(p[1] for p in parts)

    def body(i, carry):
        base = i * PITCH + HALO + first * GROUP
        place = order_of(i)
        tap = {
            t: tapb[pl.ds(pl.multiple_of((i * 16 + t) * 8, 8), 8), :]
            for t in range(lowest, highest)
        }
        for s in range(4):
            at = [
                pl.ds(pl.multiple_of((p[3] * 128 + s * 32 + place) * 8, 8), 8) for p in parts
            ]
            cols = [slice(c * LANES, (c + 1) * LANES) for c in range(2)]
            acc = [
                [p[2][at[g], cols[c]] if extend else None for c in range(2)]
                for g, p in enumerate(parts)
            ]
            for w in range(1 - highest, 8 * (groups - 1) - lowest + 1):
                users = [g for g, p in enumerate(parts) if p[0] <= 8 * g - w < p[1]]
                if not users:
                    continue
                x = [xf[2 * s + c, pl.ds(base + w, 8), :] for c in range(2)]
                for g in users:
                    for c in range(2):
                        term = tap[8 * g - w] * x[c]
                        acc[g][c] = term if acc[g][c] is None else acc[g][c] + term
            for g, p in enumerate(parts):
                for c in range(2):
                    p[2][at[g], cols[c]] = acc[g][c]
        return carry

    lax.fori_loop(0, ROWS, body, 0)


def transform(refs, row_group, groups, fresh=False):
    (y, wh, wl, twc, tws, v, u, pbuf, sums) = refs

    def stage1(m, carry):
        at = pl.ds(pl.multiple_of(m * 1024, 1024), 1024)
        x = y[at, :]
        h = x.astype(jnp.bfloat16)
        l = (x - h.astype(jnp.float32)).astype(jnp.bfloat16)
        dot = functools.partial(jnp.dot, preferred_element_type=jnp.float32)
        v[at, :] = dot(h, wh[...]) + dot(l, wh[...]) + dot(h, wl[...])
        return carry

    lax.fori_loop(0, groups, stage1, 0)

    def tile(n):
        return pl.ds(pl.multiple_of(n * 8, 8), 8)

    def stage2a(gs, carry):
        for i0 in range(4):
            xs = []
            for i1 in range(8):
                i = 4 * i1 + i0
                at = tile(gs * 32 + i0 * 8 + i1)
                x = (v[at, :LANES], v[at, LANES:])
                if i:
                    c = jnp.broadcast_to(twc[i : i + 1, :], (8, LANES))
                    d = jnp.broadcast_to(tws[i : i + 1, :], (8, LANES))
                    x = (x[0] * c + x[1] * d, x[1] * c - x[0] * d)
                xs.append(x)
            for ka, x in enumerate(fft8(xs)):
                x = rotate(x, i0 * ka, 32)
                at = tile(gs * 37 + i0 * 9 + ka)
                u[0, at, :] = x[0]
                u[1, at, :] = x[1]
        return carry

    lax.fori_loop(0, 4 * groups, stage2a, 0)

    def stage2b(n, carry, fresh=False):
        g = n // 8
        ka = lax.rem(n, 8)
        rows = tile(row_group + g)

        def tally(q, value):
            sums[q, at, :] = value if fresh else sums[q, at, :] + value

        spectra = []
        for s in range(4):
            xs = []
            for i0 in range(4):
                at = tile((g * 4 + s) * 37 + i0 * 9 + ka)
                xs.append((u[0, at, :], u[1, at, :]))
            spectra.append(fft4(xs))
        for kb in range(4):
            k1 = ka + 8 * kb
            z = [spectra[s][kb] for s in range(4)]
            at = tile(k1)
            for s in range(4):
                tally(s, z[s][0] * z[s][0] + z[s][1] * z[s][1])
            cols = pl.ds(pl.multiple_of(k1 * LANES, LANES), LANES)
            for p in range(4):
                a, b = z[p // 2], z[2 + p % 2]
                re = a[0] * b[0] + a[1] * b[1]
                im = a[1] * b[0] - a[0] * b[1]
                tally(4 + p, re)
                tally(8 + p, im)
                pbuf[0, p, rows, cols] = re
                pbuf[1, p, rows, cols] = im
        return carry

    if fresh:
        lax.fori_loop(0, 8, functools.partial(stage2b, fresh=True), 0)
    if groups > 1 or not fresh:
        lax.fori_loop(8 if fresh else 0, 8 * groups, stage2b, 0)


HALF = ROWS // 2


def turned(index, by, size):
    return lax.rem(index + by, size) if by else index


class Ring:
    def __init__(self, half, a, b):
        self.half, self.a, self.b, self.c = half, a, b, TM[2]
        self.na, self.nb, self.nc = (lax.axis_size(n) for n in (a, b, self.c))
        self.members = self.na * self.nc
        self.per = HALF // self.members
        far = sorted(range(self.na), key=lambda d: -min(d, self.na - d))
        self.steps = [(d, e) for d in far for e in range(self.nc) if (d, e) != (0, 0)]
        self.shifts = sorted(range(1, self.nb), key=lambda d: -min(d, self.nb - d))

    def member(self, d=0, e=0):
        at = turned(lax.axis_index(self.a), d, self.na)
        return at * self.nc + turned(lax.axis_index(self.c), e, self.nc)

    def member_id(self, d, e):
        return {
            self.a: turned(lax.axis_index(self.a), d, self.na),
            self.c: turned(lax.axis_index(self.c), e, self.nc),
        }

    def column_id(self, d):
        return {self.b: turned(lax.axis_index(self.b), d, self.nb)}


def rings():
    return (Ring(0, TM[1], TM[0]), Ring(1, TM[0], TM[1]))


def remote(src, dst, send, recv, to):
    return pltpu.make_async_remote_copy(
        src_ref=src,
        dst_ref=dst,
        send_sem=send,
        recv_sem=recv,
        device_id=to,
        device_id_type=pl.DeviceIdType.MESH,
    )


def all_reduce(total, sums, more, stats_ref, scratch, ready):
    both = rings()
    work = []
    for ring in both:
        part, rows_in, mine, cols_in, stat, sems = scratch[ring.half]
        work.append((ring, part, rows_in, mine, cols_in, stat, sems))

    def row_copy(job, n):
        ring, part, rows_in, _, _, _, sems = job
        d, e = ring.steps[n]
        return remote(
            part.at[ring.member(d, e)], rows_in.at[n], sems.at[0], sems.at[1],
            ring.member_id(d, e),
        )

    def col_copy(job, n):
        ring, _, _, mine, cols_in, _, sems = job
        return remote(
            mine, cols_in.at[n], sems.at[2], sems.at[3], ring.column_id(ring.shifts[n])
        )

    def place(ring):
        return pl.ds(HALF * ring.half + ring.member() * ring.per, ring.per)

    def gather_copy(job, n):
        ring, _, _, _, _, stat, sems = job
        return remote(
            stat, stats_ref.at[place(ring)], sems.at[4], sems.at[5],
            ring.member_id(*ring.steps[n]),
        )

    def whole(job, kind):
        ring, _, rows_in, _, cols_in, _, sems = job
        if kind == 2:
            ref = stats_ref.at[pl.ds(0, (ring.members - 1) * ring.per)]
        else:
            ref = cols_in if kind else rows_in
        return remote(
            ref, ref, sems.at[2 * kind], sems.at[2 * kind + 1], ring.member_id(*ring.steps[0])
        )

    for job in work:
        ring, part = job[:2]
        for k in range(HALF):
            k1 = HALF * ring.half + k
            for j in range(3):
                part[k // ring.per, k % ring.per, j] = jnp.concatenate(
                    [
                        jnp.sum(
                            sums[4 * j + q, k1 * 8 : k1 * 8 + 8, :]
                            + more[4 * j + q, k1 * 8 : k1 * 8 + 8, :],
                            axis=0,
                            keepdims=True,
                        )
                        for q in range(4)
                    ],
                    axis=0,
                )

    ready()
    for n in range(max(len(job[0].steps) for job in work)):
        for job in work:
            if n < len(job[0].steps):
                row_copy(job, n).start()

    totals = []
    for job in work:
        ring, part, rows_in, mine = job[:4]
        acc = part[ring.member()]
        whole(job, 0).wait_recv()
        for n in range(len(ring.steps)):
            acc = acc + rows_in[n]
        mine[...] = acc
        for n in range(len(ring.shifts)):
            col_copy(job, n).start()
        totals.append(acc)

    for job, acc in zip(work, totals):
        ring, _, _, _, cols_in, stat, _ = job
        if ring.shifts:
            whole(job, 1).wait_recv()
        for n in range(len(ring.shifts)):
            acc = acc + cols_in[n]
        mean = acc * np.float32(1.0 / total)
        for r in range(ring.per):
            power, re, im = mean[r, 0], mean[r, 1], mean[r, 2]
            raised = power + 1e-06
            denom = jnp.concatenate(
                [raised[p // 2 : p // 2 + 1] * raised[2 + p % 2 : 3 + p % 2] for p in range(4)],
                axis=0,
            )
            stat[r, 0] = power
            stat[r, 1] = (re * re + im * im) / denom
        for n in range(len(ring.steps)):
            gather_copy(job, n).start()
        stats_ref[place(ring)] = stat[...]

    for job in work:
        whole(job, 2).wait_recv()
    for job in work:
        whole(job, 0).wait_send()
        if job[0].shifts:
            whole(job, 1).wait_send()
        whole(job, 2).wait_send()


def filter_kernel(
    samples_ref, taps_ref,
    prod_ref, y0_ref, sums, wh, wl, twc, tws,
    raw, hraw, xf, tapb, y, v, u, in_sems, halo_send, halo_recv,
):
    x_name, y_name, c_name = TM
    nx, ny, nc = (lax.axis_size(n) for n in TM)
    me = [lax.axis_index(n) for n in TM]
    place = (me[0] * ny + me[1]) * nc + me[2]
    has_next = place < nx * ny * nc - 1
    has_prev = place > 0

    def tm_id(index):
        return {
            x_name: index // (ny * nc),
            y_name: lax.rem(index // nc, ny),
            c_name: lax.rem(index, nc),
        }

    barrier = pltpu.get_barrier_semaphore()

    @pl.when(has_prev)
    def _():
        pl.semaphore_signal(
            barrier, inc=1, device_id=tm_id(place - 1), device_id_type=pl.DeviceIdType.MESH
        )

    frames = samples_ref.shape[1] // 64

    def halo_copy(b):
        lead = 1 if b == 0 else 0
        at = (4 * b + lead) * 64
        size = (4 - lead) * 64
        start = (frames - HALO) * 64 + at
        return remote(
            samples_ref.at[:, pl.ds(start, size), :], hraw.at[:, pl.ds(at, size), :],
            halo_send.at[b], halo_recv.at[b], tm_id(place + 1),
        )

    def in_copy(b):
        rows = pl.ds(pl.multiple_of(b * 256, 256), 256)
        return pltpu.make_async_copy(samples_ref.at[:, rows, :], raw.at[:, rows, :], in_sems.at[b])

    for b in range(12):
        in_copy(b).start()

    @pl.when(has_next)
    def _():
        pl.semaphore_wait(barrier, 1)
        for b in (3, 2, 1, 0):
            halo_copy(b).start()

    @pl.when(jnp.logical_not(has_prev))
    def _():
        hraw[...] = jnp.zeros_like(hraw)

    def halo_wait(b):
        @pl.when(has_prev)
        def _():
            halo_copy(b).wait_recv()

    refs = (y, wh, wl, twc, tws, v, u, prod_ref, sums)
    fill_tables(wh, wl, twc, tws)
    permute_taps(taps_ref, tapb)

    def own_batch(b, carry):
        in_copy(b).wait()
        permute_batch(raw, xf, b, HALO)
        return carry

    lax.fori_loop(0, 12, own_batch, 0)

    fir(xf, tapb, 2, [(0, 16, y, g) for g in range(4)])
    transform(refs, 1, 4, fresh=True)

    halo_wait(3)
    halo_wait(2)
    permute_batch(hraw, xf, 3, 0)
    permute_batch(hraw, xf, 2, 0)
    fir(xf, tapb, 0, [(0, 9, y0_ref, 0), (0, 16, y, 0)])
    transform(refs, 0, 1)

    halo_wait(1)
    permute_batch(hraw, xf, 1, 0)
    halo_wait(0)
    permute_batch(hraw, xf, 0, 0)
    fir(xf, tapb, 0, [(9, 16, y0_ref, 0)], extend=True)

    @pl.when(has_next)
    def _():
        for b in range(4):
            halo_copy(b).wait_send()


def reduce_kernel(
    total, y0, sums_ref, wh, wl, twc, tws, prod_ref, stats_ref,
    v, u, sums, part0, rows0, mine0, cols0, stat0, sems0,
    part1, rows1, mine1, cols1, stat1, sems1,
):
    barrier = pltpu.get_barrier_semaphore()
    greeted = 0
    for ring in rings():
        for d, e in ring.steps:
            if ring.half == 1 and d == 0:
                continue
            pl.semaphore_signal(
                barrier,
                inc=1,
                device_id=ring.member_id(d, e),
                device_id_type=pl.DeviceIdType.MESH,
            )
            greeted += 1

    transform((y0, wh, wl, twc, tws, v, u, prod_ref, sums), 0, 1, fresh=True)
    all_reduce(
        total, sums, sums_ref, stats_ref,
        (
            (part0, rows0, mine0, cols0, stat0, sems0),
            (part1, rows1, mine1, cols1, stat1, sems1),
        ),
        lambda: pl.semaphore_wait(barrier, greeted),
    )


VMEM_ALL = pl.BlockSpec(memory_space=pltpu.VMEM)
ANYWHERE = pl.BlockSpec(memory_space=pl.ANY)
WIDE = 4096 + LANES
MIB = 1024 * 1024


def filter_call(rows, taps_rows):
    frames = rows.shape[1] // 64
    f32, i32 = jnp.float32, jnp.int32
    dma = pltpu.SemaphoreType.DMA
    return pl.pallas_call(
        filter_kernel,
        out_shape=(
            jax.ShapeDtypeStruct((2, 4, frames - GROUP, WIDE), f32),
            jax.ShapeDtypeStruct((1024, 256), f32),
            jax.ShapeDtypeStruct((12, (ROWS + 1) * 8, LANES), f32),
            *[jax.ShapeDtypeStruct((256, 256), jnp.bfloat16)] * 2,
            *[jax.ShapeDtypeStruct((ROWS, LANES), f32)] * 2,
        ),
        in_specs=[ANYWHERE, VMEM_ALL],
        out_specs=(VMEM_ALL,) * 7,
        scratch_shapes=[
            pltpu.VMEM((4, frames * 64, LANES), i32),
            pltpu.VMEM((4, HALO * 64, LANES), i32),
            pltpu.VMEM((8, ROWS * PITCH + 7, LANES), f32),
            pltpu.VMEM((ROWS * 16 * 8, LANES), f32),
            pltpu.VMEM((4096, 256), f32),
            pltpu.VMEM((4096, 256), f32),
            pltpu.VMEM((2, 16 * 37 * 8 + 16, LANES), f32),
            dma((12,)),
            dma((4,)),
            dma((4,)),
        ],
        compiler_params=pltpu.CompilerParams(
            vmem_limit_bytes=45 * MIB, collective_id=0, has_side_effects=True
        ),
        cost_estimate=pl.CostEstimate(
            flops=4_000_000_000, bytes_accessed=16_000_000, transcendentals=0
        ),
        name="filter",
    )(rows, taps_rows)


def reduce_call(y0, sums, consts, total):
    f32 = jnp.float32
    dma = pltpu.SemaphoreType.DMA
    exchange = []
    for ring in rings():
        exchange += [
            pltpu.VMEM((ring.members, ring.per, 3, 4, LANES), f32),
            pltpu.VMEM((ring.members - 1, ring.per, 3, 4, LANES), f32),
            pltpu.VMEM((ring.per, 3, 4, LANES), f32),
            pltpu.VMEM((max(ring.nb - 1, 1), ring.per, 3, 4, LANES), f32),
            pltpu.VMEM((ring.per, 2, 4, LANES), f32),
            dma((6,)),
        ]
    return pl.pallas_call(
        functools.partial(reduce_kernel, total),
        out_shape=(
            jax.ShapeDtypeStruct((2, 4, GROUP, WIDE), f32),
            jax.ShapeDtypeStruct((ROWS, 2, 4, LANES), f32),
        ),
        in_specs=[VMEM_ALL] * 6,
        out_specs=(VMEM_ALL, VMEM_ALL),
        scratch_shapes=[
            pltpu.VMEM((1024, 256), f32),
            pltpu.VMEM((2, 4 * 37 * 8 + 16, LANES), f32),
            pltpu.VMEM((12, (ROWS + 1) * 8, LANES), f32),
            *exchange,
        ],
        compiler_params=pltpu.CompilerParams(
            vmem_limit_bytes=16 * MIB, collective_id=1, has_side_effects=True
        ),
        cost_estimate=pl.CostEstimate(
            flops=400_000_000, bytes_accessed=3_000_000, transcendentals=0
        ),
        name="reduce",
    )(y0, sums, *consts)


def normalize_kernel(
    pairs_ref, stats_ref, first_ref, rest_ref, coh_out, out_ref, buf, coh_ref, writes, coh_sem
):
    frames = buf.shape[2]

    def write(p, part):
        return pltpu.make_async_copy(
            buf.at[p, part], out_ref.at[part, p], writes.at[2 * p + part]
        )

    def stat(q):
        return stats_ref[pl.ds(q, ROWS, stride=8), :]

    def pair(p, carry):
        which = pairs_ref[0, p] * 2 + pairs_ref[1, p] - 2
        power = (stat(pairs_ref[0, p]) + 1e-06) * (stat(pairs_ref[1, p]) + 1e-06)
        factor = 1.0 / jnp.sqrt(power)
        for part in range(2):
            for k1 in range(ROWS):
                cols = slice(k1 * LANES, (k1 + 1) * LANES)
                row = factor[k1 : k1 + 1]
                buf[p, part, 0:GROUP, cols] = first_ref[part, which, :, cols] * row
                buf[p, part, GROUP:frames, cols] = rest_ref[part, which, :, cols] * row
            write(p, part).start()
        return carry

    lax.fori_loop(0, 4, pair, 0)
    for p in range(4):
        value = stat(4 + pairs_ref[0, p] * 2 + pairs_ref[1, p] - 2)
        for k1 in range(ROWS):
            coh_ref[p : p + 1, k1 * LANES : (k1 + 1) * LANES] = value[k1 : k1 + 1]
    coh_copy = pltpu.make_async_copy(coh_ref, coh_out, coh_sem)
    coh_copy.start()
    for p in range(4):
        for part in range(2):
            write(p, part).wait()
    coh_copy.wait()


def normalize_call(pairs, stats, first, rest):
    frames = first.shape[2] + rest.shape[2]
    f32 = jnp.float32
    return pl.pallas_call(
        normalize_kernel,
        in_specs=[pl.BlockSpec(memory_space=pltpu.SMEM)] + [VMEM_ALL] * 3,
        out_specs=(ANYWHERE, ANYWHERE),
        out_shape=(
            jax.ShapeDtypeStruct((4, 4096), f32),
            jax.ShapeDtypeStruct((2, 4, frames, 4096), f32),
        ),
        scratch_shapes=[
            pltpu.VMEM((4, 2, frames, 4096), f32),
            pltpu.VMEM((4, 4096), f32),
            pltpu.SemaphoreType.DMA((8,)),
            pltpu.SemaphoreType.DMA,
        ],
        compiler_params=pltpu.CompilerParams(vmem_limit_bytes=20 * MIB),
        cost_estimate=pl.CostEstimate(flops=2_000_000, bytes_accessed=13_000_000, transcendentals=0),
        name="normalize",
    )(pairs.T, stats.reshape(-1, LANES), first, rest)


def sample_rows(volts):
    streams, comps, local = volts.shape
    rows = volts.reshape(streams, comps, local // LANES, LANES)
    return jnp.transpose(rows, (0, 2, 1, 3)).reshape(streams, local // LANES * comps, LANES)


def tap_rows(taps):
    taps = taps.reshape(2, 8, ROWS, LANES)
    return jnp.transpose(taps, (0, 2, 1, 3)).reshape(512, LANES)


def on_device(volts, taps, pairs):
    rows = sample_rows(volts)
    total = rows.shape[1] // 64 * lax.axis_size(TM)
    rest, y0, sums, *held = filter_call(rows, tap_rows(taps))
    first, stats = reduce_call(y0, sums, held, total)
    return normalize_call(pairs, stats, first, rest)


def solution(mesh):
    devices = mesh.devices
    finer = Mesh(
        devices.reshape(mesh.shape["band"], 8, 8, 2), ("band", "tm_0", "tm_1", "tm_2")
    )
    return jax.shard_map(
        on_device,
        mesh=finer,
        in_specs=(P("band", None, TM), P(), P()),
        out_specs=(P("band", None), P(None, "band", TM, None)),
        check_vma=False,
    )
```
